16 devices in a mesh: dp: 2 (over y, z), cp: 8 (over x, core).
Axes of the slice: x: 4, y: 2, z: 1, core: 2. Of those that a mesh axis runs over, the one named last changes fastest.
The devices are a block of a 4x4x8 slice.
Arguments:
- query: bfloat16 [64, 512, 16, 256], P('dp', 'cp'), parts along dimension 0
- keys: bfloat16 [64, 512, 1, 256], P('dp', 'cp'), parts along dimension 0
- values: bfloat16 [64, 512, 1, 256], P('dp', 'cp'), parts along dimension 0
- grad_out: bfloat16 [64, 512, 16, 256], P('dp', 'cp'), parts along dimension 0
- doc_id: int32 [64, 512], P('dp', 'cp'), parts along dimension 0
Outputs:
- output 1: bfloat16 [64, 512, 16, 256], P('dp', 'cp'), parts along dimension 0
- output 2: bfloat16 [64, 512, 16, 256], P('dp', 'cp'), parts along dimension 0
- output 3: bfloat16 [64, 512, 1, 256], P('dp', 'cp'), parts along dimension 0
- output 4: bfloat16 [64, 512, 1, 256], P('dp', 'cp'), parts along dimension 0
There are 2 independent parts. The reference program is written for one: setup_inputs(seed, part) draws one part's arguments, and reference() takes and returns one part's arrays. A program takes and returns all parts, laid end to end along the dimension named above; each array names one.
All inputs are finite; a program needn't handle non-finite values.
Results may differ from the reference program's by a relative error of at most 0.0110074.
Values are sent between devices in bfloat16 or wider.
A program may use at most 768 MiB of HBM per device.

```python
import jax
import jax.numpy as jnp
from jax import lax

BATCH = 32
SEQ = 512
HEADS = 16
HEAD = 256
ROW_BLOCK = 8
DOC_CUTS = 4
NEG_BIG = -1e30


def doc_ids_row(key):
    key_cut, key_count = jax.random.split(key)
    cut_pos = jax.random.permutation(key_cut, SEQ - 1)[:DOC_CUTS] + 1
    cut_count = jax.random.randint(key_count, (), 1, DOC_CUTS + 1)
    cut_valid = jnp.arange(DOC_CUTS) < cut_count
    positions = jnp.arange(SEQ)
    cut_hits = (cut_pos[None, :] <= positions[:, None]) & cut_valid[None, :]
    return jnp.sum(cut_hits.astype(jnp.int32), axis=1).astype(jnp.int32)


def setup_inputs(seed: int = 0, part: int = 0) -> dict:
    key = jax.random.fold_in(jax.random.key(seed), part)
    key_q, key_k, key_v, key_slow, key_g, key_doc = jax.random.split(key, 6)
    query = 1.5 * jax.random.normal(key_q, (BATCH, SEQ, HEADS, HEAD), jnp.float32)
    keys = 1.5 * jax.random.normal(key_k, (BATCH, SEQ, 1, HEAD), jnp.float32)
    slow = jax.random.normal(key_slow, (BATCH, 16, 1, HEAD), jnp.float32)
    noise = jax.random.normal(key_v, (BATCH, SEQ, 1, HEAD), jnp.float32)
    values = 0.8 * jnp.repeat(slow, SEQ // 16, axis=1) + 0.6 * noise
    grad_out = 0.5 * jax.random.normal(key_g, (BATCH, SEQ, HEADS, HEAD), jnp.float32)
    doc_id = jax.vmap(doc_ids_row)(jax.random.split(key_doc, BATCH))
    return {'query': query.astype(jnp.bfloat16), 'keys': keys.astype(jnp.bfloat16), 'values': values.astype(jnp.bfloat16), 'grad_out': grad_out.astype(jnp.bfloat16), 'doc_id': doc_id}


def reference(query, keys, values, grad_out, doc_id):
    score_scale = HEAD ** -0.5
    n_blocks = SEQ // ROW_BLOCK
    key_pos = jnp.arange(SEQ)
    pos_blocks = key_pos.reshape(n_blocks, ROW_BLOCK)

    def one_row(row):
        q_row, k_row, v_row, g_row, doc_row = row
        k_mat = k_row[:, 0, :].astype(jnp.float32)
        v_mat = v_row[:, 0, :].astype(jnp.float32)
        q_blocks = q_row.reshape(n_blocks, ROW_BLOCK, HEADS, HEAD)
        g_blocks = g_row.reshape(n_blocks, ROW_BLOCK, HEADS, HEAD)
        doc_blocks = doc_row.reshape(n_blocks, ROW_BLOCK)

        def step(carry, block):
            dk_acc, dv_acc = carry
            q_block, g_block, doc_block, pos_block = block
            q_wide = q_block.astype(jnp.float32)
            g_wide = g_block.astype(jnp.float32)
            visible = (key_pos[None, :] <= pos_block[:, None]) & (doc_row[None, :] == doc_block[:, None])
            raw_scores = jnp.einsum('qhd,kd->qhk', q_wide, k_mat) * score_scale
            scores = jnp.where(visible[:, None, :], raw_scores, NEG_BIG)
            exp_scores = jnp.exp(scores - jnp.max(scores, axis=-1, keepdims=True))
            prob_f32 = exp_scores / jnp.sum(exp_scores, axis=-1, keepdims=True)
            prob_low = prob_f32.astype(jnp.bfloat16).astype(jnp.float32)
            out_block = jnp.einsum('qhk,kd->qhd', prob_low, v_mat).astype(jnp.bfloat16)
            row_delta = jnp.einsum('qhd,qhd->qh', g_wide, out_block.astype(jnp.float32))
            grad_prob = jnp.einsum('qhd,kd->qhk', g_wide, v_mat)
            grad_score = (prob_f32 * (grad_prob - row_delta[:, :, None])).astype(jnp.bfloat16).astype(jnp.float32)
            dq_block = (jnp.einsum('qhk,kd->qhd', grad_score, k_mat) * score_scale).astype(jnp.bfloat16)
            dk_acc = dk_acc + jnp.einsum('qhk,qhd->kd', grad_score, q_wide)
            dv_acc = dv_acc + jnp.einsum('qhk,qhd->kd', prob_low, g_wide)
            return (dk_acc, dv_acc), (out_block, dq_block)

        kv_zero = jnp.zeros((SEQ, HEAD), jnp.float32)
        sums, blocks = lax.scan(step, (kv_zero, kv_zero), (q_blocks, g_blocks, doc_blocks, pos_blocks))
        out_row = blocks[0].reshape(SEQ, HEADS, HEAD)
        dq_row = blocks[1].reshape(SEQ, HEADS, HEAD)
        dk_row = (sums[0] * score_scale).astype(jnp.bfloat16)[:, None, :]
        dv_row = sums[1].astype(jnp.bfloat16)[:, None, :]
        return out_row, dq_row, dk_row, dv_row

    attn_out, grad_query, grad_keys, grad_values = lax.map(one_row, (query, keys, values, grad_out, doc_id))
    return (attn_out, grad_query, grad_keys, grad_values)
```

```python
import functools

import jax
import jax.numpy as jnp
from jax import lax
from jax.experimental import pallas as pl
from jax.experimental.pallas import tpu as pltpu
from jax.sharding import PartitionSpec as P

MESH = pl.DeviceIdType.MESH
LOG2E = 1.4426950408889634
HIDDEN = -3.0e38
NACC = 8
NPRX = 4
PUSH = 4
TAKE = 2
N_ROWCHUNK = 4

OWN_TO = {0: (1, 3), 1: (2,), 2: (3,), 3: ()}
PASS_TO = {(1, 0): (2,), (2, 1): (3,)}


def attention_kernel(n_dev, n_heads, *refs):
    (q_ref, g_ref, k_ref, v_ref, doc_ref, o_ref, dq_ref, dk_ref, dv_ref,
     kv, rxx, rxy, acc, oth, prx, qb, gb, ob, dqb, pb, dsb, fin, fin_tx, fin_rx, docs, kdoc, odoc, vis,
     load_sem, doc_tx, doc_rx, kv_tx, kv_rx, kvp_tx, kvp_rx, q_sem, g_sem, o_sem, dq_sem,
     oth_tx, prx_sem, rxx_sem, rxy_sem, tx_sem, fwd_tx, fint_sem, finr_sem) = refs
    n_seq, n_rows, head_dim = q_ref.shape
    piece = k_ref.shape[1]
    two = 2 * piece
    n_chip = n_dev // 2
    scale = head_dim ** -0.5
    me = lax.axis_index('cp')
    chip = me // 2
    core = me % 2
    partner = chip * 2 + (1 - core)
    my_rows = pl.ds(pl.multiple_of(me * piece, piece), piece)
    own_half = pl.multiple_of(core * piece, piece)
    oth_half = pl.multiple_of((1 - core) * piece, piece)

    def dev(c):
        return {'cp': c * 2 + core}

    def remote(src, dst, tx, rx, to):
        return pltpu.make_async_remote_copy(src_ref=src, dst_ref=dst, send_sem=tx, recv_sem=rx,
                                            device_id=to, device_id_type=MESH)

    def local_wait(ref, sem):
        pltpu.make_async_copy(ref, ref, sem).wait()

    barrier = pltpu.get_barrier_semaphore()
    for hop in range(1, n_dev):
        pl.semaphore_signal(barrier, inc=1, device_id={'cp': (me + hop) % n_dev}, device_id_type=MESH)

    own_k = pltpu.make_async_copy(k_ref, kv.at[:, 0, my_rows, :], load_sem.at[0])
    own_v = pltpu.make_async_copy(v_ref, kv.at[:, 1, my_rows, :], load_sem.at[1])
    own_d = pltpu.make_async_copy(doc_ref, docs.at[me], load_sem.at[2])
    own_k.start()
    own_v.start()
    own_d.start()

    def q_copy(b):
        return pltpu.make_async_copy(q_ref.at[b], qb.at[b % 2], q_sem.at[b % 2])

    def g_copy(b):
        return pltpu.make_async_copy(g_ref.at[b], gb.at[b % 2], g_sem.at[b % 2])

    def o_copy(b):
        return pltpu.make_async_copy(ob.at[b % 2], o_ref.at[b], o_sem.at[b % 2])

    def dq_copy(b):
        return pltpu.make_async_copy(dqb.at[b % 2], dq_ref.at[b], dq_sem.at[b % 2])

    q_copy(0).start()
    g_copy(0).start()
    own_k.wait()
    own_v.wait()
    own_d.wait()
    odoc[...] = docs[me].reshape(n_seq, 1, piece)
    pl.semaphore_wait(barrier, n_dev - 1)

    def run_chip(c):
        n_key = two * (c + 1)
        last = two * c
        keys_here = pl.ds(0, n_key)

        def doc_copy(to):
            return remote(docs.at[me], docs.at[me], doc_tx, doc_rx, to)

        doc_dests = [{'cp': partner}] + [{'cp': d} for d in range(two // piece * (c + 1), n_dev)]
        for to in doc_dests:
            doc_copy(to).start()

        def kv_block(src, src_core, b):
            rows = pl.ds(pl.multiple_of((src * 2 + src_core) * piece, piece), piece)
            return kv.at[b, :, rows, :]

        flows = [(c, to) for to in OWN_TO[c]]
        for src in range(c):
            flows += [(src, to) for to in PASS_TO.get((c, src), ())]

        def kv_copy(src, to, b):
            blk = kv_block(src, core, b)
            return remote(blk, blk, kv_tx.at[flows.index((src, to))], kv_rx.at[src, b], dev(to))

        def kvp_copy(src, b):
            blk = kv_block(src, core, b)
            return remote(blk, blk, kvp_tx.at[src], kvp_rx.at[src, b], {'cp': partner})

        def push(b):
            for to in OWN_TO[c]:
                kv_copy(c, to, b).start()
            kvp_copy(c, b).start()

        def take(b):
            for src in range(c):
                local_wait(kv_block(src, core, b), kv_rx.at[src, b])
                for to in PASS_TO.get((c, src), ()):
                    kv_copy(src, to, b).start()
                kvp_copy(src, b).start()

        def arrived(b):
            for src in range(c + 1):
                local_wait(kv_block(src, 1 - core, b), kvp_rx.at[src, b])

        for b in range(PUSH):
            push(b)
        for b in range(TAKE):
            take(b)

        n_doc = 2 * c + 1
        pltpu.make_async_copy(docs.at[pl.ds(0, n_doc)], docs.at[pl.ds(0, n_doc)], doc_rx).wait()
        for p in range(2 * c + 2):
            kdoc[:, :, p * piece:(p + 1) * piece] = docs[p].reshape(n_seq, 1, piece)

        def compute(b):
            slot = b % 2
            keys = kv[b, 0, 0:n_key, :]
            vals = kv[b, 1, 0:n_key, :]
            tok = lax.broadcasted_iota(jnp.int32, (piece, piece), 0)
            tok_t = lax.broadcasted_iota(jnp.int32, (piece, piece), 1)
            own_doc = odoc[b]
            q_doc = jnp.sum(jnp.where(tok == tok_t, own_doc, 0), axis=1, keepdims=True)
            key_doc = kdoc[b, :, 0:n_key]
            q_pos = me * piece + lax.broadcasted_iota(jnp.int32, (piece, n_key), 0)
            k_pos = lax.broadcasted_iota(jnp.int32, (piece, n_key), 1)
            seen = (q_doc == key_doc) & (k_pos <= q_pos)
            vis[:, 0:n_key] = jnp.where(seen, 1.0, 0.0)
            rc = n_rows // N_ROWCHUNK
            tc = rc // n_heads
            for ch in range(N_ROWCHUNK):
                rows = slice(ch * rc, (ch + 1) * rc)
                qc = qb[slot, rows, :]
                gc = gb[slot, rows, :]
                s = lax.dot_general(qc, keys, (((1,), (1,)), ((), ())), preferred_element_type=jnp.float32)
                dp = lax.dot_general(gc, vals, (((1,), (1,)), ((), ())), preferred_element_type=jnp.float32)
                seen_c = vis[ch * tc:(ch + 1) * tc, 0:n_key].reshape(tc, 1, n_key)
                s3 = s.reshape(tc, n_heads, n_key)
                s3 = jnp.where(seen_c > 0.5, s3 * (scale * LOG2E), HIDDEN)
                s = s3.reshape(rc, n_key)
                e = jnp.exp2(s - jnp.max(s, axis=1, keepdims=True))
                p = e * (1.0 / jnp.sum(e, axis=1, keepdims=True))
                p16 = p.astype(jnp.bfloat16)
                o16 = jnp.dot(p16, vals, preferred_element_type=jnp.float32).astype(jnp.bfloat16)
                ob[slot, rows, :] = o16
                delta = jnp.sum(gc.astype(jnp.float32) * o16.astype(jnp.float32), axis=1, keepdims=True)
                ds16 = (p * (dp - delta)).astype(jnp.bfloat16)
                pb[rows, 0:n_key] = p16
                dsb[rows, 0:n_key] = ds16
                dq = jnp.dot(ds16, keys, preferred_element_type=jnp.float32)
                dqb[slot, rows, :] = (dq * scale).astype(jnp.bfloat16)
            dn = (((0,), (0,)), ((), ()))
            dk = lax.dot_general(dsb[:, 0:n_key], qb[slot], dn, preferred_element_type=jnp.float32)
            dv = lax.dot_general(pb[:, 0:n_key], gb[slot], dn, preferred_element_type=jnp.float32)

            @pl.when(core == 0)
            def _():
                acc[b % NACC, keys_here, :] = dk
                oth[slot, keys_here, :] = dv

            @pl.when(core == 1)
            def _():
                acc[b % NACC, keys_here, :] = dv
                oth[slot, keys_here, :] = dk

        def oth_copy(b):
            return remote(oth.at[b % 2, keys_here, :], prx.at[b % NPRX, keys_here, :], oth_tx.at[b % 2],
                          prx_sem.at[b % NPRX], {'cp': partner})

        def sum_copy(b, i, lo, n, to, buf, to_lo):
            dst, sem = (rxx, rxx_sem) if buf == 'x' else (rxy, rxy_sem)
            return remote(acc.at[b % NACC, pl.ds(lo, n), :], dst.at[b, pl.ds(to_lo, n), :],
                          tx_sem.at[i, b % NACC], sem.at[b], dev(to))

        dk_sends = {3: [(two, 2 * two, 2, 'x', 0), (0, two, 0, 'y', 0)], 2: [(0, 2 * two, 1, 'x', 0)],
                    1: [(0, two, 0, 'x', 0)], 0: []}[c]
        dv_sends = {3: [(2 * two, two, 2, 'y', 0), (0, 2 * two, 0, 'x', 0)], 2: [(two, two, 1, 'y', 0), (0, two, 3, 'y', 0)],
                    1: [(0, two, 0, 'y', 0)], 0: []}[c]

        def dk_send(b, i):
            return sum_copy(b, i, *dk_sends[i])

        def dv_send(b, i):
            return sum_copy(b, i, *dv_sends[i])

        def fwd_copy(b):
            rows = pl.ds(two, two)
            return remote(rxx.at[b, rows, :], rxx.at[b, rows, :], fwd_tx, rxx_sem.at[b], dev(1))

        def got(buf, b, lo, n):
            dst, sem = (rxx, rxx_sem) if buf == 'x' else (rxy, rxy_sem)
            local_wait(dst.at[b, pl.ds(lo, n), :], sem.at[b])

        def fin_copy(b):
            return remote(fin_tx.at[b], fin_rx.at[b], fint_sem, finr_sem, {'cp': partner})

        def finish(b, terms):
            mult = jnp.where(core == 0, scale, 1.0).astype(jnp.float32)

            def total(half):
                out = acc[b % NACC, pl.ds(last + half, piece), :]
                for ref, lo in terms:
                    out = out + ref[b, pl.ds(lo + half, piece), :]
                return (out * mult).astype(jnp.bfloat16)

            fin_tx[b] = total(oth_half)
            fin_copy(b).start()
            fin[b] = total(own_half)

        def merge_partner(b):
            local_wait(prx.at[b % NPRX, keys_here, :], prx_sem.at[b % NPRX])
            acc[b % NACC, keys_here, :] = acc[b % NACC, keys_here, :] + prx[b % NPRX, keys_here, :]
            if c == 3:
                @pl.when(core == 0)
                def _():
                    dk_send(b, 0).start()
                    dk_send(b, 1).start()

                @pl.when(core == 1)
                def _():
                    dv_send(b, 0).start()

                finish(b, [])
            if c == 2:
                @pl.when(core == 1)
                def _():
                    dv_send(b, 0).start()
                    dv_send(b, 1).start()
            if c == 1:
                @pl.when(core == 1)
                def _():
                    dv_send(b, 0).start()

        def add_rows(b, lo, n, ref, ref_lo):
            acc[b % NACC, pl.ds(lo, n), :] = acc[b % NACC, pl.ds(lo, n), :] + ref[b, pl.ds(ref_lo, n), :]

        def merge_dk(b):
            if c == 2:
                got('x', b, 0, 2 * two)
                add_rows(b, two, two, rxx, 0)
                dk_send(b, 0).start()
                finish(b, [(rxx, two)])
            if c == 1:
                got('x', b, 0, 2 * two)
                add_rows(b, 0, two, rxx, 0)
                dk_send(b, 0).start()
                finish(b, [(rxx, two)])
            if c == 0:
                got('x', b, 0, two)
                got('y', b, 0, two)
                finish(b, [(rxx, 0), (rxy, 0)])

        def merge_dv(b):
            if c == 3:
                got('y', b, 0, two)
                add_rows(b, 0, two, rxy, 0)
                dv_send(b, 1).start()
            if c == 2:
                got('y', b, 0, two)
                finish(b, [(rxy, 0)])
            if c == 0:
                got('x', b, 0, 2 * two)
                fwd_copy(b).start()
                got('y', b, 0, two)
                finish(b, [(rxx, 0), (rxy, 0)])
            if c == 1:
                got('x', b, two, two)
                got('y', b, 0, two)
                finish(b, [(rxx, two), (rxy, 0)])

        lag_dk = {3: None, 2: 3, 1: 5, 0: 7}[c]
        lag_dv = {3: 3, 2: 3, 1: 7, 0: 5}[c]
        n_step = n_seq + 7

        def when_seq(b, fn):
            pl.when((b >= 0) & (b < n_seq))(lambda: fn(b))

        def step(t, carry):
            @pl.when(t < n_seq)
            def _():
                when_seq(t + PUSH, push)
                when_seq(t + TAKE, take)

                @pl.when(t + 1 < n_seq)
                def _():
                    q_copy(t + 1).start()
                    g_copy(t + 1).start()

                @pl.when(t >= 2)
                def _():
                    o_copy(t - 2).wait()
                    dq_copy(t - 2).wait()
                    oth_copy(t - 2).wait_send()

                @pl.when((t >= NACC) & (core == 0))
                def _():
                    for i in range(len(dk_sends)):
                        dk_send(t - NACC, i).wait_send()

                @pl.when((t >= NACC) & (core == 1))
                def _():
                    for i in range(len(dv_sends)):
                        dv_send(t - NACC, i).wait_send()

                arrived(t)
                q_copy(t).wait()
                g_copy(t).wait()
                compute(t)
                o_copy(t).start()
                dq_copy(t).start()
                oth_copy(t).start()

            when_seq(t - 1, merge_partner)

            if lag_dk is not None:
                @pl.when(core == 0)
                def _():
                    when_seq(t - lag_dk, merge_dk)

            @pl.when(core == 1)
            def _():
                when_seq(t - lag_dv, merge_dv)
            return carry

        lax.fori_loop(0, n_step, step, 0)

        for b in (n_seq - 2, n_seq - 1):
            o_copy(b).wait()
            dq_copy(b).wait()
            oth_copy(b).wait_send()
        for b in range(n_seq - NACC, n_seq):
            @pl.when(core == 0)
            def _():
                for i in range(len(dk_sends)):
                    dk_send(b, i).wait_send()

            @pl.when(core == 1)
            def _():
                for i in range(len(dv_sends)):
                    dv_send(b, i).wait_send()
        whole = kv.at[:, :, pl.ds(0, piece), :]
        for i in range(len(flows)):
            local_wait(whole, kv_tx.at[i])
        for src in range(c + 1):
            local_wait(whole, kvp_tx.at[src])
        for to in doc_dests:
            doc_copy(to).wait_send()
        if c == 0:
            @pl.when(core == 1)
            def _():
                local_wait(rxx.at[:, pl.ds(0, two), :], fwd_tx)
        local_wait(fin_tx, fint_sem)
        local_wait(fin_rx, finr_sem)

    for c in range(n_chip):
        pl.when(chip == c)(functools.partial(run_chip, c))

    @pl.when(core == 0)
    def _():
        a = pltpu.make_async_copy(fin, dk_ref, load_sem.at[0])
        b = pltpu.make_async_copy(fin_rx, dv_ref, load_sem.at[1])
        a.start()
        b.start()
        a.wait()
        b.wait()

    @pl.when(core == 1)
    def _():
        a = pltpu.make_async_copy(fin, dv_ref, load_sem.at[0])
        b = pltpu.make_async_copy(fin_rx, dk_ref, load_sem.at[1])
        a.start()
        b.start()
        a.wait()
        b.wait()


def solution(mesh):
    n_dev = mesh.shape['cp']
    seq_spec = P('dp', 'cp', None, None)

    def per_device(query, keys, values, grad_out, doc_id):
        n_seq, piece, n_heads, head_dim = query.shape
        n_rows = piece * n_heads
        n_key = piece * n_dev
        two = 2 * piece
        rows_shape = (n_seq, n_rows, head_dim)
        kv_shape = (n_seq, piece, head_dim)
        bf16, f32, i32 = jnp.bfloat16, jnp.float32, jnp.int32
        dma = pltpu.SemaphoreType.DMA
        any_spec = pl.BlockSpec(memory_space=pl.ANY)
        n_chip = n_dev // 2
        out = pl.pallas_call(
            functools.partial(attention_kernel, n_dev, n_heads),
            name='attention',
            out_shape=[jax.ShapeDtypeStruct(rows_shape, bf16)] * 2 + [jax.ShapeDtypeStruct(kv_shape, bf16)] * 2,
            in_specs=[any_spec] * 5,
            out_specs=[any_spec] * 4,
            scratch_shapes=[
                pltpu.VMEM((n_seq, 2, n_key, head_dim), bf16),
                pltpu.VMEM((n_seq, 2 * two, head_dim), f32),
                pltpu.VMEM((n_seq, two, head_dim), f32),
                pltpu.VMEM((NACC, n_key, head_dim), f32),
                pltpu.VMEM((2, n_key, head_dim), f32),
                pltpu.VMEM((NPRX, n_key, head_dim), f32),
                pltpu.VMEM((2, n_rows, head_dim), bf16),
                pltpu.VMEM((2, n_rows, head_dim), bf16),
                pltpu.VMEM((2, n_rows, head_dim), bf16),
                pltpu.VMEM((2, n_rows, head_dim), bf16),
                pltpu.VMEM((n_rows, n_key), bf16),
                pltpu.VMEM((n_rows, n_key), bf16),
                pltpu.VMEM(kv_shape, bf16),
                pltpu.VMEM(kv_shape, bf16),
                pltpu.VMEM(kv_shape, bf16),
                pltpu.VMEM((n_dev, n_seq, piece), i32),
                pltpu.VMEM((n_seq, 1, n_key), i32),
                pltpu.VMEM((n_seq, 1, piece), i32),
                pltpu.VMEM((piece, n_key), f32),
                dma((3,)), dma, dma,
                dma((2,)), dma((n_chip, n_seq)), dma((n_chip,)), dma((n_chip, n_seq)),
                dma((2,)), dma((2,)), dma((2,)), dma((2,)),
                dma((2,)), dma((NPRX,)), dma((n_seq,)), dma((n_seq,)), dma((2, NACC)), dma, dma, dma,
            ],
            compiler_params=pltpu.CompilerParams(collective_id=0, has_side_effects=True, vmem_limit_bytes=63 * 1024 * 1024),
        )(query.reshape(rows_shape), grad_out.reshape(rows_shape), keys.reshape(kv_shape), values.reshape(kv_shape), doc_id)
        attn_out, grad_query, grad_keys, grad_values = out
        return (attn_out.reshape(query.shape), grad_query.reshape(query.shape),
                grad_keys.reshape(keys.shape), grad_values.reshape(values.shape))

    return jax.shard_map(per_device, mesh=mesh, in_specs=(seq_spec,) * 4 + (P('dp', 'cp'),), out_specs=(seq_spec,) * 4, check_vma=False)
```

```python
import functools

import jax
import jax.numpy as jnp
from jax import lax
from jax.experimental import pallas as pl
from jax.experimental.pallas import tpu as pltpu
from jax.sharding import PartitionSpec as P

MESH = pl.DeviceIdType.MESH
LOG2E = 1.4426950408889634
HIDDEN = -3.0e38
NACC = 12
NPRX = 4
PUSH = {0: 12, 1: 10, 2: 8, 3: 4}
TAKE = {0: 9, 1: 8, 2: 6, 3: 2}
LAG_DK = {3: None, 2: 4, 1: 6, 0: 8}
LAG_DV = {3: 4, 2: 4, 1: 9, 0: 6}
LAG_MAX = 9
N_ROWCHUNK = 4

HOPS = ((0, 0, 1, None), (0, 0, 3, None), (1, 0, 2, None), (1, 1, 2, None), (1, 1, 0, 1), (0, 1, 3, 1),
        (2, 1, 3, 0), (2, 2, 3, None))


def attention_kernel(n_dev, n_heads, *refs):
    (q_ref, g_ref, k_ref, v_ref, doc_ref, o_ref, dq_ref, dk_ref, dv_ref,
     kv, rxx, rxy, acc, oth, prx, qb, gb, ob, dqb, pb, dsb, fin, fin_tx, fin_rx, docs, kdoc, odoc, vis,
     load_sem, doc_tx, doc_rx, kv_tx, kv_rx, kvp_tx, kvp_rx, q_sem, g_sem, o_sem, dq_sem,
     oth_tx, prx_sem, rxx_sem, rxy_sem, tx_sem, fwd_tx, fint_sem, finr_sem) = refs
    n_seq, n_rows, head_dim = q_ref.shape
    piece = k_ref.shape[1]
    two = 2 * piece
    n_chip = n_dev // 2
    scale = head_dim ** -0.5
    me = lax.axis_index('cp')
    chip = me // 2
    core = me % 2
    partner = chip * 2 + (1 - core)
    my_rows = pl.ds(pl.multiple_of(me * piece, piece), piece)
    own_half = pl.multiple_of(core * piece, piece)
    oth_half = pl.multiple_of((1 - core) * piece, piece)

    def dev(c):
        return {'cp': c * 2 + core}

    def remote(src, dst, tx, rx, to):
        return pltpu.make_async_remote_copy(src_ref=src, dst_ref=dst, send_sem=tx, recv_sem=rx,
                                            device_id=to, device_id_type=MESH)

    def local_wait(ref, sem):
        pltpu.make_async_copy(ref, ref, sem).wait()

    barrier = pltpu.get_barrier_semaphore()
    for hop in range(1, n_dev):
        pl.semaphore_signal(barrier, inc=1, device_id={'cp': (me + hop) % n_dev}, device_id_type=MESH)

    own_k = pltpu.make_async_copy(k_ref, kv.at[:, 0, my_rows, :], load_sem.at[0])
    own_v = pltpu.make_async_copy(v_ref, kv.at[:, 1, my_rows, :], load_sem.at[1])
    own_d = pltpu.make_async_copy(doc_ref, docs.at[me], load_sem.at[2])
    own_k.start()
    own_v.start()
    own_d.start()

    def q_copy(b):
        return pltpu.make_async_copy(q_ref.at[b], qb.at[b % 2], q_sem.at[b % 2])

    def g_copy(b):
        return pltpu.make_async_copy(g_ref.at[b], gb.at[b % 2], g_sem.at[b % 2])

    def o_copy(b):
        return pltpu.make_async_copy(ob.at[b % 2], o_ref.at[b], o_sem.at[b % 2])

    def dq_copy(b):
        return pltpu.make_async_copy(dqb.at[b % 2], dq_ref.at[b], dq_sem.at[b % 2])

    q_copy(0).start()
    g_copy(0).start()
    own_k.wait()
    own_v.wait()
    own_d.wait()
    odoc[...] = docs[me].reshape(n_seq, 1, piece)
    pl.semaphore_wait(barrier, n_dev - 1)

    def run_chip(c):
        n_key = two * (c + 1)
        last = two * c
        keys_here = pl.ds(0, n_key)

        def doc_copy(to):
            return remote(docs.at[me], docs.at[me], doc_tx, doc_rx, to)

        doc_dests = [{'cp': partner}] + [{'cp': d} for d in range(two // piece * (c + 1), n_dev)]
        for to in doc_dests:
            doc_copy(to).start()

        def kv_block(src, src_core, b):
            rows = pl.ds(pl.multiple_of((src * 2 + src_core) * piece, piece), piece)
            return kv.at[b, :, rows, :]

        flows = [hop[1:] for hop in HOPS if hop[0] == c]
        through = [src for src, _, _ in flows if src > c]

        def by_core(who, fn):
            if who is None:
                fn()
            else:
                pl.when(core == who)(fn)

        def kv_copy(i, b):
            src, to, _ = flows[i]
            blk = kv_block(src, core, b)
            return remote(blk, blk, kv_tx.at[i], kv_rx.at[src, b], dev(to))

        def send_on(src, b):
            for i, (s, _, who) in enumerate(flows):
                if s == src:
                    by_core(who, lambda: kv_copy(i, b).start())

        def kvp_copy(src, b):
            blk = kv_block(src, core, b)
            return remote(blk, blk, kvp_tx.at[src], kvp_rx.at[src, b], {'cp': partner})

        def push(b):
            send_on(c, b)
            kvp_copy(c, b).start()

        def take(b):
            for src in range(c):
                local_wait(kv_block(src, core, b), kv_rx.at[src, b])
                send_on(src, b)
                kvp_copy(src, b).start()
            for src in through:
                who = [w for s, _, w in flows if s == src][0]

                def pass_on():
                    local_wait(kv_block(src, core, b), kv_rx.at[src, b])
                    for i, (s, _, _) in enumerate(flows):
                        if s == src:
                            kv_copy(i, b).start()

                by_core(who, pass_on)

        def arrived(b):
            for src in range(c + 1):
                local_wait(kv_block(src, 1 - core, b), kvp_rx.at[src, b])

        for b in range(PUSH[c]):
            push(b)
        for b in range(TAKE[c]):
            take(b)

        n_doc = 2 * c + 1
        pltpu.make_async_copy(docs.at[pl.ds(0, n_doc)], docs.at[pl.ds(0, n_doc)], doc_rx).wait()
        for p in range(2 * c + 2):
            kdoc[:, :, p * piece:(p + 1) * piece] = docs[p].reshape(n_seq, 1, piece)

        def compute(b):
            slot = b % 2
            keys = kv[b, 0, 0:n_key, :]
            vals = kv[b, 1, 0:n_key, :]
            tok = lax.broadcasted_iota(jnp.int32, (piece, piece), 0)
            tok_t = lax.broadcasted_iota(jnp.int32, (piece, piece), 1)
            own_doc = odoc[b]
            q_doc = jnp.sum(jnp.where(tok == tok_t, own_doc, 0), axis=1, keepdims=True)
            key_doc = kdoc[b, :, 0:n_key]
            q_pos = me * piece + lax.broadcasted_iota(jnp.int32, (piece, n_key), 0)
            k_pos = lax.broadcasted_iota(jnp.int32, (piece, n_key), 1)
            seen = (q_doc == key_doc) & (k_pos <= q_pos)
            vis[:, 0:n_key] = jnp.where(seen, 1.0, 0.0)
            rc = n_rows // N_ROWCHUNK
            tc = rc // n_heads
            for ch in range(N_ROWCHUNK):
                rows = slice(ch * rc, (ch + 1) * rc)
                qc = qb[slot, rows, :]
                gc = gb[slot, rows, :]
                s = lax.dot_general(qc, keys, (((1,), (1,)), ((), ())), preferred_element_type=jnp.float32)
                dp = lax.dot_general(gc, vals, (((1,), (1,)), ((), ())), preferred_element_type=jnp.float32)
                seen_c = vis[ch * tc:(ch + 1) * tc, 0:n_key].reshape(tc, 1, n_key)
                s3 = s.reshape(tc, n_heads, n_key)
                s3 = jnp.where(seen_c > 0.5, s3 * (scale * LOG2E), HIDDEN)
                s = s3.reshape(rc, n_key)
                e = jnp.exp2(s - jnp.max(s, axis=1, keepdims=True))
                p = e * (1.0 / jnp.sum(e, axis=1, keepdims=True))
                p16 = p.astype(jnp.bfloat16)
                o16 = jnp.dot(p16, vals, preferred_element_type=jnp.float32).astype(jnp.bfloat16)
                ob[slot, rows, :] = o16
                delta = jnp.sum(gc.astype(jnp.float32) * o16.astype(jnp.float32), axis=1, keepdims=True)
                ds16 = (p * (dp - delta)).astype(jnp.bfloat16)
                pb[rows, 0:n_key] = p16
                dsb[rows, 0:n_key] = ds16
                dq = jnp.dot(ds16, keys, preferred_element_type=jnp.float32)
                dqb[slot, rows, :] = (dq * scale).astype(jnp.bfloat16)
            dn = (((0,), (0,)), ((), ()))
            dk = lax.dot_general(dsb[:, 0:n_key], qb[slot], dn, preferred_element_type=jnp.float32)
            dv = lax.dot_general(pb[:, 0:n_key], gb[slot], dn, preferred_element_type=jnp.float32)

            @pl.when(core == 0)
            def _():
                acc[b % NACC, keys_here, :] = dk
                oth[slot, keys_here, :] = dv

            @pl.when(core == 1)
            def _():
                acc[b % NACC, keys_here, :] = dv
                oth[slot, keys_here, :] = dk

        def oth_copy(b):
            return remote(oth.at[b % 2, keys_here, :], prx.at[b % NPRX, keys_here, :], oth_tx.at[b % 2],
                          prx_sem.at[b % NPRX], {'cp': partner})

        def sum_copy(b, i, lo, n, to, buf, to_lo):
            dst, sem = (rxx, rxx_sem) if buf == 'x' else (rxy, rxy_sem)
            return remote(acc.at[b % NACC, pl.ds(lo, n), :], dst.at[b, pl.ds(to_lo, n), :],
                          tx_sem.at[i, b % NACC], sem.at[b], dev(to))

        dk_sends = {3: [(two, 2 * two, 2, 'x', 0), (0, two, 0, 'y', 0)], 2: [(0, 2 * two, 1, 'x', 0)],
                    1: [(0, two, 0, 'x', 0)], 0: []}[c]
        dv_sends = {3: [(2 * two, two, 2, 'y', 0), (0, 2 * two, 0, 'x', 0)], 2: [(two, two, 1, 'y', 0), (0, two, 3, 'y', 0)],
                    1: [(0, two, 0, 'y', 0)], 0: []}[c]

        def dk_send(b, i):
            return sum_copy(b, i, *dk_sends[i])

        def dv_send(b, i):
            return sum_copy(b, i, *dv_sends[i])

        def fwd_copy(b):
            rows = pl.ds(two, two)
            return remote(rxx.at[b, rows, :], rxx.at[b, rows, :], fwd_tx, rxx_sem.at[b], dev(1))

        def got(buf, b, lo, n):
            dst, sem = (rxx, rxx_sem) if buf == 'x' else (rxy, rxy_sem)
            local_wait(dst.at[b, pl.ds(lo, n), :], sem.at[b])

        def fin_copy(b):
            return remote(fin_tx.at[b], fin_rx.at[b], fint_sem, finr_sem, {'cp': partner})

        def finish(b, terms):
            mult = jnp.where(core == 0, scale, 1.0).astype(jnp.float32)

            def total(half):
                out = acc[b % NACC, pl.ds(last + half, piece), :]
                for ref, lo in terms:
                    out = out + ref[b, pl.ds(lo + half, piece), :]
                return (out * mult).astype(jnp.bfloat16)

            fin_tx[b] = total(oth_half)
            fin_copy(b).start()
            fin[b] = total(own_half)

        def merge_partner(b):
            local_wait(prx.at[b % NPRX, keys_here, :], prx_sem.at[b % NPRX])
            acc[b % NACC, keys_here, :] = acc[b % NACC, keys_here, :] + prx[b % NPRX, keys_here, :]
            if c == 3:
                @pl.when(core == 0)
                def _():
                    dk_send(b, 0).start()
                    dk_send(b, 1).start()

                @pl.when(core == 1)
                def _():
                    dv_send(b, 0).start()

                finish(b, [])
            if c == 2:
                @pl.when(core == 1)
                def _():
                    dv_send(b, 0).start()
                    dv_send(b, 1).start()
            if c == 1:
                @pl.when(core == 1)
                def _():
                    dv_send(b, 0).start()

        def add_rows(b, lo, n, ref, ref_lo):
            acc[b % NACC, pl.ds(lo, n), :] = acc[b % NACC, pl.ds(lo, n), :] + ref[b, pl.ds(ref_lo, n), :]

        def merge_dk(b):
            if c == 2:
                got('x', b, 0, 2 * two)
                add_rows(b, two, two, rxx, 0)
                dk_send(b, 0).start()
                finish(b, [(rxx, two)])
            if c == 1:
                got('x', b, 0, 2 * two)
                add_rows(b, 0, two, rxx, 0)
                dk_send(b, 0).start()
                finish(b, [(rxx, two)])
            if c == 0:
                got('x', b, 0, two)
                got('y', b, 0, two)
                finish(b, [(rxx, 0), (rxy, 0)])

        def merge_dv(b):
            if c == 3:
                got('y', b, 0, two)
                add_rows(b, 0, two, rxy, 0)
                dv_send(b, 1).start()
            if c == 2:
                got('y', b, 0, two)
                finish(b, [(rxy, 0)])
            if c == 0:
                got('x', b, 0, 2 * two)
                fwd_copy(b).start()
                got('y', b, 0, two)
                finish(b, [(rxx, 0), (rxy, 0)])
            if c == 1:
                got('x', b, two, two)
                got('y', b, 0, two)
                finish(b, [(rxx, two), (rxy, 0)])

        lag_dk, lag_dv = LAG_DK[c], LAG_DV[c]
        n_step = n_seq + LAG_MAX

        def when_seq(b, fn):
            pl.when((b >= 0) & (b < n_seq))(lambda: fn(b))

        def step(t, carry):
            @pl.when(t < n_seq)
            def _():
                when_seq(t + PUSH[c], push)
                when_seq(t + TAKE[c], take)

                @pl.when(t + 1 < n_seq)
                def _():
                    q_copy(t + 1).start()
                    g_copy(t + 1).start()

                @pl.when(t >= 2)
                def _():
                    o_copy(t - 2).wait()
                    dq_copy(t - 2).wait()
                    oth_copy(t - 2).wait_send()

                @pl.when((t >= NACC) & (core == 0))
                def _():
                    for i in range(len(dk_sends)):
                        dk_send(t - NACC, i).wait_send()

                @pl.when((t >= NACC) & (core == 1))
                def _():
                    for i in range(len(dv_sends)):
                        dv_send(t - NACC, i).wait_send()

                arrived(t)
                q_copy(t).wait()
                g_copy(t).wait()
                compute(t)
                o_copy(t).start()
                dq_copy(t).start()
                oth_copy(t).start()

            when_seq(t - 1, merge_partner)

            if lag_dk is not None:
                @pl.when(core == 0)
                def _():
                    when_seq(t - lag_dk, merge_dk)

            @pl.when(core == 1)
            def _():
                when_seq(t - lag_dv, merge_dv)
            return carry

        lax.fori_loop(0, n_step, step, 0)

        for b in (n_seq - 2, n_seq - 1):
            o_copy(b).wait()
            dq_copy(b).wait()
            oth_copy(b).wait_send()
        for b in range(n_seq - NACC, n_seq):
            @pl.when(core == 0)
            def _():
                for i in range(len(dk_sends)):
                    dk_send(b, i).wait_send()

            @pl.when(core == 1)
            def _():
                for i in range(len(dv_sends)):
                    dv_send(b, i).wait_send()
        whole = kv.at[:, :, pl.ds(0, piece), :]
        for i, (_, _, who) in enumerate(flows):
            by_core(who, lambda: local_wait(whole, kv_tx.at[i]))
        for src in range(c + 1):
            local_wait(whole, kvp_tx.at[src])
        for to in doc_dests:
            doc_copy(to).wait_send()
        if c == 0:
            @pl.when(core == 1)
            def _():
                local_wait(rxx.at[:, pl.ds(0, two), :], fwd_tx)
        local_wait(fin_tx, fint_sem)
        local_wait(fin_rx, finr_sem)

    for c in range(n_chip):
        pl.when(chip == c)(functools.partial(run_chip, c))

    @pl.when(core == 0)
    def _():
        a = pltpu.make_async_copy(fin, dk_ref, load_sem.at[0])
        b = pltpu.make_async_copy(fin_rx, dv_ref, load_sem.at[1])
        a.start()
        b.start()
        a.wait()
        b.wait()

    @pl.when(core == 1)
    def _():
        a = pltpu.make_async_copy(fin, dv_ref, load_sem.at[0])
        b = pltpu.make_async_copy(fin_rx, dk_ref, load_sem.at[1])
        a.start()
        b.start()
        a.wait()
        b.wait()


def solution(mesh):
    n_dev = mesh.shape['cp']
    seq_spec = P('dp', 'cp', None, None)

    def per_device(query, keys, values, grad_out, doc_id):
        n_seq, piece, n_heads, head_dim = query.shape
        n_rows = piece * n_heads
        n_key = piece * n_dev
        two = 2 * piece
        rows_shape = (n_seq, n_rows, head_dim)
        kv_shape = (n_seq, piece, head_dim)
        bf16, f32, i32 = jnp.bfloat16, jnp.float32, jnp.int32
        dma = pltpu.SemaphoreType.DMA
        any_spec = pl.BlockSpec(memory_space=pl.ANY)
        n_chip = n_dev // 2
        out = pl.pallas_call(
            functools.partial(attention_kernel, n_dev, n_heads),
            name='attention',
            out_shape=[jax.ShapeDtypeStruct(rows_shape, bf16)] * 2 + [jax.ShapeDtypeStruct(kv_shape, bf16)] * 2,
            in_specs=[any_spec] * 5,
            out_specs=[any_spec] * 4,
            scratch_shapes=[
                pltpu.VMEM((n_seq, 2, n_key, head_dim), bf16),
                pltpu.VMEM((n_seq, 2 * two, head_dim), f32),
                pltpu.VMEM((n_seq, two, head_dim), f32),
                pltpu.VMEM((NACC, n_key, head_dim), f32),
                pltpu.VMEM((2, n_key, head_dim), f32),
                pltpu.VMEM((NPRX, n_key, head_dim), f32),
                pltpu.VMEM((2, n_rows, head_dim), bf16),
                pltpu.VMEM((2, n_rows, head_dim), bf16),
                pltpu.VMEM((2, n_rows, head_dim), bf16),
                pltpu.VMEM((2, n_rows, head_dim), bf16),
                pltpu.VMEM((n_rows, n_key), bf16),
                pltpu.VMEM((n_rows, n_key), bf16),
                pltpu.VMEM(kv_shape, bf16),
                pltpu.VMEM(kv_shape, bf16),
                pltpu.VMEM(kv_shape, bf16),
                pltpu.VMEM((n_dev, n_seq, piece), i32),
                pltpu.VMEM((n_seq, 1, n_key), i32),
                pltpu.VMEM((n_seq, 1, piece), i32),
                pltpu.VMEM((piece, n_key), f32),
                dma((3,)), dma, dma,
                dma((4,)), dma((n_chip, n_seq)), dma((n_chip,)), dma((n_chip, n_seq)),
                dma((2,)), dma((2,)), dma((2,)), dma((2,)),
                dma((2,)), dma((NPRX,)), dma((n_seq,)), dma((n_seq,)), dma((2, NACC)), dma, dma, dma,
            ],
            compiler_params=pltpu.CompilerParams(collective_id=0, has_side_effects=True, vmem_limit_bytes=63 * 1024 * 1024),
        )(query.reshape(rows_shape), grad_out.reshape(rows_shape), keys.reshape(kv_shape), values.reshape(kv_shape), doc_id)
        attn_out, grad_query, grad_keys, grad_values = out
        return (attn_out.reshape(query.shape), grad_query.reshape(query.shape),
                grad_keys.reshape(keys.shape), grad_values.reshape(values.shape))

    return jax.shard_map(per_device, mesh=mesh, in_specs=(seq_spec,) * 4 + (P('dp', 'cp'),), out_specs=(seq_spec,) * 4, check_vma=False)
```

```python
import functools

import jax
import jax.numpy as jnp
from jax import lax
from jax.experimental import pallas as pl
from jax.experimental.pallas import tpu as pltpu
from jax.sharding import PartitionSpec as P

MESH = pl.DeviceIdType.MESH
LOG2E = 1.4426950408889634
HIDDEN = -3.0e38
NACC = 12
NPRX = 4
N_ROWCHUNK = 4


HOPS = ((1, 1, 2, None), (1, 1, 0, 1), (2, 1, 3, 0), (0, 1, 3, 1), (1, 0, 2, None), (2, 2, 3, None), (0, 0, 1, None),
        (0, 0, 3, None))
PUSH = {0: (1, 7), 1: (3, 9), 2: (3, 2), 3: (2, 5)}
TAKE = {0: (0, 8), 1: (4, 4), 2: (2, 2), 3: (0, 1)}
SENDS = {(3, 0): ((1, 2, 0, False), (0, 0, 1, False), (2, 2, 1, False)),
         (3, 1): ((2, 2, 0, False), (0, 0, 0, True), (1, 0, 2, False)),
         (2, 0): ((0, 1, 0, False), (1, 1, 1, True)),
         (2, 1): ((0, 3, 0, False), (1, 1, 0, False)),
         (1, 0): ((0, 0, 0, True),),
         (1, 1): ((0, 0, 1, False),)}
RELAY = {(3, 1): (2, 0), (2, 0): (2, 0), (1, 0): (3, 0), (0, 1): (4, 2)}
FINISH = {(3, 0): (1, ()), (3, 1): (1, ()), (2, 0): (5, (1,)), (2, 1): (5, (0,)), (1, 0): (8, (1,)), (1, 1): (6, (0, 1)),
          (0, 0): (8, (0, 1)), (0, 1): (8, (0, 1))}
LAG_MAX = 8


def row_plan(n):
    out = [('A', 0), ('A', 1)]
    for i in range(n + 2):
        if i + 2 < n:
            out.append(('A', i + 2))
        if i < n:
            out.append(('B', i))
        if 0 <= i - 1 < n:
            out.append(('D', i - 1))
            out.append(('E', i - 1))
        if i < n:
            out.append(('C', i))
        if i == n - 1:
            out.append(('V', 0))
    return out


def attention_kernel(n_dev, n_heads, *refs):
    (q_ref, g_ref, k_ref, v_ref, doc_ref, o_ref, dq_ref, dk_ref, dv_ref,
     kv, rx0, rx1, rx2, acc, part, prx, qb, gb, ob, dqb, pb, dsb, fin_k, fin_v, docs, kdoc, odoc, vis,
     load_sem, doc_tx, doc_rx, kv_tx, kv_rx, kvp_tx, kvp_rx, q_sem, g_sem, o_sem, dq_sem,
     part_tx, prx_sem, rx_sem, tx_sem, fwd_tx) = refs
    rx = (rx0, rx1, rx2)
    n_seq, n_rows, head_dim = q_ref.shape
    piece = k_ref.shape[1]
    two = 2 * piece
    n_chip = n_dev // 2
    scale = head_dim ** -0.5
    me = lax.axis_index('cp')
    chip = me // 2
    core = me % 2
    partner = chip * 2 + (1 - core)
    my_rows = pl.ds(pl.multiple_of(me * piece, piece), piece)

    def dev(c):
        return {'cp': c * 2 + core}

    def remote(src, dst, tx, rx, to):
        return pltpu.make_async_remote_copy(src_ref=src, dst_ref=dst, send_sem=tx, recv_sem=rx,
                                            device_id=to, device_id_type=MESH)

    def local_wait(ref, sem):
        pltpu.make_async_copy(ref, ref, sem).wait()

    barrier = pltpu.get_barrier_semaphore()
    for hop in range(1, n_dev):
        pl.semaphore_signal(barrier, inc=1, device_id={'cp': (me + hop) % n_dev}, device_id_type=MESH)

    own_k = pltpu.make_async_copy(k_ref, kv.at[:, 0, my_rows, :], load_sem.at[0])
    own_v = pltpu.make_async_copy(v_ref, kv.at[:, 1, my_rows, :], load_sem.at[1])
    own_d = pltpu.make_async_copy(doc_ref, docs.at[me], load_sem.at[2])
    own_k.start()
    own_v.start()
    own_d.start()

    def q_copy(b):
        return pltpu.make_async_copy(q_ref.at[b], qb.at[b % 2], q_sem.at[b % 2])

    def g_copy(b):
        return pltpu.make_async_copy(g_ref.at[b], gb.at[b % 2], g_sem.at[b % 2])

    def o_copy(b):
        return pltpu.make_async_copy(ob.at[b % 2], o_ref.at[b], o_sem.at[b % 2])

    def dq_copy(b):
        return pltpu.make_async_copy(dqb.at[b % 2], dq_ref.at[b], dq_sem.at[b % 2])

    q_copy(0).start()
    g_copy(0).start()
    own_k.wait()
    own_v.wait()
    own_d.wait()
    odoc[...] = docs[me].reshape(n_seq, 1, piece)
    pl.semaphore_wait(barrier, n_dev - 1)

    def run_chip(c):
        n_key = two * (c + 1)
        here = pl.ds(0, c + 1)

        def doc_copy(to):
            return remote(docs.at[me], docs.at[me], doc_tx, doc_rx, to)

        doc_dests = [{'cp': partner}] + [{'cp': d} for d in range(two // piece * (c + 1), n_dev)]
        for to in doc_dests:
            doc_copy(to).start()

        def kv_block(src, src_core, b):
            rows = pl.ds(pl.multiple_of((src * 2 + src_core) * piece, piece), piece)
            return kv.at[b, :, rows, :]

        flows = [hop[1:] for hop in HOPS if hop[0] == c]
        through = [src for src, _, _ in flows if src > c]

        def by_core(who, fn):
            if who is None:
                fn()
            else:
                pl.when(core == who)(fn)

        def kv_copy(i, b):
            src, to, _ = flows[i]
            blk = kv_block(src, core, b)
            return remote(blk, blk, kv_tx.at[i], kv_rx.at[src, b], dev(to))

        def send_on(src, b):
            for i, (s, _, who) in enumerate(flows):
                if s == src:
                    by_core(who, lambda: kv_copy(i, b).start())

        def kvp_copy(src, b):
            blk = kv_block(src, core, b)
            return remote(blk, blk, kvp_tx.at[src], kvp_rx.at[src, b], {'cp': partner})

        def push(b):
            send_on(c, b)
            kvp_copy(c, b).start()

        def take(b):
            for src in range(c - 1, -1, -1):
                local_wait(kv_block(src, core, b), kv_rx.at[src, b])
                send_on(src, b)
                kvp_copy(src, b).start()
            for src in through:
                who = [w for s, _, w in flows if s == src][0]

                def pass_on():
                    local_wait(kv_block(src, core, b), kv_rx.at[src, b])
                    for i, (s, _, _) in enumerate(flows):
                        if s == src:
                            kv_copy(i, b).start()

                by_core(who, pass_on)

        def ramp(lead, fn):
            first, most = lead
            start = min(first, most)

            def at_step(t):
                b = jnp.minimum(start + 2 * t, t + most)
                pl.when(b < n_seq)(lambda: fn(b))
                if most - start > 0:
                    pl.when(t < most - start)(lambda: fn(b + 1))

            return start, at_step

        def arrived(b):
            for src in range(c + 1):
                local_wait(kv_block(src, 1 - core, b), kvp_rx.at[src, b])

        n_push, push_at = ramp(PUSH[c], push)
        n_take, take_at = ramp(TAKE[c], take)
        for b in range(n_push):
            push(b)
        for b in range(n_take):
            take(b)

        n_doc = 2 * c + 1
        pltpu.make_async_copy(docs.at[pl.ds(0, n_doc)], docs.at[pl.ds(0, n_doc)], doc_rx).wait()
        for p in range(2 * c + 2):
            kdoc[:, :, p * piece:(p + 1) * piece] = docs[p].reshape(n_seq, 1, piece)

        def compute(b):
            slot = b % 2
            keys = kv[b, 0, 0:n_key, :]
            vals = kv[b, 1, 0:n_key, :]
            tok = lax.broadcasted_iota(jnp.int32, (piece, piece), 0)
            tok_t = lax.broadcasted_iota(jnp.int32, (piece, piece), 1)
            own_doc = odoc[b]
            q_doc = jnp.sum(jnp.where(tok == tok_t, own_doc, 0), axis=1, keepdims=True)
            key_doc = kdoc[b, :, 0:n_key]
            q_pos = me * piece + lax.broadcasted_iota(jnp.int32, (piece, n_key), 0)
            k_pos = lax.broadcasted_iota(jnp.int32, (piece, n_key), 1)
            seen = (q_doc == key_doc) & (k_pos <= q_pos)
            vis[:, 0:n_key] = jnp.where(seen, 1.0, 0.0)
            rc = n_rows // N_ROWCHUNK
            tc = rc // n_heads
            nt = (((1,), (1,)), ((), ()))
            tn = (((0,), (0,)), ((), ()))
            live = {}

            def span(ch):
                return slice(ch * rc, (ch + 1) * rc)

            def scores(ch):
                live['s', ch] = lax.dot_general(qb[slot, span(ch), :], keys, nt, preferred_element_type=jnp.float32)
                live['dp', ch] = lax.dot_general(gb[slot, span(ch), :], vals, nt, preferred_element_type=jnp.float32)

            def softmax(ch):
                seen_c = vis[ch * tc:(ch + 1) * tc, 0:n_key].reshape(tc, 1, n_key)
                s3 = live.pop(('s', ch)).reshape(tc, n_heads, n_key)
                s = jnp.where(seen_c > 0.5, s3 * (scale * LOG2E), HIDDEN).reshape(rc, n_key)
                e = jnp.exp2(s - jnp.max(s, axis=1, keepdims=True))
                p = e * (1.0 / jnp.sum(e, axis=1, keepdims=True))
                live['p', ch] = p
                pb[span(ch), 0:n_key] = p.astype(jnp.bfloat16)

            def attend(ch):
                o = jnp.dot(pb[span(ch), 0:n_key], vals, preferred_element_type=jnp.float32)
                live['o', ch] = o.astype(jnp.bfloat16)

            def dscores(ch):
                o16 = live.pop(('o', ch))
                ob[slot, span(ch), :] = o16
                gc = gb[slot, span(ch), :].astype(jnp.float32)
                delta = jnp.sum(gc * o16.astype(jnp.float32), axis=1, keepdims=True)
                dsb[span(ch), 0:n_key] = (live.pop(('p', ch)) * (live.pop(('dp', ch)) - delta)).astype(jnp.bfloat16)

            def dquery(ch):
                dq = jnp.dot(dsb[span(ch), 0:n_key], keys, preferred_element_type=jnp.float32)
                dqb[slot, span(ch), :] = (dq * scale).astype(jnp.bfloat16)

            def key_sums():
                live['dv'] = lax.dot_general(pb[:, 0:n_key], gb[slot], tn, preferred_element_type=jnp.float32)

            stages = row_plan(N_ROWCHUNK)
            for name, ch in stages:
                if name == 'A':
                    scores(ch)
                elif name == 'B':
                    softmax(ch)
                elif name == 'C':
                    attend(ch)
                elif name == 'D':
                    dscores(ch)
                elif name == 'E':
                    dquery(ch)
                elif name == 'V':
                    key_sums()
            dv = live['dv']
            dk = lax.dot_general(dsb[:, 0:n_key], qb[slot], tn, preferred_element_type=jnp.float32)

            for a in range(c + 1):
                for p in range(2):
                    rows = slice((2 * a + p) * piece, (2 * a + p + 1) * piece)
                    part[slot, p, a, 0:piece, :] = dk[rows]
                    part[slot, p, a, piece:two, :] = dv[rows]

        def part_copy(b):
            return remote(part.at[b % 2, 1 - core, here], prx.at[b % NPRX, here], part_tx.at[b % 2],
                          prx_sem.at[b % NPRX], {'cp': partner})

        def unit_copy(b, core_, i):
            a, to, buf, _ = SENDS[c, core_][i]
            return remote(acc.at[b % NACC, a], rx[buf].at[b], tx_sem.at[i, b % NACC], rx_sem.at[buf, b], dev(to))

        def got(buf, b):
            local_wait(rx[buf].at[b], rx_sem.at[buf, b])

        def merge_partner(b):
            local_wait(prx.at[b % NPRX, here], prx_sem.at[b % NPRX])
            acc[b % NACC, here] = part[b % 2, core, here] + prx[b % NPRX, here]
            for e in range(2):
                sends = [i for i, s in enumerate(SENDS.get((c, e), ())) if not s[3]]
                if sends:
                    @pl.when(core == e)
                    def _():
                        for i in sends:
                            unit_copy(b, e, i).start()

        def relay(b, e):
            buf = RELAY[c, e][1]
            got(buf, b)
            if c == 0:
                fwd_copy(b).start()
                return
            for i, (a, _, _, after) in enumerate(SENDS[c, e]):
                if after:
                    acc[b % NACC, a] = acc[b % NACC, a] + rx[buf][b]
                    unit_copy(b, e, i).start()

        def fwd_copy(b):
            return remote(rx2.at[b], rx1.at[b], fwd_tx, rx_sem.at[1, b], dev(1))

        def finish(b, e):
            total = acc[b % NACC, c]
            for buf in FINISH[c, e][1]:
                got(buf, b)
                total = total + rx[buf][b]
            fin_k[b] = (total[0:piece] * scale).astype(jnp.bfloat16)
            fin_v[b] = total[piece:two].astype(jnp.bfloat16)

        n_step = n_seq + LAG_MAX

        def when_seq(b, fn):
            pl.when((b >= 0) & (b < n_seq))(lambda: fn(b))

        def sent(b):
            for e in range(2):
                if (c, e) in SENDS:
                    @pl.when(core == e)
                    def _():
                        for i in range(len(SENDS[c, e])):
                            unit_copy(b, e, i).wait_send()

        def step(t, carry):
            @pl.when(t < n_seq)
            def _():
                push_at(t)
                take_at(t)

                @pl.when(t + 1 < n_seq)
                def _():
                    q_copy(t + 1).start()
                    g_copy(t + 1).start()

                @pl.when(t >= 2)
                def _():
                    o_copy(t - 2).wait()
                    dq_copy(t - 2).wait()
                    part_copy(t - 2).wait_send()

                pl.when(t >= NACC)(lambda: sent(t - NACC))
                arrived(t)
                q_copy(t).wait()
                g_copy(t).wait()
                compute(t)
                o_copy(t).start()
                dq_copy(t).start()
                part_copy(t).start()

            when_seq(t - 1, merge_partner)
            for e in range(2):
                @pl.when(core == e)
                def _():
                    if (c, e) in RELAY:
                        when_seq(t - RELAY[c, e][0], lambda b: relay(b, e))
                    when_seq(t - FINISH[c, e][0], lambda b: finish(b, e))
            return carry

        lax.fori_loop(0, n_step, step, 0)

        for b in (n_seq - 2, n_seq - 1):
            o_copy(b).wait()
            dq_copy(b).wait()
            part_copy(b).wait_send()
        for b in range(n_seq - NACC, n_seq):
            sent(b)
        whole = kv.at[:, :, pl.ds(0, piece), :]
        for i, (_, _, who) in enumerate(flows):
            by_core(who, lambda: local_wait(whole, kv_tx.at[i]))
        for src in range(c + 1):
            local_wait(whole, kvp_tx.at[src])
        for to in doc_dests:
            doc_copy(to).wait_send()
        if c == 0:
            pl.when(core == 1)(lambda: local_wait(rx2, fwd_tx))

    for c in range(n_chip):
        pl.when(chip == c)(functools.partial(run_chip, c))

    out_k = pltpu.make_async_copy(fin_k, dk_ref, load_sem.at[0])
    out_v = pltpu.make_async_copy(fin_v, dv_ref, load_sem.at[1])
    out_k.start()
    out_v.start()
    out_k.wait()
    out_v.wait()


def solution(mesh):
    n_dev = mesh.shape['cp']
    seq_spec = P('dp', 'cp', None, None)

    def per_device(query, keys, values, grad_out, doc_id):
        n_seq, piece, n_heads, head_dim = query.shape
        n_rows = piece * n_heads
        n_key = piece * n_dev
        two = 2 * piece
        rows_shape = (n_seq, n_rows, head_dim)
        kv_shape = (n_seq, piece, head_dim)
        bf16, f32, i32 = jnp.bfloat16, jnp.float32, jnp.int32
        dma = pltpu.SemaphoreType.DMA
        any_spec = pl.BlockSpec(memory_space=pl.ANY)
        n_chip = n_dev // 2
        out = pl.pallas_call(
            functools.partial(attention_kernel, n_dev, n_heads),
            name='attention',
            out_shape=[jax.ShapeDtypeStruct(rows_shape, bf16)] * 2 + [jax.ShapeDtypeStruct(kv_shape, bf16)] * 2,
            in_specs=[any_spec] * 5,
            out_specs=[any_spec] * 4,
            scratch_shapes=[
                pltpu.VMEM((n_seq, 2, n_key, head_dim), bf16),
                pltpu.VMEM((n_seq, two, head_dim), f32),
                pltpu.VMEM((n_seq, two, head_dim), f32),
                pltpu.VMEM((n_seq, two, head_dim), f32),
                pltpu.VMEM((NACC, n_chip, two, head_dim), f32),
                pltpu.VMEM((2, 2, n_chip, two, head_dim), f32),
                pltpu.VMEM((NPRX, n_chip, two, head_dim), f32),
                pltpu.VMEM((2, n_rows, head_dim), bf16),
                pltpu.VMEM((2, n_rows, head_dim), bf16),
                pltpu.VMEM((2, n_rows, head_dim), bf16),
                pltpu.VMEM((2, n_rows, head_dim), bf16),
                pltpu.VMEM((n_rows, n_key), bf16),
                pltpu.VMEM((n_rows, n_key), bf16),
                pltpu.VMEM(kv_shape, bf16),
                pltpu.VMEM(kv_shape, bf16),
                pltpu.VMEM((n_dev, n_seq, piece), i32),
                pltpu.VMEM((n_seq, 1, n_key), i32),
                pltpu.VMEM((n_seq, 1, piece), i32),
                pltpu.VMEM((piece, n_key), f32),
                dma((3,)), dma, dma,
                dma((4,)), dma((n_chip, n_seq)), dma((n_chip,)), dma((n_chip, n_seq)),
                dma((2,)), dma((2,)), dma((2,)), dma((2,)),
                dma((2,)), dma((NPRX,)), dma((3, n_seq)), dma((3, NACC)), dma,
            ],
            compiler_params=pltpu.CompilerParams(collective_id=0, has_side_effects=True, vmem_limit_bytes=63 * 1024 * 1024),
        )(query.reshape(rows_shape), grad_out.reshape(rows_shape), keys.reshape(kv_shape), values.reshape(kv_shape), doc_id)
        attn_out, grad_query, grad_keys, grad_values = out
        return (attn_out.reshape(query.shape), grad_query.reshape(query.shape),
                grad_keys.reshape(keys.shape), grad_values.reshape(values.shape))

    return jax.shard_map(per_device, mesh=mesh, in_specs=(seq_spec,) * 4 + (P('dp', 'cp'),), out_specs=(seq_spec,) * 4, check_vma=False)
```

```python
import functools

import jax
import jax.numpy as jnp
from jax import lax
from jax.experimental import pallas as pl
from jax.experimental.pallas import tpu as pltpu
from jax.sharding import PartitionSpec as P

MESH = pl.DeviceIdType.MESH
LOG2E = 1.4426950408889634
HIDDEN = -3.0e38
NACC = 12
NPRX = 4
N_ROWCHUNK = 4
N_COPY = 16
N_LATE = 6


HOPS = ((1, 1, 2, None), (1, 1, 0, 1), (2, 1, 3, 0), (0, 1, 3, 1), (1, 0, 2, None), (2, 2, 3, None), (0, 0, 1, None),
        (0, 0, 3, None))
PUSH = {0: (1, 7), 1: (3, 9), 2: (3, 2), 3: (2, 5)}
TAKE = {0: (0, 8), 1: (4, 4), 2: (2, 2), 3: (0, 1)}
SENDS = {(3, 0): ((1, 2, 0, False, None), (0, 0, 1, False, 1), (2, 2, 1, False, 0)),
         (3, 1): ((2, 2, 0, False, 0), (0, 0, 0, True, 1), (1, 0, 2, False, None)),
         (2, 0): ((0, 1, 0, False, None), (1, 1, 1, True, 0)),
         (2, 1): ((0, 3, 0, False, None), (1, 1, 0, False, 0)),
         (1, 0): ((0, 0, 0, True, 0),),
         (1, 1): ((0, 0, 1, False, 0),)}
RELAY = {(3, 1): (2, 0), (2, 0): (2, 0), (1, 0): (3, 0), (0, 1): (4, 2)}
FINISH = {(3, 0): (1, ()), (3, 1): (1, ()), (2, 0): (5, (1,)), (2, 1): (5, (0,)), (1, 0): (8, (1,)), (1, 1): (6, (0, 1)),
          (0, 0): (8, (0, 1)), (0, 1): (8, (0, 1))}
LAG_MAX = 8
FINISH_LATE = {(1, 1): (1,)}


def row_plan(n):
    out = [('A', 0), ('A', 1)]
    for i in range(n + 2):
        if i + 2 < n:
            out.append(('A', i + 2))
        if i < n:
            out.append(('B', i))
        if 0 <= i - 1 < n:
            out.append(('D', i - 1))
            out.append(('E', i - 1))
        if i < n:
            out.append(('C', i))
        if i == n - 1:
            out.append(('V', 0))
    return out


def attention_kernel(n_dev, n_heads, *refs):
    (q_ref, g_ref, k_ref, v_ref, doc_ref, o_ref, dq_ref, dk_ref, dv_ref, near_ref, far_ref, own_ref,
     kv, rx0, rx1, rx2, acc, part, prx, qb, gb, ob, dqb, pb, dsb, fin_k, fin_v, own, docs, kdoc, odoc, vis,
     load_sem, doc_tx, doc_rx, kv_tx, kv_rx, kvp_tx, kvp_rx, q_sem, g_sem, o_sem, dq_sem,
     part_tx, prx_sem, rx_sem, tx_sem, fwd_tx, late_sem) = refs
    rx = (rx0, rx1, rx2)
    n_seq, n_rows, head_dim = q_ref.shape
    piece = k_ref.shape[1]
    two = 2 * piece
    n_chip = n_dev // 2
    scale = head_dim ** -0.5
    me = lax.axis_index('cp')
    chip = me // 2
    core = me % 2
    partner = chip * 2 + (1 - core)
    my_rows = pl.ds(pl.multiple_of(me * piece, piece), piece)

    def dev(c):
        return {'cp': c * 2 + core}

    def remote(src, dst, tx, rx, to):
        return pltpu.make_async_remote_copy(src_ref=src, dst_ref=dst, send_sem=tx, recv_sem=rx,
                                            device_id=to, device_id_type=MESH)

    def local_wait(ref, sem):
        pltpu.make_async_copy(ref, ref, sem).wait()

    barrier = pltpu.get_barrier_semaphore()
    for hop in range(1, n_dev):
        pl.semaphore_signal(barrier, inc=1, device_id={'cp': (me + hop) % n_dev}, device_id_type=MESH)

    own_k = pltpu.make_async_copy(k_ref, kv.at[:, 0, my_rows, :], load_sem.at[0])
    own_v = pltpu.make_async_copy(v_ref, kv.at[:, 1, my_rows, :], load_sem.at[1])
    own_d = pltpu.make_async_copy(doc_ref, docs.at[me], load_sem.at[2])
    own_k.start()
    own_v.start()
    own_d.start()

    def q_copy(b):
        return pltpu.make_async_copy(q_ref.at[b], qb.at[b % 2], q_sem.at[b % 2])

    def g_copy(b):
        return pltpu.make_async_copy(g_ref.at[b], gb.at[b % 2], g_sem.at[b % 2])

    def o_copy(b):
        return pltpu.make_async_copy(ob.at[b % 2], o_ref.at[b], o_sem.at[b % 2])

    def dq_copy(b):
        return pltpu.make_async_copy(dqb.at[b % 2], dq_ref.at[b], dq_sem.at[b % 2])

    q_copy(0).start()
    g_copy(0).start()
    own_k.wait()
    own_v.wait()
    own_d.wait()
    odoc[...] = docs[me].reshape(n_seq, 1, piece)
    pl.semaphore_wait(barrier, n_dev - 1)

    def run_chip(c):
        n_key = two * (c + 1)
        here = pl.ds(0, c + 1)
        first_late = n_seq - N_LATE

        def doc_copy(to):
            return remote(docs.at[me], docs.at[me], doc_tx, doc_rx, to)

        doc_dests = [{'cp': partner}] + [{'cp': d} for d in range(two // piece * (c + 1), n_dev)]
        for to in doc_dests:
            doc_copy(to).start()

        def kv_block(src, src_core, b):
            rows = pl.ds(pl.multiple_of((src * 2 + src_core) * piece, piece), piece)
            return kv.at[b, :, rows, :]

        flows = [hop[1:] for hop in HOPS if hop[0] == c]
        through = [src for src, _, _ in flows if src > c]

        def by_core(who, fn):
            if who is None:
                fn()
            else:
                pl.when(core == who)(fn)

        def kv_copy(i, b):
            src, to, _ = flows[i]
            blk = kv_block(src, core, b)
            return remote(blk, blk, kv_tx.at[i], kv_rx.at[src, b], dev(to))

        def send_on(src, b):
            for i, (s, _, who) in enumerate(flows):
                if s == src:
                    by_core(who, lambda: kv_copy(i, b).start())

        def kvp_copy(src, b):
            blk = kv_block(src, core, b)
            return remote(blk, blk, kvp_tx.at[src], kvp_rx.at[src, b], {'cp': partner})

        def push(b):
            send_on(c, b)
            kvp_copy(c, b).start()

        def take(b):
            for src in range(c - 1, -1, -1):
                local_wait(kv_block(src, core, b), kv_rx.at[src, b])
                send_on(src, b)
                kvp_copy(src, b).start()
            for src in through:
                who = [w for s, _, w in flows if s == src][0]

                def pass_on():
                    local_wait(kv_block(src, core, b), kv_rx.at[src, b])
                    for i, (s, _, _) in enumerate(flows):
                        if s == src:
                            kv_copy(i, b).start()

                by_core(who, pass_on)

        def ramp(lead, fn):
            first, most = lead
            start = min(first, most)

            def at_step(t):
                b = jnp.minimum(start + 2 * t, t + most)
                pl.when(b < n_seq)(lambda: fn(b))
                if most - start > 0:
                    pl.when(t < most - start)(lambda: fn(b + 1))

            return start, at_step

        def arrived(b):
            for src in range(c + 1):
                local_wait(kv_block(src, 1 - core, b), kvp_rx.at[src, b])

        n_push, push_at = ramp(PUSH[c], push)
        n_take, take_at = ramp(TAKE[c], take)
        for b in range(n_push):
            push(b)
        for b in range(n_take):
            take(b)

        n_doc = 2 * c + 1
        pltpu.make_async_copy(docs.at[pl.ds(0, n_doc)], docs.at[pl.ds(0, n_doc)], doc_rx).wait()
        for p in range(2 * c + 2):
            kdoc[:, :, p * piece:(p + 1) * piece] = docs[p].reshape(n_seq, 1, piece)

        def compute(b):
            slot = b % 2
            keys = kv[b, 0, 0:n_key, :]
            vals = kv[b, 1, 0:n_key, :]
            tok = lax.broadcasted_iota(jnp.int32, (piece, piece), 0)
            tok_t = lax.broadcasted_iota(jnp.int32, (piece, piece), 1)
            own_doc = odoc[b]
            q_doc = jnp.sum(jnp.where(tok == tok_t, own_doc, 0), axis=1, keepdims=True)
            key_doc = kdoc[b, :, 0:n_key]
            q_pos = me * piece + lax.broadcasted_iota(jnp.int32, (piece, n_key), 0)
            k_pos = lax.broadcasted_iota(jnp.int32, (piece, n_key), 1)
            seen = (q_doc == key_doc) & (k_pos <= q_pos)
            vis[:, 0:n_key] = jnp.where(seen, 1.0, 0.0)
            rc = n_rows // N_ROWCHUNK
            tc = rc // n_heads
            nt = (((1,), (1,)), ((), ()))
            tn = (((0,), (0,)), ((), ()))
            live = {}

            def span(ch):
                return slice(ch * rc, (ch + 1) * rc)

            def scores(ch):
                live['s', ch] = lax.dot_general(qb[slot, span(ch), :], keys, nt, preferred_element_type=jnp.float32)
                live['dp', ch] = lax.dot_general(gb[slot, span(ch), :], vals, nt, preferred_element_type=jnp.float32)

            def softmax(ch):
                seen_c = vis[ch * tc:(ch + 1) * tc, 0:n_key].reshape(tc, 1, n_key)
                s3 = live.pop(('s', ch)).reshape(tc, n_heads, n_key)
                s = jnp.where(seen_c > 0.5, s3 * (scale * LOG2E), HIDDEN).reshape(rc, n_key)
                e = jnp.exp2(s - jnp.max(s, axis=1, keepdims=True))
                p = e * (1.0 / jnp.sum(e, axis=1, keepdims=True))
                live['p', ch] = p
                pb[span(ch), 0:n_key] = p.astype(jnp.bfloat16)

            def attend(ch):
                o = jnp.dot(pb[span(ch), 0:n_key], vals, preferred_element_type=jnp.float32)
                live['o', ch] = o.astype(jnp.bfloat16)

            def dscores(ch):
                o16 = live.pop(('o', ch))
                ob[slot, span(ch), :] = o16
                gc = gb[slot, span(ch), :].astype(jnp.float32)
                delta = jnp.sum(gc * o16.astype(jnp.float32), axis=1, keepdims=True)
                dsb[span(ch), 0:n_key] = (live.pop(('p', ch)) * (live.pop(('dp', ch)) - delta)).astype(jnp.bfloat16)

            def dquery(ch):
                dq = jnp.dot(dsb[span(ch), 0:n_key], keys, preferred_element_type=jnp.float32)
                dqb[slot, span(ch), :] = (dq * scale).astype(jnp.bfloat16)

            def key_sums():
                live['dv'] = lax.dot_general(pb[:, 0:n_key], gb[slot], tn, preferred_element_type=jnp.float32)

            stages = row_plan(N_ROWCHUNK)
            for name, ch in stages:
                if name == 'A':
                    scores(ch)
                elif name == 'B':
                    softmax(ch)
                elif name == 'C':
                    attend(ch)
                elif name == 'D':
                    dscores(ch)
                elif name == 'E':
                    dquery(ch)
                elif name == 'V':
                    key_sums()
            dv = live['dv']
            dk = lax.dot_general(dsb[:, 0:n_key], qb[slot], tn, preferred_element_type=jnp.float32)

            for a in range(c + 1):
                for p in range(2):
                    rows = slice((2 * a + p) * piece, (2 * a + p + 1) * piece)
                    part[slot, p, a, 0:piece, :] = dk[rows]
                    part[slot, p, a, piece:two, :] = dv[rows]

        def part_copy(b):
            return remote(part.at[b % 2, 1 - core, here], prx.at[b % NPRX, here], part_tx.at[b % 2],
                          prx_sem.at[b % NPRX], {'cp': partner})

        def unit_send(b, e, i):
            a, to, buf, _, late = SENDS[c, e][i]
            unit = acc.at[b % NACC, a]
            sem = tx_sem.at[i, b % NACC]

            def now():
                remote(unit, rx[buf].at[b], sem, rx_sem.at[buf, b], dev(to)).start()

            if late is None:
                now()
            else:
                pl.when(b < first_late)(now)

                @pl.when(b >= first_late)
                def _():
                    pltpu.make_async_copy(unit, (near_ref, far_ref)[late].at[b - first_late], sem).start()

        def got(buf, b):
            local_wait(rx[buf].at[b], rx_sem.at[buf, b])

        def merge_partner(b):
            local_wait(prx.at[b % NPRX, here], prx_sem.at[b % NPRX])
            acc[b % NACC, here] = part[b % 2, core, here] + prx[b % NPRX, here]
            for e in range(2):
                sends = [i for i, s in enumerate(SENDS.get((c, e), ())) if not s[3]]
                if sends:
                    @pl.when(core == e)
                    def _():
                        for i in sends:
                            unit_send(b, e, i)

        def relay(b, e):
            buf = RELAY[c, e][1]
            got(buf, b)
            if c == 0:
                fwd_copy(b).start()
                return
            for i, (a, _, _, after, _) in enumerate(SENDS[c, e]):
                if after:
                    acc[b % NACC, a] = acc[b % NACC, a] + rx[buf][b]
                    unit_send(b, e, i)

        def fwd_copy(b):
            return remote(rx2.at[b], rx1.at[b], fwd_tx, rx_sem.at[1, b], dev(1))

        def finish(b, e):
            def total(bufs):
                out = acc[b % NACC, c]
                for buf in bufs:
                    got(buf, b)
                    out = out + rx[buf][b]
                return out

            @pl.when(b < first_late)
            def _():
                out = total(FINISH[c, e][1])
                fin_k[b] = (out[0:piece] * scale).astype(jnp.bfloat16)
                fin_v[b] = out[piece:two].astype(jnp.bfloat16)

            @pl.when(b >= first_late)
            def _():
                own[b - first_late] = total(FINISH_LATE.get((c, e), ()))

        n_step = n_seq + LAG_MAX

        def when_seq(b, fn):
            pl.when((b >= 0) & (b < n_seq))(lambda: fn(b))

        def sent(b):
            for e in range(2):
                if (c, e) in SENDS:
                    @pl.when(core == e)
                    def _():
                        for i in range(len(SENDS[c, e])):
                            local_wait(acc.at[b % NACC, SENDS[c, e][i][0]], tx_sem.at[i, b % NACC])

        def step(t, carry):
            @pl.when(t < n_seq)
            def _():
                push_at(t)
                take_at(t)

                @pl.when(t + 1 < n_seq)
                def _():
                    q_copy(t + 1).start()
                    g_copy(t + 1).start()

                @pl.when(t >= 2)
                def _():
                    o_copy(t - 2).wait()
                    dq_copy(t - 2).wait()
                    part_copy(t - 2).wait_send()

                pl.when(t >= NACC)(lambda: sent(t - NACC))
                arrived(t)
                q_copy(t).wait()
                g_copy(t).wait()
                compute(t)
                o_copy(t).start()
                dq_copy(t).start()
                part_copy(t).start()

            when_seq(t - 1, merge_partner)
            for e in range(2):
                @pl.when(core == e)
                def _():
                    if (c, e) in RELAY:
                        when_seq(t - RELAY[c, e][0], lambda b: relay(b, e))
                    when_seq(t - FINISH[c, e][0], lambda b: finish(b, e))
            return carry

        lax.fori_loop(0, n_step, step, 0)

        for b in (n_seq - 2, n_seq - 1):
            o_copy(b).wait()
            dq_copy(b).wait()
            part_copy(b).wait_send()
        for b in range(n_seq - NACC, n_seq):
            sent(b)
        whole = kv.at[:, :, pl.ds(0, piece), :]
        for i, (_, _, who) in enumerate(flows):
            by_core(who, lambda: local_wait(whole, kv_tx.at[i]))
        for src in range(c + 1):
            local_wait(whole, kvp_tx.at[src])
        for to in doc_dests:
            doc_copy(to).wait_send()
        if c == 0:
            pl.when(core == 1)(lambda: local_wait(rx2, fwd_tx))

    for c in range(n_chip):
        pl.when(chip == c)(functools.partial(run_chip, c))

    out_k = pltpu.make_async_copy(fin_k, dk_ref, load_sem.at[0])
    out_v = pltpu.make_async_copy(fin_v, dv_ref, load_sem.at[1])
    out_own = pltpu.make_async_copy(own, own_ref, late_sem)
    out_k.start()
    out_v.start()
    out_own.start()
    out_k.wait()
    out_v.wait()
    out_own.wait()


def copy_kernel(a_ref, b_ref, a_out, b_out, buf, in_sem, out_sem):
    n_seq = a_ref.shape[0]
    n_buf = buf.shape[0]
    ahead = n_buf // 2

    def pick(i, fn):
        fn(a_ref, a_out, i // 2) if i % 2 == 0 else fn(b_ref, b_out, i // 2)

    def read(i):
        pick(i, lambda src, dst, j: pltpu.make_async_copy(src.at[j], buf.at[i % n_buf], in_sem.at[i % n_buf]).start())

    def read_done(i):
        pick(i, lambda src, dst, j: pltpu.make_async_copy(src.at[j], buf.at[i % n_buf], in_sem.at[i % n_buf]).wait())

    def write(i):
        pick(i, lambda src, dst, j: pltpu.make_async_copy(buf.at[i % n_buf], dst.at[j], out_sem.at[i % n_buf]).start())

    def write_done(i):
        pick(i, lambda src, dst, j: pltpu.make_async_copy(buf.at[i % n_buf], dst.at[j], out_sem.at[i % n_buf]).wait())

    total = 2 * n_seq
    for i in range(ahead):
        read(i)
    for i in range(total):
        if i + ahead < total:
            if i + ahead - n_buf >= 0:
                write_done(i + ahead - n_buf)
            read(i + ahead)
        read_done(i)
        write(i)
    for i in range(total - n_buf, total):
        write_done(i)


def solution(mesh):
    n_dev = mesh.shape['cp']
    seq_spec = P('dp', 'cp', None, None)

    def per_device(query, keys, values, grad_out, doc_id):
        n_seq, piece, n_heads, head_dim = query.shape
        n_rows = piece * n_heads
        n_key = piece * n_dev
        two = 2 * piece
        rows_shape = (n_seq, n_rows, head_dim)
        kv_shape = (n_seq, piece, head_dim)
        late_shape = (N_LATE, two, head_dim)
        bf16, f32, i32 = jnp.bfloat16, jnp.float32, jnp.int32
        dma = pltpu.SemaphoreType.DMA
        any_spec = pl.BlockSpec(memory_space=pl.ANY)
        n_chip = n_dev // 2
        out = pl.pallas_call(
            functools.partial(attention_kernel, n_dev, n_heads),
            name='attention',
            out_shape=[jax.ShapeDtypeStruct(rows_shape, bf16)] * 2 + [jax.ShapeDtypeStruct(kv_shape, bf16)] * 2
            + [jax.ShapeDtypeStruct(late_shape, f32)] * 3,
            in_specs=[any_spec] * 5,
            out_specs=[any_spec] * 7,
            scratch_shapes=[
                pltpu.VMEM((n_seq, 2, n_key, head_dim), bf16),
                pltpu.VMEM((n_seq, two, head_dim), f32),
                pltpu.VMEM((n_seq, two, head_dim), f32),
                pltpu.VMEM((n_seq, two, head_dim), f32),
                pltpu.VMEM((NACC, n_chip, two, head_dim), f32),
                pltpu.VMEM((2, 2, n_chip, two, head_dim), f32),
                pltpu.VMEM((NPRX, n_chip, two, head_dim), f32),
                pltpu.VMEM((2, n_rows, head_dim), bf16),
                pltpu.VMEM((2, n_rows, head_dim), bf16),
                pltpu.VMEM((2, n_rows, head_dim), bf16),
                pltpu.VMEM((2, n_rows, head_dim), bf16),
                pltpu.VMEM((n_rows, n_key), bf16),
                pltpu.VMEM((n_rows, n_key), bf16),
                pltpu.VMEM(kv_shape, bf16),
                pltpu.VMEM(kv_shape, bf16),
                pltpu.VMEM(late_shape, f32),
                pltpu.VMEM((n_dev, n_seq, piece), i32),
                pltpu.VMEM((n_seq, 1, n_key), i32),
                pltpu.VMEM((n_seq, 1, piece), i32),
                pltpu.VMEM((piece, n_key), f32),
                dma((3,)), dma, dma,
                dma((4,)), dma((n_chip, n_seq)), dma((n_chip,)), dma((n_chip, n_seq)),
                dma((2,)), dma((2,)), dma((2,)), dma((2,)),
                dma((2,)), dma((NPRX,)), dma((3, n_seq)), dma((3, NACC)), dma, dma,
            ],
            compiler_params=pltpu.CompilerParams(collective_id=0, has_side_effects=True, vmem_limit_bytes=63 * 1024 * 1024),
        )(query.reshape(rows_shape), grad_out.reshape(rows_shape), keys.reshape(kv_shape), values.reshape(kv_shape), doc_id)
        attn_out, grad_query, grad_keys, grad_values, near, far, own = out
        attn_out, grad_query = pl.pallas_call(
            copy_kernel,
            name='results',
            out_shape=[jax.ShapeDtypeStruct(rows_shape, bf16)] * 2,
            in_specs=[any_spec] * 2,
            out_specs=[any_spec] * 2,
            scratch_shapes=[pltpu.VMEM((N_COPY, n_rows, head_dim), bf16), dma((N_COPY,)), dma((N_COPY,))],
            compiler_params=pltpu.CompilerParams(vmem_limit_bytes=48 * 1024 * 1024),
            cost_estimate=pl.CostEstimate(flops=12_000_000_000, bytes_accessed=8 * n_seq * n_rows * head_dim,
                                          transcendentals=0),
        )(attn_out, grad_query)
        to_near = [(d, d - 2) for d in range(2, n_dev)]
        to_far = [(n_dev - 2 + e, e) for e in range(2)]
        late = own + lax.ppermute(near, 'cp', to_near) + lax.ppermute(far, 'cp', to_far)
        late_keys = (late[:, 0:piece] * head_dim ** -0.5).astype(bf16)
        late_values = late[:, piece:two].astype(bf16)
        grad_keys = jnp.concatenate([grad_keys[:n_seq - N_LATE], late_keys])
        grad_values = jnp.concatenate([grad_values[:n_seq - N_LATE], late_values])
        return (attn_out.reshape(query.shape), grad_query.reshape(query.shape),
                grad_keys.reshape(keys.shape), grad_values.reshape(values.shape))

    return jax.shard_map(per_device, mesh=mesh, in_specs=(seq_spec,) * 4 + (P('dp', 'cp'),), out_specs=(seq_spec,) * 4, check_vma=False)
```

```python
import functools

import jax
import jax.numpy as jnp
from jax import lax
from jax.experimental import pallas as pl
from jax.experimental.pallas import tpu as pltpu
from jax.sharding import PartitionSpec as P

MESH = pl.DeviceIdType.MESH
LOG2E = 1.4426950408889634
HIDDEN = -3.0e38
NACC = 12
NPRX = 4
N_COPY = 16
N_LATE = 6


HOPS = ((1, 1, 2, None), (1, 1, 0, 1), (2, 1, 3, 0), (0, 1, 3, 1), (1, 0, 2, None), (2, 2, 3, None), (0, 0, 1, None),
        (0, 0, 3, None))
PUSH = {0: (1, 7), 1: (3, 9), 2: (3, 2), 3: (2, 5)}
TAKE = {0: (0, 8), 1: (4, 4), 2: (2, 2), 3: (0, 1)}
SENDS = {(3, 0): ((1, 2, 0, False, None), (0, 0, 1, False, 1), (2, 2, 1, False, 0)),
         (3, 1): ((2, 2, 0, False, 0), (0, 0, 0, True, 1), (1, 0, 2, False, None)),
         (2, 0): ((0, 1, 0, False, None), (1, 1, 1, True, 0)),
         (2, 1): ((0, 3, 0, False, None), (1, 1, 0, False, 0)),
         (1, 0): ((0, 0, 0, True, 0),),
         (1, 1): ((0, 0, 1, False, 0),)}
RELAY = {(3, 1): (2, 0), (2, 0): (2, 0), (1, 0): (3, 0), (0, 1): (4, 2)}
FINISH = {(3, 0): (1, ()), (3, 1): (1, ()), (2, 0): (5, (1,)), (2, 1): (5, (0,)), (1, 0): (8, (1,)), (1, 1): (6, (0, 1)),
          (0, 0): (8, (0, 1)), (0, 1): (8, (0, 1))}
LAG_MAX = 8
FINISH_LATE = {(1, 1): (1,)}


def attention_kernel(n_dev, n_heads, *refs):
    (q_ref, g_ref, k_ref, v_ref, doc_ref, o_ref, dq_ref, dk_ref, dv_ref, near_ref, far_ref, own_ref,
     kv, rx0, rx1, rx2, acc, part, prx, qg, odq, pb, dsb, fin_k, fin_v, own, docs, kdoc, odoc, vis,
     load_sem, doc_tx, doc_rx, kv_tx, kv_rx, kvp_tx, kvp_rx, qg_sem, odq_sem,
     part_tx, prx_sem, rx_sem, tx_sem, fwd_tx, late_sem) = refs
    rx = (rx0, rx1, rx2)
    n_seq, n_rows, head_dim = q_ref.shape
    piece = k_ref.shape[1]
    two = 2 * piece
    n_chip = n_dev // 2
    scale = head_dim ** -0.5
    me = lax.axis_index('cp')
    chip = me // 2
    core = me % 2
    partner = chip * 2 + (1 - core)

    def dev(c):
        return {'cp': c * 2 + core}

    def remote(src, dst, tx, rx, to):
        return pltpu.make_async_remote_copy(src_ref=src, dst_ref=dst, send_sem=tx, recv_sem=rx,
                                            device_id=to, device_id_type=MESH)

    def local_wait(ref, sem):
        pltpu.make_async_copy(ref, ref, sem).wait()

    barrier = pltpu.get_barrier_semaphore()
    for hop in range(1, n_dev):
        pl.semaphore_signal(barrier, inc=1, device_id={'cp': (me + hop) % n_dev}, device_id_type=MESH)

    own_k = pltpu.make_async_copy(k_ref, kv.at[:, 0, chip, core], load_sem.at[0])
    own_v = pltpu.make_async_copy(v_ref, kv.at[:, 1, chip, core], load_sem.at[1])
    own_d = pltpu.make_async_copy(doc_ref, docs.at[me], load_sem.at[2])
    own_k.start()
    own_v.start()
    own_d.start()

    def qg_start(b):
        pltpu.make_async_copy(q_ref.at[b], qg.at[b % 2, 0], qg_sem.at[b % 2]).start()
        pltpu.make_async_copy(g_ref.at[b], qg.at[b % 2, 1], qg_sem.at[b % 2]).start()

    def odq_start(b):
        pltpu.make_async_copy(odq.at[b % 2, 0], o_ref.at[b], odq_sem.at[b % 2]).start()
        pltpu.make_async_copy(odq.at[b % 2, 1], dq_ref.at[b], odq_sem.at[b % 2]).start()

    def odq_wait(b):
        local_wait(odq.at[b % 2], odq_sem.at[b % 2])

    qg_start(0)
    own_k.wait()
    own_v.wait()
    own_d.wait()
    odoc[...] = docs[me].reshape(n_seq, 1, piece)
    pl.semaphore_wait(barrier, n_dev - 1)

    def run_chip(c):
        n_key = two * (c + 1)
        here = pl.ds(0, c + 1)
        first_late = n_seq - N_LATE

        def doc_copy(to):
            return remote(docs.at[me], docs.at[me], doc_tx, doc_rx, to)

        doc_dests = [{'cp': partner}] + [{'cp': d} for d in range(two // piece * (c + 1), n_dev)]
        for to in doc_dests:
            doc_copy(to).start()

        flows = [hop[1:] for hop in HOPS if hop[0] == c]
        through = [src for src, _, _ in flows if src > c]

        def by_core(who, fn):
            if who is None:
                fn()
            else:
                pl.when(core == who)(fn)

        def kv_sem(src, to, b):
            return kv_rx.at[0 if to == n_chip - 1 else src, b]

        def kv_copy(i, b):
            src, to, _ = flows[i]
            blk = kv.at[b, :, src, core]
            return remote(blk, blk, kv_tx.at[i], kv_sem(src, to, b), dev(to))

        def kvp_copy(b):
            blk = kv.at[b, :, here, core]
            return remote(blk, blk, kvp_tx, kvp_rx.at[b], {'cp': partner})

        def send_on(src, b):
            for i, (s, _, who) in enumerate(flows):
                if s == src:
                    by_core(who, lambda: kv_copy(i, b).start())

        def push(b):
            send_on(c, b)

        def take(b):
            if c == n_chip - 1:
                local_wait(kv.at[b, :, pl.ds(0, c), core], kv_rx.at[0, b])
            else:
                for src in range(c - 1, -1, -1):
                    local_wait(kv.at[b, :, src, core], kv_rx.at[src, b])
                    send_on(src, b)
            kvp_copy(b).start()
            for src in through:
                who = [w for s, _, w in flows if s == src][0]

                def pass_on():
                    local_wait(kv.at[b, :, src, core], kv_rx.at[src, b])
                    for i, (s, _, _) in enumerate(flows):
                        if s == src:
                            kv_copy(i, b).start()

                by_core(who, pass_on)

        def ramp(lead, fn):
            first, most = lead
            start = min(first, most)

            def at_step(t):
                b = jnp.minimum(start + 2 * t, t + most)
                pl.when(b < n_seq)(lambda: fn(b))
                if most - start > 0:
                    pl.when(t < most - start)(lambda: fn(b + 1))

            return start, at_step

        def arrived(b):
            local_wait(kv.at[b, :, here, 1 - core], kvp_rx.at[b])

        n_push, push_at = ramp(PUSH[c], push)
        n_take, take_at = ramp(TAKE[c], take)
        for b in range(n_push):
            push(b)
        for b in range(n_take):
            take(b)

        n_doc = 2 * c + 1
        pltpu.make_async_copy(docs.at[pl.ds(0, n_doc)], docs.at[pl.ds(0, n_doc)], doc_rx).wait()
        for p in range(2 * c + 2):
            kdoc[:, :, p * piece:(p + 1) * piece] = docs[p].reshape(n_seq, 1, piece)

        def compute(b):
            slot = b % 2
            keys = kv[b, 0, here].reshape(n_key, head_dim)
            vals = kv[b, 1, here].reshape(n_key, head_dim)
            tok = lax.broadcasted_iota(jnp.int32, (piece, piece), 0)
            tok_t = lax.broadcasted_iota(jnp.int32, (piece, piece), 1)
            own_doc = odoc[b]
            q_doc = jnp.sum(jnp.where(tok == tok_t, own_doc, 0), axis=1, keepdims=True)
            key_doc = kdoc[b, :, 0:n_key]
            q_pos = me * piece + lax.broadcasted_iota(jnp.int32, (piece, n_key), 0)
            k_pos = lax.broadcasted_iota(jnp.int32, (piece, n_key), 1)
            seen = (q_doc == key_doc) & (k_pos <= q_pos)
            vis[:, 0:n_key] = jnp.where(seen, 0.0, HIDDEN)
            nt = (((1,), (1,)), ((), ()))
            tn = (((0,), (0,)), ((), ()))
            f32 = jnp.float32
            s = lax.dot_general(qg[slot, 0], keys, nt, preferred_element_type=f32)
            dp = lax.dot_general(qg[slot, 1], vals, nt, preferred_element_type=f32)
            s = s.reshape(piece, n_heads, n_key) * (scale * LOG2E) + vis[:, 0:n_key].reshape(piece, 1, n_key)
            s = s.reshape(n_rows, n_key)
            e = jnp.exp2(s - jnp.max(s, axis=1, keepdims=True))
            p = e * (1.0 / jnp.sum(e, axis=1, keepdims=True))
            pb[:, 0:n_key] = p.astype(jnp.bfloat16)
            o16 = jnp.dot(pb[:, 0:n_key], vals, preferred_element_type=f32).astype(jnp.bfloat16)
            dv = lax.dot_general(pb[:, 0:n_key], qg[slot, 1], tn, preferred_element_type=f32)
            odq[slot, 0] = o16
            delta = jnp.sum(qg[slot, 1].astype(f32) * o16.astype(f32), axis=1, keepdims=True)
            dsb[:, 0:n_key] = (p * (dp - delta)).astype(jnp.bfloat16)
            dq = jnp.dot(dsb[:, 0:n_key], keys, preferred_element_type=f32)
            odq[slot, 1] = (dq * scale).astype(jnp.bfloat16)
            dk = lax.dot_general(dsb[:, 0:n_key], qg[slot, 0], tn, preferred_element_type=f32)
            for a in range(c + 1):
                for p in range(2):
                    rows = slice((2 * a + p) * piece, (2 * a + p + 1) * piece)
                    part[slot, p, a, 0:piece, :] = dk[rows]
                    part[slot, p, a, piece:two, :] = dv[rows]

        def part_copy(b):
            return remote(part.at[b % 2, 1 - core, here], prx.at[b % NPRX, here], part_tx.at[b % 2],
                          prx_sem.at[b % NPRX], {'cp': partner})

        def unit_send(b, e, i):
            a, to, buf, _, late = SENDS[c, e][i]
            unit = acc.at[b % NACC, a]
            sem = tx_sem.at[b % NACC]

            def now():
                remote(unit, rx[buf].at[b], sem, rx_sem.at[buf, b], dev(to)).start()

            if late is None:
                now()
            else:
                pl.when(b < first_late)(now)

                @pl.when(b >= first_late)
                def _():
                    pltpu.make_async_copy(unit, (near_ref, far_ref)[late].at[b - first_late], sem).start()

        def got(buf, b):
            local_wait(rx[buf].at[b], rx_sem.at[buf, b])

        def merge_partner(b):
            local_wait(prx.at[b % NPRX, here], prx_sem.at[b % NPRX])
            acc[b % NACC, here] = part[b % 2, core, here] + prx[b % NPRX, here]
            for e in range(2):
                sends = [i for i, s in enumerate(SENDS.get((c, e), ())) if not s[3]]
                if sends:
                    @pl.when(core == e)
                    def _():
                        for i in sends:
                            unit_send(b, e, i)

        def relay(b, e):
            buf = RELAY[c, e][1]
            got(buf, b)
            if c == 0:
                fwd_copy(b).start()
                return
            for i, (a, _, _, after, _) in enumerate(SENDS[c, e]):
                if after:
                    acc[b % NACC, a] = acc[b % NACC, a] + rx[buf][b]
                    unit_send(b, e, i)

        def fwd_copy(b):
            return remote(rx2.at[b], rx1.at[b], fwd_tx, rx_sem.at[1, b], dev(1))

        def finish(b, e):
            def total(bufs):
                out = acc[b % NACC, c]
                for buf in bufs:
                    got(buf, b)
                    out = out + rx[buf][b]
                return out

            @pl.when(b < first_late)
            def _():
                out = total(FINISH[c, e][1])
                fin_k[b] = (out[0:piece] * scale).astype(jnp.bfloat16)
                fin_v[b] = out[piece:two].astype(jnp.bfloat16)

            @pl.when(b >= first_late)
            def _():
                own[b - first_late] = total(FINISH_LATE.get((c, e), ()))

        n_step = n_seq + LAG_MAX

        def when_seq(b, fn):
            pl.when((b >= 0) & (b < n_seq))(lambda: fn(b))

        def sent(b):
            for e in range(2):
                n = len(SENDS.get((c, e), ()))
                if n:
                    pl.when(core == e)(lambda: local_wait(acc.at[b % NACC, pl.ds(0, n)], tx_sem.at[b % NACC]))

        def step(t, carry):
            @pl.when(t < n_seq)
            def _():
                push_at(t)
                take_at(t)

                @pl.when(t + 1 < n_seq)
                def _():
                    qg_start(t + 1)

                @pl.when(t >= 2)
                def _():
                    odq_wait(t - 2)
                    part_copy(t - 2).wait_send()

                pl.when(t >= NACC)(lambda: sent(t - NACC))
                arrived(t)
                local_wait(qg.at[t % 2], qg_sem.at[t % 2])
                compute(t)
                odq_start(t)
                part_copy(t).start()

            when_seq(t - 1, merge_partner)
            for e in range(2):
                @pl.when(core == e)
                def _():
                    if (c, e) in RELAY:
                        when_seq(t - RELAY[c, e][0], lambda b: relay(b, e))
                    when_seq(t - FINISH[c, e][0], lambda b: finish(b, e))
            return carry

        lax.fori_loop(0, n_step, step, 0)

        for b in (n_seq - 2, n_seq - 1):
            odq_wait(b)
            part_copy(b).wait_send()
        for b in range(n_seq - NACC, n_seq):
            sent(b)
        whole = kv.at[:, :, 0, 0]
        for i, (_, _, who) in enumerate(flows):
            by_core(who, lambda: local_wait(whole, kv_tx.at[i]))
        local_wait(kv.at[:, :, here, 0], kvp_tx)
        for to in doc_dests:
            doc_copy(to).wait_send()
        if c == 0:
            pl.when(core == 1)(lambda: local_wait(rx2, fwd_tx))

    for c in range(n_chip):
        pl.when(chip == c)(functools.partial(run_chip, c))

    out_k = pltpu.make_async_copy(fin_k, dk_ref, load_sem.at[0])
    out_v = pltpu.make_async_copy(fin_v, dv_ref, load_sem.at[1])
    out_own = pltpu.make_async_copy(own, own_ref, late_sem)
    out_k.start()
    out_v.start()
    out_own.start()
    out_k.wait()
    out_v.wait()
    out_own.wait()


def copy_kernel(a_ref, b_ref, a_out, b_out, buf, in_sem, out_sem):
    n_seq = a_ref.shape[0]
    n_buf = buf.shape[0]
    ahead = n_buf // 2

    def pick(i, fn):
        fn(a_ref, a_out, i // 2) if i % 2 == 0 else fn(b_ref, b_out, i // 2)

    def read(i):
        pick(i, lambda src, dst, j: pltpu.make_async_copy(src.at[j], buf.at[i % n_buf], in_sem.at[i % n_buf]).start())

    def read_done(i):
        pick(i, lambda src, dst, j: pltpu.make_async_copy(src.at[j], buf.at[i % n_buf], in_sem.at[i % n_buf]).wait())

    def write(i):
        pick(i, lambda src, dst, j: pltpu.make_async_copy(buf.at[i % n_buf], dst.at[j], out_sem.at[i % n_buf]).start())

    def write_done(i):
        pick(i, lambda src, dst, j: pltpu.make_async_copy(buf.at[i % n_buf], dst.at[j], out_sem.at[i % n_buf]).wait())

    total = 2 * n_seq
    for i in range(ahead):
        read(i)
    for i in range(total):
        if i + ahead < total:
            if i + ahead - n_buf >= 0:
                write_done(i + ahead - n_buf)
            read(i + ahead)
        read_done(i)
        write(i)
    for i in range(total - n_buf, total):
        write_done(i)


def solution(mesh):
    n_dev = mesh.shape['cp']
    seq_spec = P('dp', 'cp', None, None)

    def per_device(query, keys, values, grad_out, doc_id):
        n_seq, piece, n_heads, head_dim = query.shape
        n_rows = piece * n_heads
        n_key = piece * n_dev
        two = 2 * piece
        rows_shape = (n_seq, n_rows, head_dim)
        kv_shape = (n_seq, piece, head_dim)
        late_shape = (N_LATE, two, head_dim)
        main_shape = (n_seq - N_LATE, piece, head_dim)
        bf16, f32, i32 = jnp.bfloat16, jnp.float32, jnp.int32
        dma = pltpu.SemaphoreType.DMA
        any_spec = pl.BlockSpec(memory_space=pl.ANY)
        n_chip = n_dev // 2
        out = pl.pallas_call(
            functools.partial(attention_kernel, n_dev, n_heads),
            name='attention',
            out_shape=[jax.ShapeDtypeStruct(rows_shape, bf16)] * 2 + [jax.ShapeDtypeStruct(main_shape, bf16)] * 2
            + [jax.ShapeDtypeStruct(late_shape, f32)] * 3,
            in_specs=[any_spec] * 5,
            out_specs=[any_spec] * 7,
            scratch_shapes=[
                pltpu.VMEM((n_seq, 2, n_chip, 2, piece, head_dim), bf16),
                pltpu.VMEM((n_seq, two, head_dim), f32),
                pltpu.VMEM((n_seq, two, head_dim), f32),
                pltpu.VMEM((n_seq, two, head_dim), f32),
                pltpu.VMEM((NACC, n_chip, two, head_dim), f32),
                pltpu.VMEM((2, 2, n_chip, two, head_dim), f32),
                pltpu.VMEM((NPRX, n_chip, two, head_dim), f32),
                pltpu.VMEM((2, 2, n_rows, head_dim), bf16),
                pltpu.VMEM((2, 2, n_rows, head_dim), bf16),
                pltpu.VMEM((n_rows, n_key), bf16),
                pltpu.VMEM((n_rows, n_key), bf16),
                pltpu.VMEM(main_shape, bf16),
                pltpu.VMEM(main_shape, bf16),
                pltpu.VMEM(late_shape, f32),
                pltpu.VMEM((n_dev, n_seq, piece), i32),
                pltpu.VMEM((n_seq, 1, n_key), i32),
                pltpu.VMEM((n_seq, 1, piece), i32),
                pltpu.VMEM((piece, n_key), f32),
                dma((3,)), dma, dma,
                dma((4,)), dma((n_chip, n_seq)), dma, dma((n_seq,)),
                dma((2,)), dma((2,)),
                dma((2,)), dma((NPRX,)), dma((3, n_seq)), dma((NACC,)), dma, dma,
            ],
            compiler_params=pltpu.CompilerParams(collective_id=0, has_side_effects=True, vmem_limit_bytes=63 * 1024 * 1024),
        )(query.reshape(rows_shape), grad_out.reshape(rows_shape), keys.reshape(kv_shape), values.reshape(kv_shape), doc_id)
        attn_out, grad_query, grad_keys, grad_values, near, far, own = out
        attn_out, grad_query = pl.pallas_call(
            copy_kernel,
            name='results',
            out_shape=[jax.ShapeDtypeStruct(rows_shape, bf16)] * 2,
            in_specs=[any_spec] * 2,
            out_specs=[any_spec] * 2,
            scratch_shapes=[pltpu.VMEM((N_COPY, n_rows, head_dim), bf16), dma((N_COPY,)), dma((N_COPY,))],
            compiler_params=pltpu.CompilerParams(vmem_limit_bytes=48 * 1024 * 1024),
            cost_estimate=pl.CostEstimate(flops=12_000_000_000, bytes_accessed=8 * n_seq * n_rows * head_dim,
                                          transcendentals=0),
        )(attn_out, grad_query)
        to_near = [(d, d - 2) for d in range(2, n_dev)]
        to_far = [(n_dev - 2 + e, e) for e in range(2)]
        late = own + lax.ppermute(near, 'cp', to_near) + lax.ppermute(far, 'cp', to_far)
        late_keys = (late[:, 0:piece] * head_dim ** -0.5).astype(bf16)
        late_values = late[:, piece:two].astype(bf16)
        grad_keys = jnp.concatenate([grad_keys, late_keys])
        grad_values = jnp.concatenate([grad_values, late_values])
        return (attn_out.reshape(query.shape), grad_query.reshape(query.shape),
                grad_keys.reshape(keys.shape), grad_values.reshape(values.shape))

    return jax.shard_map(per_device, mesh=mesh, in_specs=(seq_spec,) * 4 + (P('dp', 'cp'),), out_specs=(seq_spec,) * 4, check_vma=False)
```

```python
import functools

import jax
import jax.numpy as jnp
from jax import lax
from jax.experimental import pallas as pl
from jax.experimental.pallas import tpu as pltpu
from jax.sharding import PartitionSpec as P

MESH = pl.DeviceIdType.MESH
LOG2E = 1.4426950408889634
HIDDEN = -3.0e38
NACC = 12
NPRX = 4
N_COPY = 16
N_LATE = 9


HOPS = ((1, 0, 2, None), (1, 1, 0, 1), (2, 2, 3, None), (0, 1, 3, 1), (1, 1, 2, None), (2, 1, 3, 0), (0, 0, 1, None), (0, 0, 3, None))
PUSH = {0: (1, 6), 1: (2, 12), 2: (3, 4), 3: (2, 5)}
TAKE = {0: (0, 10), 1: (3, 5), 2: (2, 2), 3: (0, 1)}
SENDS = {(3, 0): ((1, 2, 0, False, None), (0, 0, 1, False, 1), (2, 2, 1, False, 0)), (3, 1): ((2, 2, 0, False, 0), (0, 0, 0, True, 1), (1, 0, 2, False, None)), (2, 0): ((1, 1, 1, True, 0), (0, 1, 0, False, None)), (2, 1): ((0, 3, 0, False, None), (1, 1, 0, False, 0)), (1, 0): ((0, 0, 0, True, 0),), (1, 1): ((0, 0, 1, False, 0),)}
RELAY = {(3, 1): (3, 0), (2, 0): (7, 0), (1, 0): (5, 0), (0, 1): (6, 2)}
FINISH = {(3, 0): (1, ()), (3, 1): (1, ()), (2, 0): (9, (1,)), (2, 1): (5, (0,)), (1, 0): (10, (1,)), (1, 1): (6, (0, 1)), (0, 0): (8, (0, 1)), (0, 1): (9, (0, 1))}
LAG_MAX = 10
FINISH_LATE = {(1, 1): (1,)}


def attention_kernel(n_dev, n_heads, *refs):
    (q_ref, g_ref, k_ref, v_ref, doc_ref, o_ref, dq_ref, dk_ref, dv_ref, near_ref, far_ref, own_ref,
     kv, rx0, rx1, rx2, acc, part, prx, qg, odq, pb, dsb, fin_k, fin_v, own, docs, kdoc, odoc, vis,
     load_sem, doc_tx, doc_rx, kv_tx, kv_rx, kvp_tx, kvp_rx, qg_sem, odq_sem,
     part_tx, prx_sem, rx_sem, tx_sem, fwd_tx, late_sem) = refs
    rx = (rx0, rx1, rx2)
    n_seq, n_rows, head_dim = q_ref.shape
    piece = k_ref.shape[1]
    two = 2 * piece
    n_chip = n_dev // 2
    scale = head_dim ** -0.5
    me = lax.axis_index('cp')
    chip = me // 2
    core = me % 2
    partner = chip * 2 + (1 - core)

    def dev(c):
        return {'cp': c * 2 + core}

    def remote(src, dst, tx, rx, to):
        return pltpu.make_async_remote_copy(src_ref=src, dst_ref=dst, send_sem=tx, recv_sem=rx,
                                            device_id=to, device_id_type=MESH)

    def local_wait(ref, sem):
        pltpu.make_async_copy(ref, ref, sem).wait()

    barrier = pltpu.get_barrier_semaphore()
    for hop in range(1, n_dev):
        pl.semaphore_signal(barrier, inc=1, device_id={'cp': (me + hop) % n_dev}, device_id_type=MESH)

    own_k = pltpu.make_async_copy(k_ref, kv.at[:, 0, chip, core], load_sem.at[0])
    own_v = pltpu.make_async_copy(v_ref, kv.at[:, 1, chip, core], load_sem.at[1])
    own_d = pltpu.make_async_copy(doc_ref, docs.at[me], load_sem.at[2])
    own_k.start()
    own_v.start()
    own_d.start()

    def qg_start(b):
        pltpu.make_async_copy(q_ref.at[b], qg.at[b % 2, 0], qg_sem.at[b % 2]).start()
        pltpu.make_async_copy(g_ref.at[b], qg.at[b % 2, 1], qg_sem.at[b % 2]).start()

    def odq_start(b):
        pltpu.make_async_copy(odq.at[b % 2, 0], o_ref.at[b], odq_sem.at[b % 2]).start()
        pltpu.make_async_copy(odq.at[b % 2, 1], dq_ref.at[b], odq_sem.at[b % 2]).start()

    def odq_wait(b):
        local_wait(odq.at[b % 2], odq_sem.at[b % 2])

    qg_start(0)
    own_k.wait()
    own_v.wait()
    own_d.wait()
    odoc[...] = docs[me].reshape(n_seq, 1, piece)
    pl.semaphore_wait(barrier, n_dev - 1)

    def run_chip(c):
        n_key = two * (c + 1)
        here = pl.ds(0, c + 1)
        first_late = n_seq - N_LATE

        def doc_copy(to):
            return remote(docs.at[me], docs.at[me], doc_tx, doc_rx, to)

        doc_dests = [{'cp': partner}] + [{'cp': d} for d in range(two // piece * (c + 1), n_dev)]
        for to in doc_dests:
            doc_copy(to).start()

        flows = [hop[1:] for hop in HOPS if hop[0] == c]
        through = [src for src, _, _ in flows if src > c]

        def by_core(who, fn):
            if who is None:
                fn()
            else:
                pl.when(core == who)(fn)

        def kv_sem(src, to, b):
            return kv_rx.at[0 if to == n_chip - 1 else src, b]

        def kv_copy(i, b):
            src, to, _ = flows[i]
            blk = kv.at[b, :, src, core]
            return remote(blk, blk, kv_tx.at[i], kv_sem(src, to, b), dev(to))

        def kvp_copy(b):
            blk = kv.at[b, :, here, core]
            return remote(blk, blk, kvp_tx, kvp_rx.at[b], {'cp': partner})

        def send_on(src, b):
            for i, (s, _, who) in enumerate(flows):
                if s == src:
                    by_core(who, lambda: kv_copy(i, b).start())

        def push(b):
            send_on(c, b)

        def take(b):
            if c == n_chip - 1:
                local_wait(kv.at[b, :, pl.ds(0, c), core], kv_rx.at[0, b])
            else:
                for src in range(c - 1, -1, -1):
                    local_wait(kv.at[b, :, src, core], kv_rx.at[src, b])
                    send_on(src, b)
            kvp_copy(b).start()
            for src in through:
                who = [w for s, _, w in flows if s == src][0]

                def pass_on():
                    local_wait(kv.at[b, :, src, core], kv_rx.at[src, b])
                    for i, (s, _, _) in enumerate(flows):
                        if s == src:
                            kv_copy(i, b).start()

                by_core(who, pass_on)

        def ramp(lead, fn):
            first, most = lead
            start = min(first, most)

            def at_step(t):
                b = jnp.minimum(start + 2 * t, t + most)
                pl.when(b < n_seq)(lambda: fn(b))
                if most - start > 0:
                    pl.when(t < most - start)(lambda: fn(b + 1))

            return start, at_step

        def arrived(b):
            local_wait(kv.at[b, :, here, 1 - core], kvp_rx.at[b])

        n_push, push_at = ramp(PUSH[c], push)
        n_take, take_at = ramp(TAKE[c], take)
        for b in range(n_push):
            push(b)
        for b in range(n_take):
            take(b)

        n_doc = 2 * c + 1
        pltpu.make_async_copy(docs.at[pl.ds(0, n_doc)], docs.at[pl.ds(0, n_doc)], doc_rx).wait()
        for p in range(2 * c + 2):
            kdoc[:, :, p * piece:(p + 1) * piece] = docs[p].reshape(n_seq, 1, piece)

        def compute(b):
            slot = b % 2
            keys = kv[b, 0, here].reshape(n_key, head_dim)
            vals = kv[b, 1, here].reshape(n_key, head_dim)
            tok = lax.broadcasted_iota(jnp.int32, (piece, piece), 0)
            tok_t = lax.broadcasted_iota(jnp.int32, (piece, piece), 1)
            own_doc = odoc[b]
            q_doc = jnp.sum(jnp.where(tok == tok_t, own_doc, 0), axis=1, keepdims=True)
            key_doc = kdoc[b, :, 0:n_key]
            q_pos = me * piece + lax.broadcasted_iota(jnp.int32, (piece, n_key), 0)
            k_pos = lax.broadcasted_iota(jnp.int32, (piece, n_key), 1)
            seen = (q_doc == key_doc) & (k_pos <= q_pos)
            vis[:, 0:n_key] = jnp.where(seen, 0.0, HIDDEN)
            nt = (((1,), (1,)), ((), ()))
            tn = (((0,), (0,)), ((), ()))
            f32 = jnp.float32
            s = lax.dot_general(qg[slot, 0], keys, nt, preferred_element_type=f32)
            dp = lax.dot_general(qg[slot, 1], vals, nt, preferred_element_type=f32)
            s = s.reshape(piece, n_heads, n_key) * (scale * LOG2E) + vis[:, 0:n_key].reshape(piece, 1, n_key)
            s = s.reshape(n_rows, n_key)
            e = jnp.exp2(s - jnp.max(s, axis=1, keepdims=True))
            p = e * (1.0 / jnp.sum(e, axis=1, keepdims=True))
            pb[:, 0:n_key] = p.astype(jnp.bfloat16)
            o16 = jnp.dot(pb[:, 0:n_key], vals, preferred_element_type=f32).astype(jnp.bfloat16)
            dv = lax.dot_general(pb[:, 0:n_key], qg[slot, 1], tn, preferred_element_type=f32)
            odq[slot, 0] = o16
            delta = jnp.sum(qg[slot, 1].astype(f32) * o16.astype(f32), axis=1, keepdims=True)
            dsb[:, 0:n_key] = (p * (dp - delta)).astype(jnp.bfloat16)
            dq = jnp.dot(dsb[:, 0:n_key], keys, preferred_element_type=f32)
            odq[slot, 1] = (dq * scale).astype(jnp.bfloat16)
            dk = lax.dot_general(dsb[:, 0:n_key], qg[slot, 0], tn, preferred_element_type=f32)
            for a in range(c + 1):
                for p in range(2):
                    rows = slice((2 * a + p) * piece, (2 * a + p + 1) * piece)
                    part[slot, p, a, 0:piece, :] = dk[rows]
                    part[slot, p, a, piece:two, :] = dv[rows]

        def part_copy(b):
            return remote(part.at[b % 2, 1 - core, here], prx.at[b % NPRX, here], part_tx.at[b % 2],
                          prx_sem.at[b % NPRX], {'cp': partner})

        def unit_send(b, e, i):
            a, to, buf, _, late = SENDS[c, e][i]
            unit = acc.at[b % NACC, a]
            sem = tx_sem.at[b % NACC]

            def now():
                remote(unit, rx[buf].at[b], sem, rx_sem.at[buf, b], dev(to)).start()

            if late is None:
                now()
            else:
                pl.when(b < first_late)(now)

                @pl.when(b >= first_late)
                def _():
                    pltpu.make_async_copy(unit, (near_ref, far_ref)[late].at[b - first_late], sem).start()

        def got(buf, b):
            local_wait(rx[buf].at[b], rx_sem.at[buf, b])

        def merge_partner(b):
            local_wait(prx.at[b % NPRX, here], prx_sem.at[b % NPRX])
            acc[b % NACC, here] = part[b % 2, core, here] + prx[b % NPRX, here]
            for e in range(2):
                sends = [i for i, s in enumerate(SENDS.get((c, e), ())) if not s[3]]
                if sends:
                    @pl.when(core == e)
                    def _():
                        for i in sends:
                            unit_send(b, e, i)

        def relay(b, e):
            buf = RELAY[c, e][1]
            got(buf, b)
            if c == 0:
                fwd_copy(b).start()
                return
            for i, (a, _, _, after, _) in enumerate(SENDS[c, e]):
                if after:
                    acc[b % NACC, a] = acc[b % NACC, a] + rx[buf][b]
                    unit_send(b, e, i)

        def fwd_copy(b):
            return remote(rx2.at[b], rx1.at[b], fwd_tx, rx_sem.at[1, b], dev(1))

        def finish(b, e):
            def total(bufs):
                out = acc[b % NACC, c]
                for buf in bufs:
                    got(buf, b)
                    out = out + rx[buf][b]
                return out

            @pl.when(b < first_late)
            def _():
                out = total(FINISH[c, e][1])
                fin_k[b] = (out[0:piece] * scale).astype(jnp.bfloat16)
                fin_v[b] = out[piece:two].astype(jnp.bfloat16)

            @pl.when(b >= first_late)
            def _():
                own[b - first_late] = total(FINISH_LATE.get((c, e), ()))

        n_step = n_seq + LAG_MAX

        def when_seq(b, fn):
            pl.when((b >= 0) & (b < n_seq))(lambda: fn(b))

        def sent(b):
            for e in range(2):
                n = len(SENDS.get((c, e), ()))
                if n:
                    pl.when(core == e)(lambda: local_wait(acc.at[b % NACC, pl.ds(0, n)], tx_sem.at[b % NACC]))

        def step(t, carry):
            @pl.when(t < n_seq)
            def _():
                push_at(t)
                take_at(t)

                @pl.when(t + 1 < n_seq)
                def _():
                    qg_start(t + 1)

                @pl.when(t >= 2)
                def _():
                    odq_wait(t - 2)
                    part_copy(t - 2).wait_send()

                pl.when(t >= NACC)(lambda: sent(t - NACC))
                arrived(t)
                local_wait(qg.at[t % 2], qg_sem.at[t % 2])
                compute(t)
                odq_start(t)
                part_copy(t).start()

            when_seq(t - 1, merge_partner)
            for e in range(2):
                @pl.when(core == e)
                def _():
                    if (c, e) in RELAY:
                        when_seq(t - RELAY[c, e][0], lambda b: relay(b, e))
                    when_seq(t - FINISH[c, e][0], lambda b: finish(b, e))
            return carry

        lax.fori_loop(0, n_step, step, 0)

        for b in (n_seq - 2, n_seq - 1):
            odq_wait(b)
            part_copy(b).wait_send()
        for b in range(n_seq - NACC, n_seq):
            sent(b)
        whole = kv.at[:, :, 0, 0]
        for i, (_, _, who) in enumerate(flows):
            by_core(who, lambda: local_wait(whole, kv_tx.at[i]))
        local_wait(kv.at[:, :, here, 0], kvp_tx)
        for to in doc_dests:
            doc_copy(to).wait_send()
        if c == 0:
            pl.when(core == 1)(lambda: local_wait(rx2, fwd_tx))

    for c in range(n_chip):
        pl.when(chip == c)(functools.partial(run_chip, c))

    out_k = pltpu.make_async_copy(fin_k, dk_ref, load_sem.at[0])
    out_v = pltpu.make_async_copy(fin_v, dv_ref, load_sem.at[1])
    out_own = pltpu.make_async_copy(own, own_ref, late_sem)
    out_k.start()
    out_v.start()
    out_own.start()
    out_k.wait()
    out_v.wait()
    out_own.wait()


def copy_kernel(a_ref, b_ref, a_out, b_out, buf, in_sem, out_sem):
    n_seq = a_ref.shape[0]
    n_buf = buf.shape[0]
    ahead = n_buf // 2

    def pick(i, fn):
        fn(a_ref, a_out, i // 2) if i % 2 == 0 else fn(b_ref, b_out, i // 2)

    def read(i):
        pick(i, lambda src, dst, j: pltpu.make_async_copy(src.at[j], buf.at[i % n_buf], in_sem.at[i % n_buf]).start())

    def read_done(i):
        pick(i, lambda src, dst, j: pltpu.make_async_copy(src.at[j], buf.at[i % n_buf], in_sem.at[i % n_buf]).wait())

    def write(i):
        pick(i, lambda src, dst, j: pltpu.make_async_copy(buf.at[i % n_buf], dst.at[j], out_sem.at[i % n_buf]).start())

    def write_done(i):
        pick(i, lambda src, dst, j: pltpu.make_async_copy(buf.at[i % n_buf], dst.at[j], out_sem.at[i % n_buf]).wait())

    total = 2 * n_seq
    for i in range(ahead):
        read(i)
    for i in range(total):
        if i + ahead < total:
            if i + ahead - n_buf >= 0:
                write_done(i + ahead - n_buf)
            read(i + ahead)
        read_done(i)
        write(i)
    for i in range(total - n_buf, total):
        write_done(i)


def solution(mesh):
    n_dev = mesh.shape['cp']
    seq_spec = P('dp', 'cp', None, None)

    def per_device(query, keys, values, grad_out, doc_id):
        n_seq, piece, n_heads, head_dim = query.shape
        n_rows = piece * n_heads
        n_key = piece * n_dev
        two = 2 * piece
        rows_shape = (n_seq, n_rows, head_dim)
        kv_shape = (n_seq, piece, head_dim)
        late_shape = (N_LATE, two, head_dim)
        main_shape = (n_seq - N_LATE, piece, head_dim)
        bf16, f32, i32 = jnp.bfloat16, jnp.float32, jnp.int32
        dma = pltpu.SemaphoreType.DMA
        any_spec = pl.BlockSpec(memory_space=pl.ANY)
        n_chip = n_dev // 2
        out = pl.pallas_call(
            functools.partial(attention_kernel, n_dev, n_heads),
            name='attention',
            out_shape=[jax.ShapeDtypeStruct(rows_shape, bf16)] * 2 + [jax.ShapeDtypeStruct(main_shape, bf16)] * 2
            + [jax.ShapeDtypeStruct(late_shape, f32)] * 3,
            in_specs=[any_spec] * 5,
            out_specs=[any_spec] * 7,
            scratch_shapes=[
                pltpu.VMEM((n_seq, 2, n_chip, 2, piece, head_dim), bf16),
                pltpu.VMEM((n_seq, two, head_dim), f32),
                pltpu.VMEM((n_seq, two, head_dim), f32),
                pltpu.VMEM((n_seq, two, head_dim), f32),
                pltpu.VMEM((NACC, n_chip, two, head_dim), f32),
                pltpu.VMEM((2, 2, n_chip, two, head_dim), f32),
                pltpu.VMEM((NPRX, n_chip, two, head_dim), f32),
                pltpu.VMEM((2, 2, n_rows, head_dim), bf16),
                pltpu.VMEM((2, 2, n_rows, head_dim), bf16),
                pltpu.VMEM((n_rows, n_key), bf16),
                pltpu.VMEM((n_rows, n_key), bf16),
                pltpu.VMEM(main_shape, bf16),
                pltpu.VMEM(main_shape, bf16),
                pltpu.VMEM(late_shape, f32),
                pltpu.VMEM((n_dev, n_seq, piece), i32),
                pltpu.VMEM((n_seq, 1, n_key), i32),
                pltpu.VMEM((n_seq, 1, piece), i32),
                pltpu.VMEM((piece, n_key), f32),
                dma((3,)), dma, dma,
                dma((4,)), dma((n_chip, n_seq)), dma, dma((n_seq,)),
                dma((2,)), dma((2,)),
                dma((2,)), dma((NPRX,)), dma((3, n_seq)), dma((NACC,)), dma, dma,
            ],
            compiler_params=pltpu.CompilerParams(collective_id=0, has_side_effects=True, vmem_limit_bytes=63 * 1024 * 1024),
        )(query.reshape(rows_shape), grad_out.reshape(rows_shape), keys.reshape(kv_shape), values.reshape(kv_shape), doc_id)
        attn_out, grad_query, grad_keys, grad_values, near, far, own = out
        attn_out, grad_query = pl.pallas_call(
            copy_kernel,
            name='results',
            out_shape=[jax.ShapeDtypeStruct(rows_shape, bf16)] * 2,
            in_specs=[any_spec] * 2,
            out_specs=[any_spec] * 2,
            scratch_shapes=[pltpu.VMEM((N_COPY, n_rows, head_dim), bf16), dma((N_COPY,)), dma((N_COPY,))],
            compiler_params=pltpu.CompilerParams(vmem_limit_bytes=48 * 1024 * 1024),
            cost_estimate=pl.CostEstimate(flops=12_000_000_000, bytes_accessed=8 * n_seq * n_rows * head_dim,
                                          transcendentals=0),
        )(attn_out, grad_query)
        to_near = [(d, d - 2) for d in range(2, n_dev)]
        to_far = [(n_dev - 2 + e, e) for e in range(2)]
        late = own + lax.ppermute(near, 'cp', to_near) + lax.ppermute(far, 'cp', to_far)
        late_keys = (late[:, 0:piece] * head_dim ** -0.5).astype(bf16)
        late_values = late[:, piece:two].astype(bf16)
        grad_keys = jnp.concatenate([grad_keys, late_keys])
        grad_values = jnp.concatenate([grad_values, late_values])
        return (attn_out.reshape(query.shape), grad_query.reshape(query.shape),
                grad_keys.reshape(keys.shape), grad_values.reshape(values.shape))

    return jax.shard_map(per_device, mesh=mesh, in_specs=(seq_spec,) * 4 + (P('dp', 'cp'),), out_specs=(seq_spec,) * 4, check_vma=False)
```

```python
import functools

import jax
import jax.numpy as jnp
from jax import lax
from jax.experimental import pallas as pl
from jax.experimental.pallas import tpu as pltpu
from jax.sharding import PartitionSpec as P

MESH = pl.DeviceIdType.MESH
LOG2E = 1.4426950408889634
HIDDEN = -3.0e38
NACC = 12
NPRX = 4
N_COPY = 16
N_FIRST = 1
N_LATE = 8


HOPS = ((2, 1, 3, 0), (1, 0, 2, None), (2, 2, 3, None), (1, 1, 0, 1), (1, 1, 2, None), (0, 0, 3, None), (0, 0, 1, None), (0, 1, 3, 1))
PUSH = {0: (1, 6), 1: (2, 12), 2: (3, 4), 3: (2, 5)}
TAKE = {0: (0, 10), 1: (3, 6), 2: (2, 2), 3: (0, 1)}
SENDS = {(3, 0): ((1, 2, 0, False, None), (0, 0, 1, False, 1), (2, 2, 1, False, 0)), (3, 1): ((2, 2, 0, False, 0), (0, 0, 0, True, 1), (1, 0, 2, False, None)), (2, 0): ((1, 1, 1, True, 0), (0, 1, 0, False, None)), (2, 1): ((1, 1, 0, False, 0), (0, 3, 0, False, None)), (1, 0): ((0, 0, 0, True, 0),), (1, 1): ((0, 0, 1, False, 0),)}
RELAY = {(3, 1): (3, 0), (2, 0): (6, 0), (1, 0): (8, 0), (0, 1): (6, 2)}
FINISH = {(3, 0): (1, ()), (3, 1): (1, ()), (2, 0): (9, (1,)), (2, 1): (5, (0,)), (1, 0): (10, (1,)), (1, 1): (10, (0, 1)), (0, 0): (10, (0, 1)), (0, 1): (9, (0, 1))}
LAG_MAX = 10
FINISH_LATE = {(1, 1): (1,)}


def attention_kernel(n_dev, n_heads, *refs):
    (q_ref, g_ref, k_ref, v_ref, doc_ref, o_ref, dq_ref, dk_ref, dv_ref, near_ref, far_ref, own_ref,
     kv, rx0, rx1, rx2, acc, part, prx, qg, odq, pb, dsb, fin_k, fin_v, own, docs, kdoc, odoc, vis,
     load_sem, doc_tx, doc_rx, kv_tx, kv_rx, kvp_tx, kvp_rx, qg_sem, odq_sem,
     part_tx, prx_sem, rx_sem, tx_sem, fwd_tx, late_sem) = refs
    rx = (rx0, rx1, rx2)
    n_seq, n_rows, head_dim = q_ref.shape
    piece = k_ref.shape[1]
    two = 2 * piece
    n_chip = n_dev // 2
    scale = head_dim ** -0.5
    me = lax.axis_index('cp')
    chip = me // 2
    core = me % 2
    partner = chip * 2 + (1 - core)

    def dev(c):
        return {'cp': c * 2 + core}

    def remote(src, dst, tx, rx, to):
        return pltpu.make_async_remote_copy(src_ref=src, dst_ref=dst, send_sem=tx, recv_sem=rx,
                                            device_id=to, device_id_type=MESH)

    def local_wait(ref, sem):
        pltpu.make_async_copy(ref, ref, sem).wait()

    barrier = pltpu.get_barrier_semaphore()
    for hop in range(1, n_dev):
        pl.semaphore_signal(barrier, inc=1, device_id={'cp': (me + hop) % n_dev}, device_id_type=MESH)

    def own_copies(lo, n, sem):
        seqs = pl.ds(lo, n)
        return (pltpu.make_async_copy(k_ref.at[seqs], kv.at[seqs, 0, chip, core], load_sem.at[sem]),
                pltpu.make_async_copy(v_ref.at[seqs], kv.at[seqs, 1, chip, core], load_sem.at[sem + 1]))

    own_d = pltpu.make_async_copy(doc_ref, docs.at[me], load_sem.at[4])
    own_first = own_copies(0, N_FIRST, 0)
    own_rest = own_copies(N_FIRST, n_seq - N_FIRST, 2)
    for copy in (*own_first, own_d, *own_rest):
        copy.start()

    def qg_start(b):
        pltpu.make_async_copy(q_ref.at[b], qg.at[b % 2, 0], qg_sem.at[b % 2]).start()
        pltpu.make_async_copy(g_ref.at[b], qg.at[b % 2, 1], qg_sem.at[b % 2]).start()

    def odq_start(b):
        pltpu.make_async_copy(odq.at[b % 2, 0], o_ref.at[b], odq_sem.at[b % 2]).start()
        pltpu.make_async_copy(odq.at[b % 2, 1], dq_ref.at[b], odq_sem.at[b % 2]).start()

    def odq_wait(b):
        local_wait(odq.at[b % 2], odq_sem.at[b % 2])

    qg_start(0)
    for copy in (*own_first, own_d):
        copy.wait()
    odoc[...] = docs[me].reshape(n_seq, 1, piece)
    pl.semaphore_wait(barrier, n_dev - 1)

    def run_chip(c):
        n_key = two * (c + 1)
        here = pl.ds(0, c + 1)
        first_late = n_seq - N_LATE

        def doc_copy(to):
            return remote(docs.at[me], docs.at[me], doc_tx, doc_rx, to)

        doc_dests = [{'cp': partner}] + [{'cp': d} for d in range(two // piece * (c + 1), n_dev)]

        flows = [hop[1:] for hop in HOPS if hop[0] == c]
        through = [src for src, _, _ in flows if src > c]

        def by_core(who, fn):
            if who is None:
                fn()
            else:
                pl.when(core == who)(fn)

        def kv_sem(src, to, b):
            return kv_rx.at[0 if to == n_chip - 1 else src, b]

        def kv_copy(i, b):
            src, to, _ = flows[i]
            blk = kv.at[b, :, src, core]
            return remote(blk, blk, kv_tx.at[i], kv_sem(src, to, b), dev(to))

        def kvp_copy(b):
            blk = kv.at[b, :, here, core]
            return remote(blk, blk, kvp_tx, kvp_rx.at[b], {'cp': partner})

        def send_on(src, b):
            for i, (s, _, who) in enumerate(flows):
                if s == src:
                    by_core(who, lambda: kv_copy(i, b).start())

        def push(b):
            send_on(c, b)

        def take(b):
            if c == n_chip - 1:
                local_wait(kv.at[b, :, pl.ds(0, c), core], kv_rx.at[0, b])
            else:
                for src in range(c - 1, -1, -1):
                    local_wait(kv.at[b, :, src, core], kv_rx.at[src, b])
                    send_on(src, b)
            kvp_copy(b).start()
            for src in through:
                who = [w for s, _, w in flows if s == src][0]

                def pass_on():
                    local_wait(kv.at[b, :, src, core], kv_rx.at[src, b])
                    for i, (s, _, _) in enumerate(flows):
                        if s == src:
                            kv_copy(i, b).start()

                by_core(who, pass_on)

        def ramp(lead, fn):
            first, most = lead
            start = min(first, most)

            def at_step(t):
                b = jnp.minimum(start + 2 * t, t + most)
                pl.when(b < n_seq)(lambda: fn(b))
                if most - start > 0:
                    pl.when(t < most - start)(lambda: fn(b + 1))

            return start, at_step

        def arrived(b):
            local_wait(kv.at[b, :, here, 1 - core], kvp_rx.at[b])

        n_push, push_at = ramp(PUSH[c], push)
        n_take, take_at = ramp(TAKE[c], take)
        for b in range(n_push):
            if b == N_FIRST:
                for copy in own_rest:
                    copy.wait()
            push(b)
        if n_push <= N_FIRST:
            for copy in own_rest:
                copy.wait()
        for to in doc_dests:
            doc_copy(to).start()
        for b in range(n_take):
            take(b)

        n_doc = 2 * c + 1
        pltpu.make_async_copy(docs.at[pl.ds(0, n_doc)], docs.at[pl.ds(0, n_doc)], doc_rx).wait()
        for p in range(2 * c + 2):
            kdoc[:, :, p * piece:(p + 1) * piece] = docs[p].reshape(n_seq, 1, piece)

        def compute(b):
            slot = b % 2
            keys = kv[b, 0, here].reshape(n_key, head_dim)
            vals = kv[b, 1, here].reshape(n_key, head_dim)
            tok = lax.broadcasted_iota(jnp.int32, (piece, piece), 0)
            tok_t = lax.broadcasted_iota(jnp.int32, (piece, piece), 1)
            own_doc = odoc[b]
            q_doc = jnp.sum(jnp.where(tok == tok_t, own_doc, 0), axis=1, keepdims=True)
            key_doc = kdoc[b, :, 0:n_key]
            q_pos = me * piece + lax.broadcasted_iota(jnp.int32, (piece, n_key), 0)
            k_pos = lax.broadcasted_iota(jnp.int32, (piece, n_key), 1)
            seen = (q_doc == key_doc) & (k_pos <= q_pos)
            vis[:, 0:n_key] = jnp.where(seen, 0.0, HIDDEN)
            nt = (((1,), (1,)), ((), ()))
            tn = (((0,), (0,)), ((), ()))
            f32 = jnp.float32
            s = lax.dot_general(qg[slot, 0], keys, nt, preferred_element_type=f32)
            dp = lax.dot_general(qg[slot, 1], vals, nt, preferred_element_type=f32)
            s = s.reshape(piece, n_heads, n_key) * (scale * LOG2E) + vis[:, 0:n_key].reshape(piece, 1, n_key)
            s = s.reshape(n_rows, n_key)
            e = jnp.exp2(s - jnp.max(s, axis=1, keepdims=True))
            p = e * (1.0 / jnp.sum(e, axis=1, keepdims=True))
            pb[:, 0:n_key] = p.astype(jnp.bfloat16)
            o16 = jnp.dot(pb[:, 0:n_key], vals, preferred_element_type=f32).astype(jnp.bfloat16)
            dv = lax.dot_general(pb[:, 0:n_key], qg[slot, 1], tn, preferred_element_type=f32)
            odq[slot, 0] = o16
            delta = jnp.sum(qg[slot, 1].astype(f32) * o16.astype(f32), axis=1, keepdims=True)
            dsb[:, 0:n_key] = (p * (dp - delta)).astype(jnp.bfloat16)
            dq = jnp.dot(dsb[:, 0:n_key], keys, preferred_element_type=f32)
            odq[slot, 1] = (dq * scale).astype(jnp.bfloat16)
            dk = lax.dot_general(dsb[:, 0:n_key], qg[slot, 0], tn, preferred_element_type=f32)
            for a in range(c + 1):
                for p in range(2):
                    rows = slice((2 * a + p) * piece, (2 * a + p + 1) * piece)
                    part[slot, p, a, 0:piece, :] = dk[rows]
                    part[slot, p, a, piece:two, :] = dv[rows]

        def part_copy(b):
            return remote(part.at[b % 2, 1 - core, here], prx.at[b % NPRX, here], part_tx.at[b % 2],
                          prx_sem.at[b % NPRX], {'cp': partner})

        def unit_send(b, e, i):
            a, to, buf, _, late = SENDS[c, e][i]
            unit = acc.at[b % NACC, a]
            sem = tx_sem.at[b % NACC]

            def now():
                remote(unit, rx[buf].at[b], sem, rx_sem.at[buf, b], dev(to)).start()

            if late is None:
                now()
            else:
                pl.when(b < first_late)(now)

                @pl.when(b >= first_late)
                def _():
                    pltpu.make_async_copy(unit, (near_ref, far_ref)[late].at[b - first_late], sem).start()

        def got(buf, b):
            local_wait(rx[buf].at[b], rx_sem.at[buf, b])

        def merge_partner(b):
            local_wait(prx.at[b % NPRX, here], prx_sem.at[b % NPRX])
            acc[b % NACC, here] = part[b % 2, core, here] + prx[b % NPRX, here]
            for e in range(2):
                sends = [i for i, s in enumerate(SENDS.get((c, e), ())) if not s[3]]
                if sends:
                    @pl.when(core == e)
                    def _():
                        for i in sends:
                            unit_send(b, e, i)

        def relay(b, e):
            buf = RELAY[c, e][1]
            got(buf, b)
            if c == 0:
                fwd_copy(b).start()
                return
            for i, (a, _, _, after, _) in enumerate(SENDS[c, e]):
                if after:
                    acc[b % NACC, a] = acc[b % NACC, a] + rx[buf][b]
                    unit_send(b, e, i)

        def fwd_copy(b):
            return remote(rx2.at[b], rx1.at[b], fwd_tx, rx_sem.at[1, b], dev(1))

        def finish(b, e):
            def total(bufs):
                out = acc[b % NACC, c]
                for buf in bufs:
                    got(buf, b)
                    out = out + rx[buf][b]
                return out

            @pl.when(b < first_late)
            def _():
                out = total(FINISH[c, e][1])
                fin_k[b] = (out[0:piece] * scale).astype(jnp.bfloat16)
                fin_v[b] = out[piece:two].astype(jnp.bfloat16)

            @pl.when(b >= first_late)
            def _():
                own[b - first_late] = total(FINISH_LATE.get((c, e), ()))

        n_step = n_seq + LAG_MAX

        def when_seq(b, fn):
            pl.when((b >= 0) & (b < n_seq))(lambda: fn(b))

        def sent(b):
            for e in range(2):
                n = len(SENDS.get((c, e), ()))
                if n:
                    pl.when(core == e)(lambda: local_wait(acc.at[b % NACC, pl.ds(0, n)], tx_sem.at[b % NACC]))

        def step(t, carry):
            @pl.when(t < n_seq)
            def _():
                push_at(t)
                take_at(t)

                @pl.when(t + 1 < n_seq)
                def _():
                    qg_start(t + 1)

                @pl.when(t >= 2)
                def _():
                    odq_wait(t - 2)
                    part_copy(t - 2).wait_send()

                pl.when(t >= NACC)(lambda: sent(t - NACC))
                arrived(t)
                local_wait(qg.at[t % 2], qg_sem.at[t % 2])
                compute(t)
                odq_start(t)
                part_copy(t).start()

            when_seq(t - 1, merge_partner)
            for e in range(2):
                @pl.when(core == e)
                def _():
                    if (c, e) in RELAY:
                        when_seq(t - RELAY[c, e][0], lambda b: relay(b, e))
                    when_seq(t - FINISH[c, e][0], lambda b: finish(b, e))
            return carry

        lax.fori_loop(0, n_step, step, 0)

        for b in (n_seq - 2, n_seq - 1):
            odq_wait(b)
            part_copy(b).wait_send()
        for b in range(n_seq - NACC, n_seq):
            sent(b)
        whole = kv.at[:, :, 0, 0]
        for i, (_, _, who) in enumerate(flows):
            by_core(who, lambda: local_wait(whole, kv_tx.at[i]))
        local_wait(kv.at[:, :, here, 0], kvp_tx)
        for to in doc_dests:
            doc_copy(to).wait_send()
        if c == 0:
            pl.when(core == 1)(lambda: local_wait(rx2, fwd_tx))

    for c in range(n_chip):
        pl.when(chip == c)(functools.partial(run_chip, c))

    out_k = pltpu.make_async_copy(fin_k, dk_ref, load_sem.at[0])
    out_v = pltpu.make_async_copy(fin_v, dv_ref, load_sem.at[1])
    out_own = pltpu.make_async_copy(own, own_ref, late_sem)
    out_k.start()
    out_v.start()
    out_own.start()
    out_k.wait()
    out_v.wait()
    out_own.wait()


def copy_kernel(a_ref, b_ref, a_out, b_out, buf, in_sem, out_sem):
    n_seq = a_ref.shape[0]
    n_buf = buf.shape[0]
    ahead = n_buf // 2

    def pick(i, fn):
        fn(a_ref, a_out, i // 2) if i % 2 == 0 else fn(b_ref, b_out, i // 2)

    def read(i):
        pick(i, lambda src, dst, j: pltpu.make_async_copy(src.at[j], buf.at[i % n_buf], in_sem.at[i % n_buf]).start())

    def read_done(i):
        pick(i, lambda src, dst, j: pltpu.make_async_copy(src.at[j], buf.at[i % n_buf], in_sem.at[i % n_buf]).wait())

    def write(i):
        pick(i, lambda src, dst, j: pltpu.make_async_copy(buf.at[i % n_buf], dst.at[j], out_sem.at[i % n_buf]).start())

    def write_done(i):
        pick(i, lambda src, dst, j: pltpu.make_async_copy(buf.at[i % n_buf], dst.at[j], out_sem.at[i % n_buf]).wait())

    total = 2 * n_seq
    for i in range(ahead):
        read(i)
    for i in range(total):
        if i + ahead < total:
            if i + ahead - n_buf >= 0:
                write_done(i + ahead - n_buf)
            read(i + ahead)
        read_done(i)
        write(i)
    for i in range(total - n_buf, total):
        write_done(i)


def solution(mesh):
    n_dev = mesh.shape['cp']
    seq_spec = P('dp', 'cp', None, None)

    def per_device(query, keys, values, grad_out, doc_id):
        n_seq, piece, n_heads, head_dim = query.shape
        n_rows = piece * n_heads
        n_key = piece * n_dev
        two = 2 * piece
        rows_shape = (n_seq, n_rows, head_dim)
        kv_shape = (n_seq, piece, head_dim)
        late_shape = (N_LATE, two, head_dim)
        main_shape = (n_seq - N_LATE, piece, head_dim)
        bf16, f32, i32 = jnp.bfloat16, jnp.float32, jnp.int32
        dma = pltpu.SemaphoreType.DMA
        any_spec = pl.BlockSpec(memory_space=pl.ANY)
        n_chip = n_dev // 2
        out = pl.pallas_call(
            functools.partial(attention_kernel, n_dev, n_heads),
            name='attention',
            out_shape=[jax.ShapeDtypeStruct(rows_shape, bf16)] * 2 + [jax.ShapeDtypeStruct(main_shape, bf16)] * 2
            + [jax.ShapeDtypeStruct(late_shape, f32)] * 3,
            in_specs=[any_spec] * 5,
            out_specs=[any_spec] * 7,
            scratch_shapes=[
                pltpu.VMEM((n_seq, 2, n_chip, 2, piece, head_dim), bf16),
                pltpu.VMEM((n_seq, two, head_dim), f32),
                pltpu.VMEM((n_seq, two, head_dim), f32),
                pltpu.VMEM((n_seq, two, head_dim), f32),
                pltpu.VMEM((NACC, n_chip, two, head_dim), f32),
                pltpu.VMEM((2, 2, n_chip, two, head_dim), f32),
                pltpu.VMEM((NPRX, n_chip, two, head_dim), f32),
                pltpu.VMEM((2, 2, n_rows, head_dim), bf16),
                pltpu.VMEM((2, 2, n_rows, head_dim), bf16),
                pltpu.VMEM((n_rows, n_key), bf16),
                pltpu.VMEM((n_rows, n_key), bf16),
                pltpu.VMEM(main_shape, bf16),
                pltpu.VMEM(main_shape, bf16),
                pltpu.VMEM(late_shape, f32),
                pltpu.VMEM((n_dev, n_seq, piece), i32),
                pltpu.VMEM((n_seq, 1, n_key), i32),
                pltpu.VMEM((n_seq, 1, piece), i32),
                pltpu.VMEM((piece, n_key), f32),
                dma((5,)), dma, dma,
                dma((4,)), dma((n_chip, n_seq)), dma, dma((n_seq,)),
                dma((2,)), dma((2,)),
                dma((2,)), dma((NPRX,)), dma((3, n_seq)), dma((NACC,)), dma, dma,
            ],
            compiler_params=pltpu.CompilerParams(collective_id=0, has_side_effects=True, vmem_limit_bytes=63 * 1024 * 1024),
        )(query.reshape(rows_shape), grad_out.reshape(rows_shape), keys.reshape(kv_shape), values.reshape(kv_shape), doc_id)
        attn_out, grad_query, grad_keys, grad_values, near, far, own = out
        attn_out, grad_query = pl.pallas_call(
            copy_kernel,
            name='results',
            out_shape=[jax.ShapeDtypeStruct(rows_shape, bf16)] * 2,
            in_specs=[any_spec] * 2,
            out_specs=[any_spec] * 2,
            scratch_shapes=[pltpu.VMEM((N_COPY, n_rows, head_dim), bf16), dma((N_COPY,)), dma((N_COPY,))],
            compiler_params=pltpu.CompilerParams(vmem_limit_bytes=48 * 1024 * 1024),
            cost_estimate=pl.CostEstimate(flops=12_000_000_000, bytes_accessed=8 * n_seq * n_rows * head_dim,
                                          transcendentals=0),
        )(attn_out, grad_query)
        to_near = [(d, d - 2) for d in range(2, n_dev)]
        to_far = [(n_dev - 2 + e, e) for e in range(2)]
        late = own + lax.ppermute(near, 'cp', to_near) + lax.ppermute(far, 'cp', to_far)
        late_keys = (late[:, 0:piece] * head_dim ** -0.5).astype(bf16)
        late_values = late[:, piece:two].astype(bf16)
        grad_keys = jnp.concatenate([grad_keys, late_keys])
        grad_values = jnp.concatenate([grad_values, late_values])
        return (attn_out.reshape(query.shape), grad_query.reshape(query.shape),
                grad_keys.reshape(keys.shape), grad_values.reshape(values.shape))

    return jax.shard_map(per_device, mesh=mesh, in_specs=(seq_spec,) * 4 + (P('dp', 'cp'),), out_specs=(seq_spec,) * 4, check_vma=False)
```

```python
import functools

import jax
import jax.numpy as jnp
from jax import lax
from jax.experimental import pallas as pl
from jax.experimental.pallas import tpu as pltpu
from jax.sharding import PartitionSpec as P

MESH = pl.DeviceIdType.MESH
LOG2E = 1.4426950408889634
HIDDEN = -3.0e38
NACC = 12
NPRX = 4
N_COPY = 16
N_FIRST = 1
N_TURN = 3
N_LATE = 8


HOPS = ((1, 1, 2, None), (1, 0, 2, None), (2, 1, 3, 0), (2, 2, 3, None), (0, 1, 3, 1), (1, 1, 0, 1), (0, 0, 3, None), (0, 0, 1, None))
PUSH = {0: (0, 8), 1: (2, 12), 2: (3, 3), 3: (2, 5)}
TAKE = {0: (0, 10), 1: (2, 6), 2: (2, 2), 3: (0, 1)}
SENDS = {(3, 0): ((1, 2, 0, False, None), (0, 0, 1, False, 1), (2, 2, 1, False, 0)), (3, 1): ((2, 2, 0, False, 0), (0, 0, 0, True, 1), (1, 0, 2, False, None)), (2, 0): ((1, 1, 1, True, 0), (0, 1, 0, False, None)), (2, 1): ((1, 1, 0, False, 0), (0, 3, 0, False, None)), (1, 0): ((0, 0, 0, True, 0),), (1, 1): ((0, 0, 1, False, 0),)}
RELAY = {(3, 1): (3, 0), (2, 0): (8, 0), (1, 0): (8, 0), (0, 1): (7, 2)}
FINISH = {(3, 0): (1, ()), (3, 1): (1, ()), (2, 0): (7, (1,)), (2, 1): (5, (0,)), (1, 0): (10, (1,)), (1, 1): (10, (0, 1)), (0, 0): (10, (0, 1)), (0, 1): (9, (0, 1))}
LAG_MAX = 10
FINISH_LATE = {(1, 1): (1,)}
TURNED, TURN, TURN_LAG = (3, 1, 1), (2, 1), 4


def attention_kernel(n_dev, n_heads, *refs):
    (q_ref, g_ref, k_ref, v_ref, doc_ref, o_ref, dq_ref, dk_ref, dv_ref, near_ref, far_ref, own_ref,
     kv, rx0, rx1, rx2, acc, part, prx, qg, odq, pb, dsb, fin_k, fin_v, own, docs, kdoc, odoc, vis,
     load_sem, doc_tx, doc_rx, kv_tx, kv_rx, kvp_tx, kvp_rx, qg_sem, odq_sem,
     part_tx, prx_sem, rx_sem, tx_sem, fwd_tx, late_sem) = refs
    rx = (rx0, rx1, rx2)
    n_seq, n_rows, head_dim = q_ref.shape
    piece = k_ref.shape[1]
    two = 2 * piece
    n_chip = n_dev // 2
    scale = head_dim ** -0.5
    me = lax.axis_index('cp')
    chip = me // 2
    core = me % 2
    partner = chip * 2 + (1 - core)

    def dev(c):
        return {'cp': c * 2 + core}

    def remote(src, dst, tx, rx, to):
        return pltpu.make_async_remote_copy(src_ref=src, dst_ref=dst, send_sem=tx, recv_sem=rx,
                                            device_id=to, device_id_type=MESH)

    def local_wait(ref, sem):
        pltpu.make_async_copy(ref, ref, sem).wait()

    barrier = pltpu.get_barrier_semaphore()
    for hop in range(1, n_dev):
        pl.semaphore_signal(barrier, inc=1, device_id={'cp': (me + hop) % n_dev}, device_id_type=MESH)

    def own_copies(lo, n, sem):
        seqs = pl.ds(lo, n)
        return (pltpu.make_async_copy(k_ref.at[seqs], kv.at[seqs, 0, chip, core], load_sem.at[sem]),
                pltpu.make_async_copy(v_ref.at[seqs], kv.at[seqs, 1, chip, core], load_sem.at[sem + 1]))

    own_d = pltpu.make_async_copy(doc_ref, docs.at[me], load_sem.at[4])
    own_first = own_copies(0, N_FIRST, 0)
    own_rest = own_copies(N_FIRST, n_seq - N_FIRST, 2)
    for copy in (*own_first, own_d, *own_rest):
        copy.start()

    def qg_start(b):
        pltpu.make_async_copy(q_ref.at[b], qg.at[b % 2, 0], qg_sem.at[b % 2]).start()
        pltpu.make_async_copy(g_ref.at[b], qg.at[b % 2, 1], qg_sem.at[b % 2]).start()

    def odq_start(b):
        pltpu.make_async_copy(odq.at[b % 2, 0], o_ref.at[b], odq_sem.at[b % 2]).start()
        pltpu.make_async_copy(odq.at[b % 2, 1], dq_ref.at[b], odq_sem.at[b % 2]).start()

    def odq_wait(b):
        local_wait(odq.at[b % 2], odq_sem.at[b % 2])

    qg_start(0)
    for copy in (*own_first, own_d):
        copy.wait()
    odoc[...] = docs[me].reshape(n_seq, 1, piece)
    pl.semaphore_wait(barrier, n_dev - 1)

    def run_chip(c):
        n_key = two * (c + 1)
        here = pl.ds(0, c + 1)
        first_late = n_seq - N_LATE
        first_turn = n_seq - N_TURN

        def doc_copy(to):
            return remote(docs.at[me], docs.at[me], doc_tx, doc_rx, to)

        doc_dests = [{'cp': partner}] + [{'cp': d} for d in range(two // piece * (c + 1), n_dev)]

        flows = [hop[1:] for hop in HOPS if hop[0] == c]
        through = [src for src, _, _ in flows if src > c]

        def by_core(who, fn):
            if who is None:
                fn()
            else:
                pl.when(core == who)(fn)

        def kv_sem(src, to, b):
            return kv_rx.at[0 if to == n_chip - 1 else src, b]

        def kv_copy(i, b):
            src, to, _ = flows[i]
            blk = kv.at[b, :, src, core]
            return remote(blk, blk, kv_tx.at[i], kv_sem(src, to, b), dev(to))

        def kvp_copy(b):
            blk = kv.at[b, :, here, core]
            return remote(blk, blk, kvp_tx, kvp_rx.at[b], {'cp': partner})

        def send_on(src, b):
            for i, (s, _, who) in enumerate(flows):
                if s == src:
                    by_core(who, lambda: kv_copy(i, b).start())

        def push(b):
            send_on(c, b)

        def take(b):
            if c == n_chip - 1:
                local_wait(kv.at[b, :, pl.ds(0, c), core], kv_rx.at[0, b])
            else:
                for src in range(c - 1, -1, -1):
                    local_wait(kv.at[b, :, src, core], kv_rx.at[src, b])
                    send_on(src, b)
            kvp_copy(b).start()
            for src in through:
                who = [w for s, _, w in flows if s == src][0]

                def pass_on():
                    local_wait(kv.at[b, :, src, core], kv_rx.at[src, b])
                    for i, (s, _, _) in enumerate(flows):
                        if s == src:
                            kv_copy(i, b).start()

                by_core(who, pass_on)

        def ramp(lead, fn):
            first, most = lead
            start = min(first, most)

            def at_step(t):
                b = jnp.minimum(start + 2 * t, t + most)
                pl.when(b < n_seq)(lambda: fn(b))
                if most - start > 0:
                    pl.when(t < most - start)(lambda: fn(b + 1))

            return start, at_step

        def arrived(b):
            local_wait(kv.at[b, :, here, 1 - core], kvp_rx.at[b])

        n_push, push_at = ramp(PUSH[c], push)
        n_take, take_at = ramp(TAKE[c], take)
        for b in range(n_push):
            if b == N_FIRST:
                for copy in own_rest:
                    copy.wait()
            push(b)
        if n_push <= N_FIRST:
            for copy in own_rest:
                copy.wait()
        for to in doc_dests:
            doc_copy(to).start()
        for b in range(n_take):
            take(b)

        n_doc = 2 * c + 1
        pltpu.make_async_copy(docs.at[pl.ds(0, n_doc)], docs.at[pl.ds(0, n_doc)], doc_rx).wait()
        for p in range(2 * c + 2):
            kdoc[:, :, p * piece:(p + 1) * piece] = docs[p].reshape(n_seq, 1, piece)

        def compute(b):
            slot = b % 2
            keys = kv[b, 0, here].reshape(n_key, head_dim)
            vals = kv[b, 1, here].reshape(n_key, head_dim)
            tok = lax.broadcasted_iota(jnp.int32, (piece, piece), 0)
            tok_t = lax.broadcasted_iota(jnp.int32, (piece, piece), 1)
            own_doc = odoc[b]
            q_doc = jnp.sum(jnp.where(tok == tok_t, own_doc, 0), axis=1, keepdims=True)
            key_doc = kdoc[b, :, 0:n_key]
            q_pos = me * piece + lax.broadcasted_iota(jnp.int32, (piece, n_key), 0)
            k_pos = lax.broadcasted_iota(jnp.int32, (piece, n_key), 1)
            seen = (q_doc == key_doc) & (k_pos <= q_pos)
            vis[:, 0:n_key] = jnp.where(seen, 0.0, HIDDEN)
            nt = (((1,), (1,)), ((), ()))
            tn = (((0,), (0,)), ((), ()))
            f32 = jnp.float32
            s = lax.dot_general(qg[slot, 0], keys, nt, preferred_element_type=f32)
            dp = lax.dot_general(qg[slot, 1], vals, nt, preferred_element_type=f32)
            s = s.reshape(piece, n_heads, n_key) * (scale * LOG2E) + vis[:, 0:n_key].reshape(piece, 1, n_key)
            s = s.reshape(n_rows, n_key)
            e = jnp.exp2(s - jnp.max(s, axis=1, keepdims=True))
            p = e * (1.0 / jnp.sum(e, axis=1, keepdims=True))
            pb[:, 0:n_key] = p.astype(jnp.bfloat16)
            o16 = jnp.dot(pb[:, 0:n_key], vals, preferred_element_type=f32).astype(jnp.bfloat16)
            dv = lax.dot_general(pb[:, 0:n_key], qg[slot, 1], tn, preferred_element_type=f32)
            odq[slot, 0] = o16
            delta = jnp.sum(qg[slot, 1].astype(f32) * o16.astype(f32), axis=1, keepdims=True)
            dsb[:, 0:n_key] = (p * (dp - delta)).astype(jnp.bfloat16)
            dq = jnp.dot(dsb[:, 0:n_key], keys, preferred_element_type=f32)
            odq[slot, 1] = (dq * scale).astype(jnp.bfloat16)
            dk = lax.dot_general(dsb[:, 0:n_key], qg[slot, 0], tn, preferred_element_type=f32)
            for a in range(c + 1):
                for p in range(2):
                    rows = slice((2 * a + p) * piece, (2 * a + p + 1) * piece)
                    part[slot, p, a, 0:piece, :] = dk[rows]
                    part[slot, p, a, piece:two, :] = dv[rows]

        def part_copy(b):
            return remote(part.at[b % 2, 1 - core, here], prx.at[b % NPRX, here], part_tx.at[b % 2],
                          prx_sem.at[b % NPRX], {'cp': partner})

        def unit_send(b, e, i):
            a, to, buf, _, late = SENDS[c, e][i]
            unit = acc.at[b % NACC, a]
            sem = tx_sem.at[b % NACC]

            def now(to=to, buf=buf):
                remote(unit, rx[buf].at[b], sem, rx_sem.at[buf, b], dev(to)).start()

            if (c, e, a) == TURNED:
                pl.when(b < first_turn)(now)
                pl.when(b >= first_turn)(lambda: now(*TURN))
            elif late is None:
                now()
            else:
                pl.when(b < first_late)(now)

                @pl.when(b >= first_late)
                def _():
                    pltpu.make_async_copy(unit, (near_ref, far_ref)[late].at[b - first_late], sem).start()

        def got(buf, b):
            local_wait(rx[buf].at[b], rx_sem.at[buf, b])

        def merge_partner(b):
            local_wait(prx.at[b % NPRX, here], prx_sem.at[b % NPRX])
            acc[b % NACC, here] = part[b % 2, core, here] + prx[b % NPRX, here]
            for e in range(2):
                sends = [i for i, s in enumerate(SENDS.get((c, e), ())) if not s[3]]
                if sends:
                    @pl.when(core == e)
                    def _():
                        for i in sends:
                            if (c, e, SENDS[c, e][i][0]) == (TURN[0], TURNED[1], TURNED[2]):
                                pl.when(b < first_turn)(lambda: unit_send(b, e, i))
                            else:
                                unit_send(b, e, i)

        def relay(b, e):
            buf = RELAY[c, e][1]

            def take_in():
                got(buf, b)
                if c == 0:
                    fwd_copy(b).start()
                    return
                for i, (a, _, _, after, _) in enumerate(SENDS[c, e]):
                    if after:
                        acc[b % NACC, a] = acc[b % NACC, a] + rx[buf][b]
                        unit_send(b, e, i)

            if c == 0:
                pl.when(b < first_turn)(take_in)
            else:
                take_in()

        def add_turned(b):
            got(TURN[1], b)
            a = TURNED[2]
            acc[b % NACC, a] = acc[b % NACC, a] + rx[TURN[1]][b]
            unit_send(b, TURNED[1], [s[0] for s in SENDS[c, TURNED[1]]].index(a))

        def fwd_copy(b):
            return remote(rx2.at[b], rx1.at[b], fwd_tx, rx_sem.at[1, b], dev(1))

        def finish(b, e):
            def total(bufs):
                out = acc[b % NACC, c]
                for buf in bufs:
                    got(buf, b)
                    out = out + rx[buf][b]
                return out

            @pl.when(b < first_late)
            def _():
                out = total(FINISH[c, e][1])
                fin_k[b] = (out[0:piece] * scale).astype(jnp.bfloat16)
                fin_v[b] = out[piece:two].astype(jnp.bfloat16)

            @pl.when((b >= first_late) & (b < first_turn))
            def _():
                own[b - first_late] = total(FINISH_LATE.get((c, e), ()))

            @pl.when(b >= first_turn)
            def _():
                own[b - first_late] = total(())

        n_step = n_seq + LAG_MAX

        def when_seq(b, fn):
            pl.when((b >= 0) & (b < n_seq))(lambda: fn(b))

        def sent(b):
            for e in range(2):
                n = len(SENDS.get((c, e), ()))
                if n:
                    pl.when(core == e)(lambda: local_wait(acc.at[b % NACC, pl.ds(0, n)], tx_sem.at[b % NACC]))

        def step(t, carry):
            @pl.when(t < n_seq)
            def _():
                push_at(t)
                take_at(t)

                @pl.when(t + 1 < n_seq)
                def _():
                    qg_start(t + 1)

                @pl.when(t >= 2)
                def _():
                    odq_wait(t - 2)
                    part_copy(t - 2).wait_send()

                pl.when(t >= NACC)(lambda: sent(t - NACC))
                arrived(t)
                local_wait(qg.at[t % 2], qg_sem.at[t % 2])
                compute(t)
                odq_start(t)
                part_copy(t).start()

            when_seq(t - 1, merge_partner)
            for e in range(2):
                @pl.when(core == e)
                def _():
                    if (c, e) in RELAY:
                        when_seq(t - RELAY[c, e][0], lambda b: relay(b, e))
                    if (c, e) == (TURN[0], TURNED[1]):
                        b_turn = t - TURN_LAG
                        pl.when((b_turn >= first_turn) & (b_turn < n_seq))(lambda: add_turned(b_turn))
                    when_seq(t - FINISH[c, e][0], lambda b: finish(b, e))
            return carry

        lax.fori_loop(0, n_step, step, 0)

        for b in (n_seq - 2, n_seq - 1):
            odq_wait(b)
            part_copy(b).wait_send()
        for b in range(n_seq - NACC, n_seq):
            sent(b)
        whole = kv.at[:, :, 0, 0]
        for i, (_, _, who) in enumerate(flows):
            by_core(who, lambda: local_wait(whole, kv_tx.at[i]))
        local_wait(kv.at[:, :, here, 0], kvp_tx)
        for to in doc_dests:
            doc_copy(to).wait_send()
        if c == 0:
            pl.when(core == 1)(lambda: local_wait(rx2.at[pl.ds(0, first_turn)], fwd_tx))

    for c in range(n_chip):
        pl.when(chip == c)(functools.partial(run_chip, c))

    out_k = pltpu.make_async_copy(fin_k, dk_ref, load_sem.at[0])
    out_v = pltpu.make_async_copy(fin_v, dv_ref, load_sem.at[1])
    out_own = pltpu.make_async_copy(own, own_ref, late_sem)
    out_k.start()
    out_v.start()
    out_own.start()
    out_k.wait()
    out_v.wait()
    out_own.wait()


def copy_kernel(a_ref, b_ref, a_out, b_out, buf, in_sem, out_sem):
    n_seq = a_ref.shape[0]
    n_buf = buf.shape[0]
    ahead = n_buf // 2

    def pick(i, fn):
        fn(a_ref, a_out, i // 2) if i % 2 == 0 else fn(b_ref, b_out, i // 2)

    def read(i):
        pick(i, lambda src, dst, j: pltpu.make_async_copy(src.at[j], buf.at[i % n_buf], in_sem.at[i % n_buf]).start())

    def read_done(i):
        pick(i, lambda src, dst, j: pltpu.make_async_copy(src.at[j], buf.at[i % n_buf], in_sem.at[i % n_buf]).wait())

    def write(i):
        pick(i, lambda src, dst, j: pltpu.make_async_copy(buf.at[i % n_buf], dst.at[j], out_sem.at[i % n_buf]).start())

    def write_done(i):
        pick(i, lambda src, dst, j: pltpu.make_async_copy(buf.at[i % n_buf], dst.at[j], out_sem.at[i % n_buf]).wait())

    total = 2 * n_seq
    for i in range(ahead):
        read(i)
    for i in range(total):
        if i + ahead < total:
            if i + ahead - n_buf >= 0:
                write_done(i + ahead - n_buf)
            read(i + ahead)
        read_done(i)
        write(i)
    for i in range(total - n_buf, total):
        write_done(i)


def solution(mesh):
    n_dev = mesh.shape['cp']
    seq_spec = P('dp', 'cp', None, None)

    def per_device(query, keys, values, grad_out, doc_id):
        n_seq, piece, n_heads, head_dim = query.shape
        n_rows = piece * n_heads
        n_key = piece * n_dev
        two = 2 * piece
        rows_shape = (n_seq, n_rows, head_dim)
        kv_shape = (n_seq, piece, head_dim)
        late_shape = (N_LATE, two, head_dim)
        main_shape = (n_seq - N_LATE, piece, head_dim)
        bf16, f32, i32 = jnp.bfloat16, jnp.float32, jnp.int32
        dma = pltpu.SemaphoreType.DMA
        any_spec = pl.BlockSpec(memory_space=pl.ANY)
        n_chip = n_dev // 2
        out = pl.pallas_call(
            functools.partial(attention_kernel, n_dev, n_heads),
            name='attention',
            out_shape=[jax.ShapeDtypeStruct(rows_shape, bf16)] * 2 + [jax.ShapeDtypeStruct(main_shape, bf16)] * 2
            + [jax.ShapeDtypeStruct(late_shape, f32)] * 3,
            in_specs=[any_spec] * 5,
            out_specs=[any_spec] * 7,
            scratch_shapes=[
                pltpu.VMEM((n_seq, 2, n_chip, 2, piece, head_dim), bf16),
                pltpu.VMEM((n_seq, two, head_dim), f32),
                pltpu.VMEM((n_seq, two, head_dim), f32),
                pltpu.VMEM((n_seq, two, head_dim), f32),
                pltpu.VMEM((NACC, n_chip, two, head_dim), f32),
                pltpu.VMEM((2, 2, n_chip, two, head_dim), f32),
                pltpu.VMEM((NPRX, n_chip, two, head_dim), f32),
                pltpu.VMEM((2, 2, n_rows, head_dim), bf16),
                pltpu.VMEM((2, 2, n_rows, head_dim), bf16),
                pltpu.VMEM((n_rows, n_key), bf16),
                pltpu.VMEM((n_rows, n_key), bf16),
                pltpu.VMEM(main_shape, bf16),
                pltpu.VMEM(main_shape, bf16),
                pltpu.VMEM(late_shape, f32),
                pltpu.VMEM((n_dev, n_seq, piece), i32),
                pltpu.VMEM((n_seq, 1, n_key), i32),
                pltpu.VMEM((n_seq, 1, piece), i32),
                pltpu.VMEM((piece, n_key), f32),
                dma((5,)), dma, dma,
                dma((4,)), dma((n_chip, n_seq)), dma, dma((n_seq,)),
                dma((2,)), dma((2,)),
                dma((2,)), dma((NPRX,)), dma((3, n_seq)), dma((NACC,)), dma, dma,
            ],
            compiler_params=pltpu.CompilerParams(collective_id=0, has_side_effects=True, vmem_limit_bytes=63 * 1024 * 1024),
        )(query.reshape(rows_shape), grad_out.reshape(rows_shape), keys.reshape(kv_shape), values.reshape(kv_shape), doc_id)
        attn_out, grad_query, grad_keys, grad_values, near, far, own = out
        attn_out, grad_query = pl.pallas_call(
            copy_kernel,
            name='results',
            out_shape=[jax.ShapeDtypeStruct(rows_shape, bf16)] * 2,
            in_specs=[any_spec] * 2,
            out_specs=[any_spec] * 2,
            scratch_shapes=[pltpu.VMEM((N_COPY, n_rows, head_dim), bf16), dma((N_COPY,)), dma((N_COPY,))],
            compiler_params=pltpu.CompilerParams(vmem_limit_bytes=48 * 1024 * 1024),
            cost_estimate=pl.CostEstimate(flops=12_000_000_000, bytes_accessed=8 * n_seq * n_rows * head_dim,
                                          transcendentals=0),
        )(attn_out, grad_query)
        to_near = [(d, d - 2) for d in range(2, n_dev)]
        to_far = [(n_dev - 2 + e, e) for e in range(2)]
        late = own + lax.ppermute(near, 'cp', to_near) + lax.ppermute(far, 'cp', to_far)
        late_keys = (late[:, 0:piece] * head_dim ** -0.5).astype(bf16)
        late_values = late[:, piece:two].astype(bf16)
        grad_keys = jnp.concatenate([grad_keys, late_keys])
        grad_values = jnp.concatenate([grad_values, late_values])
        return (attn_out.reshape(query.shape), grad_query.reshape(query.shape),
                grad_keys.reshape(keys.shape), grad_values.reshape(values.shape))

    return jax.shard_map(per_device, mesh=mesh, in_specs=(seq_spec,) * 4 + (P('dp', 'cp'),), out_specs=(seq_spec,) * 4, check_vma=False)
```

```python
import functools

import jax
import jax.numpy as jnp
from jax import lax
from jax.experimental import pallas as pl
from jax.experimental.pallas import tpu as pltpu
from jax.sharding import PartitionSpec as P

MESH = pl.DeviceIdType.MESH
LOG2E = 1.4426950408889634
HIDDEN = -3.0e38
NACC = 12
NPRX = 4
COPY_BLOCK = 2
N_COPY = 32
N_FIRST = 1
N_TURN = 3
N_LATE = 8


HOPS = ((1, 1, 2, None), (1, 0, 2, None), (2, 1, 3, 0), (2, 2, 3, None), (0, 1, 3, 1), (1, 1, 0, 1), (0, 0, 3, None), (0, 0, 1, None))
PUSH = {0: (0, 8), 1: (2, 12), 2: (3, 3), 3: (2, 5)}
TAKE = {0: (0, 10), 1: (2, 6), 2: (2, 2), 3: (0, 1)}
SENDS = {(3, 0): ((1, 2, 0, False, None), (0, 0, 1, False, 1), (2, 2, 1, False, 0)), (3, 1): ((2, 2, 0, False, 0), (0, 0, 0, True, 1), (1, 0, 2, False, None)), (2, 0): ((1, 1, 1, True, 0), (0, 1, 0, False, None)), (2, 1): ((1, 1, 0, False, 0), (0, 3, 0, False, None)), (1, 0): ((0, 0, 0, True, 0),), (1, 1): ((0, 0, 1, False, 0),)}
RELAY = {(3, 1): (3, 0), (2, 0): (8, 0), (1, 0): (8, 0), (0, 1): (7, 2)}
FINISH = {(3, 0): (1, ()), (3, 1): (1, ()), (2, 0): (7, (1,)), (2, 1): (5, (0,)), (1, 0): (10, (1,)), (1, 1): (10, (0, 1)), (0, 0): (10, (0, 1)), (0, 1): (9, (0, 1))}
LAG_MAX = 10
FINISH_LATE = {(1, 1): (1,)}
TURNED, TURN, TURN_LAG = (3, 1, 1), (2, 1), 4


def attention_kernel(n_dev, n_heads, *refs):
    (q_ref, g_ref, k_ref, v_ref, doc_ref, o_ref, dq_ref, dk_ref, dv_ref, near_ref, far_ref, own_ref,
     kv, rx0, rx1, rx2, acc, part, prx, qg, odq, pb, dsb, fin_k, fin_v, own, docs, kdoc, odoc, vis,
     load_sem, doc_tx, doc_rx, kv_tx, kv_rx, kvp_tx, kvp_rx, qg_sem, odq_sem,
     part_tx, prx_sem, rx_sem, tx_sem, fwd_tx, late_sem) = refs
    rx = (rx0, rx1, rx2)
    n_seq, n_rows, head_dim = q_ref.shape
    piece = k_ref.shape[1]
    two = 2 * piece
    n_chip = n_dev // 2
    scale = head_dim ** -0.5
    me = lax.axis_index('cp')
    chip = me // 2
    core = me % 2
    partner = chip * 2 + (1 - core)

    def dev(c):
        return {'cp': c * 2 + core}

    def remote(src, dst, tx, rx, to):
        return pltpu.make_async_remote_copy(src_ref=src, dst_ref=dst, send_sem=tx, recv_sem=rx,
                                            device_id=to, device_id_type=MESH)

    def local_wait(ref, sem):
        pltpu.make_async_copy(ref, ref, sem).wait()

    barrier = pltpu.get_barrier_semaphore()
    for hop in range(1, n_dev):
        pl.semaphore_signal(barrier, inc=1, device_id={'cp': (me + hop) % n_dev}, device_id_type=MESH)

    def own_copies(lo, n, sem):
        seqs = pl.ds(lo, n)
        return (pltpu.make_async_copy(k_ref.at[seqs], kv.at[seqs, 0, chip, core], load_sem.at[sem]),
                pltpu.make_async_copy(v_ref.at[seqs], kv.at[seqs, 1, chip, core], load_sem.at[sem + 1]))

    own_d = pltpu.make_async_copy(doc_ref, docs.at[me], load_sem.at[4])
    own_first = own_copies(0, N_FIRST, 0)
    own_rest = own_copies(N_FIRST, n_seq - N_FIRST, 2)
    for copy in (*own_first, own_d, *own_rest):
        copy.start()

    def qg_start(b):
        pltpu.make_async_copy(q_ref.at[b], qg.at[b % 2, 0], qg_sem.at[b % 2]).start()
        pltpu.make_async_copy(g_ref.at[b], qg.at[b % 2, 1], qg_sem.at[b % 2]).start()

    def odq_start(b):
        pltpu.make_async_copy(odq.at[b % 2, 0], o_ref.at[b], odq_sem.at[b % 2]).start()
        pltpu.make_async_copy(odq.at[b % 2, 1], dq_ref.at[b], odq_sem.at[b % 2]).start()

    def odq_wait(b):
        local_wait(odq.at[b % 2], odq_sem.at[b % 2])

    qg_start(0)
    for copy in (*own_first, own_d):
        copy.wait()
    odoc[...] = docs[me].reshape(n_seq, 1, piece)
    pl.semaphore_wait(barrier, n_dev - 1)

    def run_chip(c):
        n_key = two * (c + 1)
        here = pl.ds(0, c + 1)
        first_late = n_seq - N_LATE
        first_turn = n_seq - N_TURN

        def doc_copy(to):
            return remote(docs.at[me], docs.at[me], doc_tx, doc_rx, to)

        doc_dests = [{'cp': partner}] + [{'cp': d} for d in range(two // piece * (c + 1), n_dev)]

        flows = [hop[1:] for hop in HOPS if hop[0] == c]
        through = [src for src, _, _ in flows if src > c]

        def by_core(who, fn):
            if who is None:
                fn()
            else:
                pl.when(core == who)(fn)

        def kv_sem(src, to, b):
            return kv_rx.at[0 if to == n_chip - 1 else src, b]

        def kv_copy(i, b):
            src, to, _ = flows[i]
            blk = kv.at[b, :, src, core]
            return remote(blk, blk, kv_tx.at[i], kv_sem(src, to, b), dev(to))

        def kvp_copy(b):
            blk = kv.at[b, :, here, core]
            return remote(blk, blk, kvp_tx, kvp_rx.at[b], {'cp': partner})

        def send_on(src, b):
            for i, (s, _, who) in enumerate(flows):
                if s == src:
                    by_core(who, lambda: kv_copy(i, b).start())

        def push(b):
            send_on(c, b)

        def take(b):
            if c == n_chip - 1:
                local_wait(kv.at[b, :, pl.ds(0, c), core], kv_rx.at[0, b])
            else:
                for src in range(c - 1, -1, -1):
                    local_wait(kv.at[b, :, src, core], kv_rx.at[src, b])
                    send_on(src, b)
            kvp_copy(b).start()
            for src in through:
                who = [w for s, _, w in flows if s == src][0]

                def pass_on():
                    local_wait(kv.at[b, :, src, core], kv_rx.at[src, b])
                    for i, (s, _, _) in enumerate(flows):
                        if s == src:
                            kv_copy(i, b).start()

                by_core(who, pass_on)

        def ramp(lead, fn):
            first, most = lead
            start = min(first, most)

            def at_step(t):
                b = jnp.minimum(start + 2 * t, t + most)
                pl.when(b < n_seq)(lambda: fn(b))
                if most - start > 0:
                    pl.when(t < most - start)(lambda: fn(b + 1))

            return start, at_step

        def arrived(b):
            local_wait(kv.at[b, :, here, 1 - core], kvp_rx.at[b])

        n_push, push_at = ramp(PUSH[c], push)
        n_take, take_at = ramp(TAKE[c], take)
        for b in range(n_push):
            if b == N_FIRST:
                for copy in own_rest:
                    copy.wait()
            push(b)
        if n_push <= N_FIRST:
            for copy in own_rest:
                copy.wait()
        for to in doc_dests:
            doc_copy(to).start()
        for b in range(n_take):
            take(b)

        n_doc = 2 * c + 1
        pltpu.make_async_copy(docs.at[pl.ds(0, n_doc)], docs.at[pl.ds(0, n_doc)], doc_rx).wait()
        for p in range(2 * c + 2):
            kdoc[:, :, p * piece:(p + 1) * piece] = docs[p].reshape(n_seq, 1, piece)

        def compute(b):
            slot = b % 2
            keys = kv[b, 0, here].reshape(n_key, head_dim)
            vals = kv[b, 1, here].reshape(n_key, head_dim)
            tok = lax.broadcasted_iota(jnp.int32, (piece, piece), 0)
            tok_t = lax.broadcasted_iota(jnp.int32, (piece, piece), 1)
            own_doc = odoc[b]
            q_doc = jnp.sum(jnp.where(tok == tok_t, own_doc, 0), axis=1, keepdims=True)
            key_doc = kdoc[b, :, 0:n_key]
            q_pos = me * piece + lax.broadcasted_iota(jnp.int32, (piece, n_key), 0)
            k_pos = lax.broadcasted_iota(jnp.int32, (piece, n_key), 1)
            seen = (q_doc == key_doc) & (k_pos <= q_pos)
            vis[:, 0:n_key] = jnp.where(seen, 0.0, HIDDEN)
            nt = (((1,), (1,)), ((), ()))
            tn = (((0,), (0,)), ((), ()))
            f32 = jnp.float32
            s = lax.dot_general(qg[slot, 0], keys, nt, preferred_element_type=f32)
            dp = lax.dot_general(qg[slot, 1], vals, nt, preferred_element_type=f32)
            s = s.reshape(piece, n_heads, n_key) * (scale * LOG2E) + vis[:, 0:n_key].reshape(piece, 1, n_key)
            s = s.reshape(n_rows, n_key)
            e = jnp.exp2(s - jnp.max(s, axis=1, keepdims=True))
            p = e * (1.0 / jnp.sum(e, axis=1, keepdims=True))
            pb[:, 0:n_key] = p.astype(jnp.bfloat16)
            o16 = jnp.dot(pb[:, 0:n_key], vals, preferred_element_type=f32).astype(jnp.bfloat16)
            dv = lax.dot_general(pb[:, 0:n_key], qg[slot, 1], tn, preferred_element_type=f32)
            odq[slot, 0] = o16
            delta = jnp.sum(qg[slot, 1].astype(f32) * o16.astype(f32), axis=1, keepdims=True)
            dsb[:, 0:n_key] = (p * (dp - delta)).astype(jnp.bfloat16)
            dq = jnp.dot(dsb[:, 0:n_key], keys, preferred_element_type=f32)
            odq[slot, 1] = (dq * scale).astype(jnp.bfloat16)
            dk = lax.dot_general(dsb[:, 0:n_key], qg[slot, 0], tn, preferred_element_type=f32)
            for a in range(c + 1):
                for p in range(2):
                    rows = slice((2 * a + p) * piece, (2 * a + p + 1) * piece)
                    part[slot, p, a, 0:piece, :] = dk[rows]
                    part[slot, p, a, piece:two, :] = dv[rows]

        def part_copy(b):
            return remote(part.at[b % 2, 1 - core, here], prx.at[b % NPRX, here], part_tx.at[b % 2],
                          prx_sem.at[b % NPRX], {'cp': partner})

        def unit_send(b, e, i):
            a, to, buf, _, late = SENDS[c, e][i]
            unit = acc.at[b % NACC, a]
            sem = tx_sem.at[b % NACC]

            def now(to=to, buf=buf):
                remote(unit, rx[buf].at[b], sem, rx_sem.at[buf, b], dev(to)).start()

            if (c, e, a) == TURNED:
                pl.when(b < first_turn)(now)
                pl.when(b >= first_turn)(lambda: now(*TURN))
            elif late is None:
                now()
            else:
                pl.when(b < first_late)(now)

                @pl.when(b >= first_late)
                def _():
                    pltpu.make_async_copy(unit, (near_ref, far_ref)[late].at[b - first_late], sem).start()

        def got(buf, b):
            local_wait(rx[buf].at[b], rx_sem.at[buf, b])

        def merge_partner(b):
            local_wait(prx.at[b % NPRX, here], prx_sem.at[b % NPRX])
            acc[b % NACC, here] = part[b % 2, core, here] + prx[b % NPRX, here]
            for e in range(2):
                sends = [i for i, s in enumerate(SENDS.get((c, e), ())) if not s[3]]
                if sends:
                    @pl.when(core == e)
                    def _():
                        for i in sends:
                            if (c, e, SENDS[c, e][i][0]) == (TURN[0], TURNED[1], TURNED[2]):
                                pl.when(b < first_turn)(lambda: unit_send(b, e, i))
                            else:
                                unit_send(b, e, i)

        def relay(b, e):
            buf = RELAY[c, e][1]

            def take_in():
                got(buf, b)
                if c == 0:
                    fwd_copy(b).start()
                    return
                for i, (a, _, _, after, _) in enumerate(SENDS[c, e]):
                    if after:
                        acc[b % NACC, a] = acc[b % NACC, a] + rx[buf][b]
                        unit_send(b, e, i)

            if c == 0:
                pl.when(b < first_turn)(take_in)
            else:
                take_in()

        def add_turned(b):
            got(TURN[1], b)
            a = TURNED[2]
            acc[b % NACC, a] = acc[b % NACC, a] + rx[TURN[1]][b]
            unit_send(b, TURNED[1], [s[0] for s in SENDS[c, TURNED[1]]].index(a))

        def fwd_copy(b):
            return remote(rx2.at[b], rx1.at[b], fwd_tx, rx_sem.at[1, b], dev(1))

        def finish(b, e):
            def total(bufs):
                out = acc[b % NACC, c]
                for buf in bufs:
                    got(buf, b)
                    out = out + rx[buf][b]
                return out

            @pl.when(b < first_late)
            def _():
                out = total(FINISH[c, e][1])
                fin_k[b] = (out[0:piece] * scale).astype(jnp.bfloat16)
                fin_v[b] = out[piece:two].astype(jnp.bfloat16)

            @pl.when((b >= first_late) & (b < first_turn))
            def _():
                own[b - first_late] = total(FINISH_LATE.get((c, e), ()))

            @pl.when(b >= first_turn)
            def _():
                own[b - first_late] = total(())

        n_step = n_seq + LAG_MAX

        def when_seq(b, fn):
            pl.when((b >= 0) & (b < n_seq))(lambda: fn(b))

        def sent(b):
            for e in range(2):
                n = len(SENDS.get((c, e), ()))
                if n:
                    pl.when(core == e)(lambda: local_wait(acc.at[b % NACC, pl.ds(0, n)], tx_sem.at[b % NACC]))

        def step(t, carry):
            @pl.when(t < n_seq)
            def _():
                push_at(t)
                take_at(t)

                @pl.when(t + 1 < n_seq)
                def _():
                    qg_start(t + 1)

                @pl.when(t >= 2)
                def _():
                    odq_wait(t - 2)
                    part_copy(t - 2).wait_send()

                pl.when(t >= NACC)(lambda: sent(t - NACC))
                arrived(t)
                local_wait(qg.at[t % 2], qg_sem.at[t % 2])
                compute(t)
                odq_start(t)
                part_copy(t).start()

            when_seq(t - 1, merge_partner)
            for e in range(2):
                @pl.when(core == e)
                def _():
                    if (c, e) in RELAY:
                        when_seq(t - RELAY[c, e][0], lambda b: relay(b, e))
                    if (c, e) == (TURN[0], TURNED[1]):
                        b_turn = t - TURN_LAG
                        pl.when((b_turn >= first_turn) & (b_turn < n_seq))(lambda: add_turned(b_turn))
                    when_seq(t - FINISH[c, e][0], lambda b: finish(b, e))
            return carry

        lax.fori_loop(0, n_step, step, 0)

        for b in (n_seq - 2, n_seq - 1):
            odq_wait(b)
            part_copy(b).wait_send()
        for b in range(n_seq - NACC, n_seq):
            sent(b)
        whole = kv.at[:, :, 0, 0]
        for i, (_, _, who) in enumerate(flows):
            by_core(who, lambda: local_wait(whole, kv_tx.at[i]))
        local_wait(kv.at[:, :, here, 0], kvp_tx)
        for to in doc_dests:
            doc_copy(to).wait_send()
        if c == 0:
            pl.when(core == 1)(lambda: local_wait(rx2.at[pl.ds(0, first_turn)], fwd_tx))

    for c in range(n_chip):
        pl.when(chip == c)(functools.partial(run_chip, c))

    out_k = pltpu.make_async_copy(fin_k, dk_ref, load_sem.at[0])
    out_v = pltpu.make_async_copy(fin_v, dv_ref, load_sem.at[1])
    out_own = pltpu.make_async_copy(own, own_ref, late_sem)
    out_k.start()
    out_v.start()
    out_own.start()
    out_k.wait()
    out_v.wait()
    out_own.wait()


def copy_kernel(a_ref, b_ref, a_out, b_out, buf, in_sem, out_sem):
    n_buf, n_block = buf.shape[:2]
    total = 2 * a_ref.shape[0] // n_block
    ahead = n_buf // 2

    def read(i):
        src = (a_ref, b_ref)[i % 2].at[pl.ds(i // 2 * n_block, n_block)]
        return pltpu.make_async_copy(src, buf.at[i % n_buf], in_sem.at[i % n_buf])

    def write(i):
        dst = (a_out, b_out)[i % 2].at[pl.ds(i // 2 * n_block, n_block)]
        return pltpu.make_async_copy(buf.at[i % n_buf], dst, out_sem.at[i % n_buf])

    for i in range(ahead):
        read(i).start()
    for i in range(total):
        if i + ahead < total:
            if i + ahead >= n_buf:
                write(i + ahead - n_buf).wait()
            read(i + ahead).start()
        read(i).wait()
        write(i).start()
    for i in range(max(total - n_buf, 0), total):
        write(i).wait()


def solution(mesh):
    n_dev = mesh.shape['cp']
    seq_spec = P('dp', 'cp', None, None)

    def per_device(query, keys, values, grad_out, doc_id):
        n_seq, piece, n_heads, head_dim = query.shape
        n_rows = piece * n_heads
        n_key = piece * n_dev
        two = 2 * piece
        rows_shape = (n_seq, n_rows, head_dim)
        kv_shape = (n_seq, piece, head_dim)
        late_shape = (N_LATE, two, head_dim)
        main_shape = (n_seq - N_LATE, piece, head_dim)
        bf16, f32, i32 = jnp.bfloat16, jnp.float32, jnp.int32
        dma = pltpu.SemaphoreType.DMA
        any_spec = pl.BlockSpec(memory_space=pl.ANY)
        n_chip = n_dev // 2
        out = pl.pallas_call(
            functools.partial(attention_kernel, n_dev, n_heads),
            name='attention',
            out_shape=[jax.ShapeDtypeStruct(rows_shape, bf16)] * 2 + [jax.ShapeDtypeStruct(main_shape, bf16)] * 2
            + [jax.ShapeDtypeStruct(late_shape, f32)] * 3,
            in_specs=[any_spec] * 5,
            out_specs=[any_spec] * 7,
            scratch_shapes=[
                pltpu.VMEM((n_seq, 2, n_chip, 2, piece, head_dim), bf16),
                pltpu.VMEM((n_seq, two, head_dim), f32),
                pltpu.VMEM((n_seq, two, head_dim), f32),
                pltpu.VMEM((n_seq, two, head_dim), f32),
                pltpu.VMEM((NACC, n_chip, two, head_dim), f32),
                pltpu.VMEM((2, 2, n_chip, two, head_dim), f32),
                pltpu.VMEM((NPRX, n_chip, two, head_dim), f32),
                pltpu.VMEM((2, 2, n_rows, head_dim), bf16),
                pltpu.VMEM((2, 2, n_rows, head_dim), bf16),
                pltpu.VMEM((n_rows, n_key), bf16),
                pltpu.VMEM((n_rows, n_key), bf16),
                pltpu.VMEM(main_shape, bf16),
                pltpu.VMEM(main_shape, bf16),
                pltpu.VMEM(late_shape, f32),
                pltpu.VMEM((n_dev, n_seq, piece), i32),
                pltpu.VMEM((n_seq, 1, n_key), i32),
                pltpu.VMEM((n_seq, 1, piece), i32),
                pltpu.VMEM((piece, n_key), f32),
                dma((5,)), dma, dma,
                dma((4,)), dma((n_chip, n_seq)), dma, dma((n_seq,)),
                dma((2,)), dma((2,)),
                dma((2,)), dma((NPRX,)), dma((3, n_seq)), dma((NACC,)), dma, dma,
            ],
            compiler_params=pltpu.CompilerParams(collective_id=0, has_side_effects=True, vmem_limit_bytes=63 * 1024 * 1024),
        )(query.reshape(rows_shape), grad_out.reshape(rows_shape), keys.reshape(kv_shape), values.reshape(kv_shape), doc_id)
        attn_out, grad_query, grad_keys, grad_values, near, far, own = out
        attn_out, grad_query = pl.pallas_call(
            copy_kernel,
            name='results',
            out_shape=[jax.ShapeDtypeStruct(rows_shape, bf16)] * 2,
            in_specs=[any_spec] * 2,
            out_specs=[any_spec] * 2,
            scratch_shapes=[pltpu.VMEM((N_COPY, COPY_BLOCK, n_rows, head_dim), bf16), dma((N_COPY,)), dma((N_COPY,))],
            compiler_params=pltpu.CompilerParams(vmem_limit_bytes=52 * 1024 * 1024),
            cost_estimate=pl.CostEstimate(flops=12_000_000_000, bytes_accessed=8 * n_seq * n_rows * head_dim,
                                          transcendentals=0),
        )(attn_out, grad_query)
        to_near = [(d, d - 2) for d in range(2, n_dev)]
        to_far = [(n_dev - 2 + e, e) for e in range(2)]
        late = own + lax.ppermute(near, 'cp', to_near) + lax.ppermute(far, 'cp', to_far)
        late_keys = (late[:, 0:piece] * head_dim ** -0.5).astype(bf16)
        late_values = late[:, piece:two].astype(bf16)
        grad_keys = jnp.concatenate([grad_keys, late_keys])
        grad_values = jnp.concatenate([grad_values, late_values])
        return (attn_out.reshape(query.shape), grad_query.reshape(query.shape),
                grad_keys.reshape(keys.shape), grad_values.reshape(values.shape))

    return jax.shard_map(per_device, mesh=mesh, in_specs=(seq_spec,) * 4 + (P('dp', 'cp'),), out_specs=(seq_spec,) * 4, check_vma=False)
```

```python
import functools

import jax
import jax.numpy as jnp
from jax import lax
from jax.experimental import pallas as pl
from jax.experimental.pallas import tpu as pltpu
from jax.sharding import PartitionSpec as P

MESH = pl.DeviceIdType.MESH
LOG2E = 1.4426950408889634
HIDDEN = -3.0e38
NACC = 12
NPRX = 4
COPY_BLOCK = 2
N_COPY = 32
N_FIRST = 1
N_TURN = 3
N_LATE = 9


HOPS = ((1, 1, 2, None), (1, 0, 2, None), (2, 1, 3, 0), (2, 2, 3, None), (0, 1, 3, 1), (1, 1, 0, 1), (0, 0, 3, None), (0, 0, 1, None))
PUSH = {0: (0, 8), 1: (2, 12), 2: (3, 3), 3: (2, 5)}
TAKE = {0: (0, 10), 1: (2, 6), 2: (2, 2), 3: (0, 1)}
SENDS = {(3, 0): ((1, 2, 0, False, None), (0, 0, 1, False, 1), (2, 2, 1, False, 0)), (3, 1): ((2, 2, 0, False, 0), (0, 0, 0, True, 1), (1, 0, 2, False, None)), (2, 0): ((1, 1, 1, True, 0), (0, 1, 0, False, None)), (2, 1): ((1, 1, 0, False, 0), (0, 3, 0, False, None)), (1, 0): ((0, 0, 0, True, 0),), (1, 1): ((0, 0, 1, False, 0),)}
RELAY = {(3, 1): (3, 0), (2, 0): (8, 0), (1, 0): (8, 0), (0, 1): (7, 2)}
FINISH = {(3, 0): (1, ()), (3, 1): (1, ()), (2, 0): (7, (1,)), (2, 1): (5, (0,)), (1, 0): (10, (1,)), (1, 1): (10, (0, 1)), (0, 0): (10, (0, 1)), (0, 1): (9, (0, 1))}
LAG_MAX = 10
FINISH_LATE = {(1, 1): (1,)}
TURNED, TURN, TURN_LAG = (3, 1, 1), (2, 1), 4


def attention_kernel(n_dev, n_heads, *refs):
    (q_ref, g_ref, k_ref, v_ref, doc_ref, o_ref, dq_ref, dk_ref, dv_ref, near_ref, far_ref, own_ref,
     kv, rx0, rx1, rx2, acc, part, prx, qg, odq, pb, dsb, fin_k, fin_v, own, docs, kdoc, odoc, vis,
     load_sem, doc_tx, doc_rx, kv_tx, kv_rx, kvp_tx, kvp_rx, qg_sem, odq_sem,
     part_tx, prx_sem, rx_sem, tx_sem, fwd_tx, late_sem) = refs
    rx = (rx0, rx1, rx2)
    n_seq, n_rows, head_dim = q_ref.shape
    piece = k_ref.shape[1]
    two = 2 * piece
    n_chip = n_dev // 2
    scale = head_dim ** -0.5
    me = lax.axis_index('cp')
    chip = me // 2
    core = me % 2
    partner = chip * 2 + (1 - core)

    def dev(c):
        return {'cp': c * 2 + core}

    def remote(src, dst, tx, rx, to):
        return pltpu.make_async_remote_copy(src_ref=src, dst_ref=dst, send_sem=tx, recv_sem=rx,
                                            device_id=to, device_id_type=MESH)

    def local_wait(ref, sem):
        pltpu.make_async_copy(ref, ref, sem).wait()

    barrier = pltpu.get_barrier_semaphore()
    for hop in range(1, n_dev):
        pl.semaphore_signal(barrier, inc=1, device_id={'cp': (me + hop) % n_dev}, device_id_type=MESH)

    def own_copies(lo, n, sem):
        seqs = pl.ds(lo, n)
        return (pltpu.make_async_copy(k_ref.at[seqs], kv.at[seqs, 0, chip, core], load_sem.at[sem]),
                pltpu.make_async_copy(v_ref.at[seqs], kv.at[seqs, 1, chip, core], load_sem.at[sem + 1]))

    own_d = pltpu.make_async_copy(doc_ref, docs.at[me], load_sem.at[4])
    own_first = own_copies(0, N_FIRST, 0)
    own_rest = own_copies(N_FIRST, n_seq - N_FIRST, 2)
    for copy in (*own_first, own_d, *own_rest):
        copy.start()

    def qg_start(b):
        pltpu.make_async_copy(q_ref.at[b], qg.at[b % 2, 0], qg_sem.at[b % 2]).start()
        pltpu.make_async_copy(g_ref.at[b], qg.at[b % 2, 1], qg_sem.at[b % 2]).start()

    def odq_start(b):
        pltpu.make_async_copy(odq.at[b % 2, 0], o_ref.at[b], odq_sem.at[b % 2]).start()
        pltpu.make_async_copy(odq.at[b % 2, 1], dq_ref.at[b], odq_sem.at[b % 2]).start()

    def odq_wait(b):
        local_wait(odq.at[b % 2], odq_sem.at[b % 2])

    qg_start(0)
    for copy in (*own_first, own_d):
        copy.wait()
    odoc[...] = docs[me].reshape(n_seq, 1, piece)
    pl.semaphore_wait(barrier, n_dev - 1)

    def run_chip(c):
        n_key = two * (c + 1)
        here = pl.ds(0, c + 1)
        first_late = n_seq - N_LATE
        first_turn = n_seq - N_TURN

        def doc_copy(to):
            return remote(docs.at[me], docs.at[me], doc_tx, doc_rx, to)

        doc_dests = [{'cp': partner}] + [{'cp': d} for d in range(two // piece * (c + 1), n_dev)]

        flows = [hop[1:] for hop in HOPS if hop[0] == c]
        through = [src for src, _, _ in flows if src > c]

        def by_core(who, fn):
            if who is None:
                fn()
            else:
                pl.when(core == who)(fn)

        def kv_sem(src, to, b):
            return kv_rx.at[0 if to == n_chip - 1 else src, b]

        def kv_copy(i, b):
            src, to, _ = flows[i]
            blk = kv.at[b, :, src, core]
            return remote(blk, blk, kv_tx.at[i], kv_sem(src, to, b), dev(to))

        def kvp_copy(b):
            blk = kv.at[b, :, here, core]
            return remote(blk, blk, kvp_tx, kvp_rx.at[b], {'cp': partner})

        def send_on(src, b):
            for i, (s, _, who) in enumerate(flows):
                if s == src:
                    by_core(who, lambda: kv_copy(i, b).start())

        def push(b):
            send_on(c, b)

        def take(b):
            if c == n_chip - 1:
                local_wait(kv.at[b, :, pl.ds(0, c), core], kv_rx.at[0, b])
            else:
                for src in range(c - 1, -1, -1):
                    local_wait(kv.at[b, :, src, core], kv_rx.at[src, b])
                    send_on(src, b)
            kvp_copy(b).start()
            for src in through:
                who = [w for s, _, w in flows if s == src][0]

                def pass_on():
                    local_wait(kv.at[b, :, src, core], kv_rx.at[src, b])
                    for i, (s, _, _) in enumerate(flows):
                        if s == src:
                            kv_copy(i, b).start()

                by_core(who, pass_on)

        def ramp(lead, fn):
            first, most = lead
            start = min(first, most)

            def at_step(t):
                b = jnp.minimum(start + 2 * t, t + most)
                pl.when(b < n_seq)(lambda: fn(b))
                if most - start > 0:
                    pl.when(t < most - start)(lambda: fn(b + 1))

            return start, at_step

        def arrived(b):
            local_wait(kv.at[b, :, here, 1 - core], kvp_rx.at[b])

        n_push, push_at = ramp(PUSH[c], push)
        n_take, take_at = ramp(TAKE[c], take)
        for b in range(n_push):
            if b == N_FIRST:
                for copy in own_rest:
                    copy.wait()
            push(b)
        if n_push <= N_FIRST:
            for copy in own_rest:
                copy.wait()
        for to in doc_dests:
            doc_copy(to).start()
        for b in range(n_take):
            take(b)

        n_doc = 2 * c + 1
        pltpu.make_async_copy(docs.at[pl.ds(0, n_doc)], docs.at[pl.ds(0, n_doc)], doc_rx).wait()
        for p in range(2 * c + 2):
            kdoc[:, :, p * piece:(p + 1) * piece] = docs[p].reshape(n_seq, 1, piece)

        def compute(b):
            slot = b % 2
            keys = kv[b, 0, here].reshape(n_key, head_dim)
            vals = kv[b, 1, here].reshape(n_key, head_dim)
            tok = lax.broadcasted_iota(jnp.int32, (piece, piece), 0)
            tok_t = lax.broadcasted_iota(jnp.int32, (piece, piece), 1)
            own_doc = odoc[b]
            q_doc = jnp.sum(jnp.where(tok == tok_t, own_doc, 0), axis=1, keepdims=True)
            key_doc = kdoc[b, :, 0:n_key]
            q_pos = me * piece + lax.broadcasted_iota(jnp.int32, (piece, n_key), 0)
            k_pos = lax.broadcasted_iota(jnp.int32, (piece, n_key), 1)
            seen = (q_doc == key_doc) & (k_pos <= q_pos)
            vis[:, 0:n_key] = jnp.where(seen, 0.0, HIDDEN)
            nt = (((1,), (1,)), ((), ()))
            tn = (((0,), (0,)), ((), ()))
            f32 = jnp.float32
            s = lax.dot_general(qg[slot, 0], keys, nt, preferred_element_type=f32)
            dp = lax.dot_general(qg[slot, 1], vals, nt, preferred_element_type=f32)
            s = s.reshape(piece, n_heads, n_key) * (scale * LOG2E) + vis[:, 0:n_key].reshape(piece, 1, n_key)
            s = s.reshape(n_rows, n_key)
            e = jnp.exp2(s - jnp.max(s, axis=1, keepdims=True))
            p = e * (1.0 / jnp.sum(e, axis=1, keepdims=True))
            pb[:, 0:n_key] = p.astype(jnp.bfloat16)
            o16 = jnp.dot(pb[:, 0:n_key], vals, preferred_element_type=f32).astype(jnp.bfloat16)
            dv = lax.dot_general(pb[:, 0:n_key], qg[slot, 1], tn, preferred_element_type=f32)
            odq[slot, 0] = o16
            delta = jnp.sum(qg[slot, 1].astype(f32) * o16.astype(f32), axis=1, keepdims=True)
            dsb[:, 0:n_key] = (p * (dp - delta)).astype(jnp.bfloat16)
            dq = jnp.dot(dsb[:, 0:n_key], keys, preferred_element_type=f32)
            odq[slot, 1] = (dq * scale).astype(jnp.bfloat16)
            dk = lax.dot_general(dsb[:, 0:n_key], qg[slot, 0], tn, preferred_element_type=f32)
            for a in range(c + 1):
                for p in range(2):
                    rows = slice((2 * a + p) * piece, (2 * a + p + 1) * piece)
                    part[slot, p, a, 0:piece, :] = dk[rows]
                    part[slot, p, a, piece:two, :] = dv[rows]

        def part_copy(b):
            return remote(part.at[b % 2, 1 - core, here], prx.at[b % NPRX, here], part_tx.at[b % 2],
                          prx_sem.at[b % NPRX], {'cp': partner})

        def unit_send(b, e, i):
            a, to, buf, _, late = SENDS[c, e][i]
            unit = acc.at[b % NACC, a]
            sem = tx_sem.at[b % NACC]

            def now(to=to, buf=buf):
                remote(unit, rx[buf].at[b], sem, rx_sem.at[buf, b], dev(to)).start()

            if (c, e, a) == TURNED:
                pl.when(b < first_turn)(now)
                pl.when(b >= first_turn)(lambda: now(*TURN))
            elif late is None:
                now()
            else:
                pl.when(b < first_late)(now)

                @pl.when(b >= first_late)
                def _():
                    pltpu.make_async_copy(unit, (near_ref, far_ref)[late].at[b - first_late], sem).start()

        def got(buf, b):
            local_wait(rx[buf].at[b], rx_sem.at[buf, b])

        def merge_partner(b):
            local_wait(prx.at[b % NPRX, here], prx_sem.at[b % NPRX])
            acc[b % NACC, here] = part[b % 2, core, here] + prx[b % NPRX, here]
            for e in range(2):
                sends = [i for i, s in enumerate(SENDS.get((c, e), ())) if not s[3]]
                if sends:
                    @pl.when(core == e)
                    def _():
                        for i in sends:
                            if (c, e, SENDS[c, e][i][0]) == (TURN[0], TURNED[1], TURNED[2]):
                                pl.when(b < first_turn)(lambda: unit_send(b, e, i))
                            else:
                                unit_send(b, e, i)

        def relay(b, e):
            buf = RELAY[c, e][1]

            def take_in():
                got(buf, b)
                if c == 0:
                    fwd_copy(b).start()
                    return
                for i, (a, _, _, after, _) in enumerate(SENDS[c, e]):
                    if after:
                        acc[b % NACC, a] = acc[b % NACC, a] + rx[buf][b]
                        unit_send(b, e, i)

            if c == 0:
                pl.when(b < first_turn)(take_in)
            else:
                take_in()

        def add_turned(b):
            got(TURN[1], b)
            a = TURNED[2]
            acc[b % NACC, a] = acc[b % NACC, a] + rx[TURN[1]][b]
            unit_send(b, TURNED[1], [s[0] for s in SENDS[c, TURNED[1]]].index(a))

        def fwd_copy(b):
            return remote(rx2.at[b], rx1.at[b], fwd_tx, rx_sem.at[1, b], dev(1))

        def finish(b, e):
            def total(bufs):
                out = acc[b % NACC, c]
                for buf in bufs:
                    got(buf, b)
                    out = out + rx[buf][b]
                return out

            @pl.when(b < first_late)
            def _():
                out = total(FINISH[c, e][1])
                fin_k[b] = (out[0:piece] * scale).astype(jnp.bfloat16)
                fin_v[b] = out[piece:two].astype(jnp.bfloat16)

            @pl.when((b >= first_late) & (b < first_turn))
            def _():
                own[b - first_late] = total(FINISH_LATE.get((c, e), ()))

            @pl.when(b >= first_turn)
            def _():
                own[b - first_late] = total(())

        n_step = n_seq + LAG_MAX

        def when_seq(b, fn):
            pl.when((b >= 0) & (b < n_seq))(lambda: fn(b))

        def sent(b):
            for e in range(2):
                n = len(SENDS.get((c, e), ()))
                if n:
                    pl.when(core == e)(lambda: local_wait(acc.at[b % NACC, pl.ds(0, n)], tx_sem.at[b % NACC]))

        def step(t, carry):
            @pl.when(t < n_seq)
            def _():
                push_at(t)
                take_at(t)

                @pl.when(t + 1 < n_seq)
                def _():
                    qg_start(t + 1)

                @pl.when(t >= 2)
                def _():
                    odq_wait(t - 2)
                    part_copy(t - 2).wait_send()

                pl.when(t >= NACC)(lambda: sent(t - NACC))
                arrived(t)
                local_wait(qg.at[t % 2], qg_sem.at[t % 2])
                compute(t)
                odq_start(t)
                part_copy(t).start()

            when_seq(t - 1, merge_partner)
            for e in range(2):
                @pl.when(core == e)
                def _():
                    if (c, e) in RELAY:
                        when_seq(t - RELAY[c, e][0], lambda b: relay(b, e))
                    if (c, e) == (TURN[0], TURNED[1]):
                        b_turn = t - TURN_LAG
                        pl.when((b_turn >= first_turn) & (b_turn < n_seq))(lambda: add_turned(b_turn))
                    when_seq(t - FINISH[c, e][0], lambda b: finish(b, e))
            return carry

        lax.fori_loop(0, n_step, step, 0)

        for b in (n_seq - 2, n_seq - 1):
            odq_wait(b)
            part_copy(b).wait_send()
        for b in range(n_seq - NACC, n_seq):
            sent(b)
        whole = kv.at[:, :, 0, 0]
        for i, (_, _, who) in enumerate(flows):
            by_core(who, lambda: local_wait(whole, kv_tx.at[i]))
        local_wait(kv.at[:, :, here, 0], kvp_tx)
        for to in doc_dests:
            doc_copy(to).wait_send()
        if c == 0:
            pl.when(core == 1)(lambda: local_wait(rx2.at[pl.ds(0, first_turn)], fwd_tx))

    for c in range(n_chip):
        pl.when(chip == c)(functools.partial(run_chip, c))

    out_k = pltpu.make_async_copy(fin_k, dk_ref, load_sem.at[0])
    out_v = pltpu.make_async_copy(fin_v, dv_ref, load_sem.at[1])
    out_own = pltpu.make_async_copy(own, own_ref, late_sem)
    out_k.start()
    out_v.start()
    out_own.start()
    out_k.wait()
    out_v.wait()
    out_own.wait()


def copy_kernel(a_ref, b_ref, a_out, b_out, buf, in_sem, out_sem):
    n_buf, n_block = buf.shape[:2]
    total = 2 * a_ref.shape[0] // n_block
    ahead = n_buf // 2

    def read(i):
        src = (a_ref, b_ref)[i % 2].at[pl.ds(i // 2 * n_block, n_block)]
        return pltpu.make_async_copy(src, buf.at[i % n_buf], in_sem.at[i % n_buf])

    def write(i):
        dst = (a_out, b_out)[i % 2].at[pl.ds(i // 2 * n_block, n_block)]
        return pltpu.make_async_copy(buf.at[i % n_buf], dst, out_sem.at[i % n_buf])

    for i in range(ahead):
        read(i).start()
    for i in range(total):
        if i + ahead < total:
            if i + ahead >= n_buf:
                write(i + ahead - n_buf).wait()
            read(i + ahead).start()
        read(i).wait()
        write(i).start()
    for i in range(max(total - n_buf, 0), total):
        write(i).wait()


def solution(mesh):
    n_dev = mesh.shape['cp']
    seq_spec = P('dp', 'cp', None, None)

    def per_device(query, keys, values, grad_out, doc_id):
        n_seq, piece, n_heads, head_dim = query.shape
        n_rows = piece * n_heads
        n_key = piece * n_dev
        two = 2 * piece
        rows_shape = (n_seq, n_rows, head_dim)
        kv_shape = (n_seq, piece, head_dim)
        late_shape = (N_LATE, two, head_dim)
        main_shape = (n_seq - N_LATE, piece, head_dim)
        bf16, f32, i32 = jnp.bfloat16, jnp.float32, jnp.int32
        dma = pltpu.SemaphoreType.DMA
        any_spec = pl.BlockSpec(memory_space=pl.ANY)
        n_chip = n_dev // 2
        out = pl.pallas_call(
            functools.partial(attention_kernel, n_dev, n_heads),
            name='attention',
            out_shape=[jax.ShapeDtypeStruct(rows_shape, bf16)] * 2 + [jax.ShapeDtypeStruct(main_shape, bf16)] * 2
            + [jax.ShapeDtypeStruct(late_shape, f32)] * 3,
            in_specs=[any_spec] * 5,
            out_specs=[any_spec] * 7,
            scratch_shapes=[
                pltpu.VMEM((n_seq, 2, n_chip, 2, piece, head_dim), bf16),
                pltpu.VMEM((n_seq, two, head_dim), f32),
                pltpu.VMEM((n_seq, two, head_dim), f32),
                pltpu.VMEM((n_seq, two, head_dim), f32),
                pltpu.VMEM((NACC, n_chip, two, head_dim), f32),
                pltpu.VMEM((2, 2, n_chip, two, head_dim), f32),
                pltpu.VMEM((NPRX, n_chip, two, head_dim), f32),
                pltpu.VMEM((2, 2, n_rows, head_dim), bf16),
                pltpu.VMEM((2, 2, n_rows, head_dim), bf16),
                pltpu.VMEM((n_rows, n_key), bf16),
                pltpu.VMEM((n_rows, n_key), bf16),
                pltpu.VMEM(main_shape, bf16),
                pltpu.VMEM(main_shape, bf16),
                pltpu.VMEM(late_shape, f32),
                pltpu.VMEM((n_dev, n_seq, piece), i32),
                pltpu.VMEM((n_seq, 1, n_key), i32),
                pltpu.VMEM((n_seq, 1, piece), i32),
                pltpu.VMEM((piece, n_key), f32),
                dma((5,)), dma, dma,
                dma((4,)), dma((n_chip, n_seq)), dma, dma((n_seq,)),
                dma((2,)), dma((2,)),
                dma((2,)), dma((NPRX,)), dma((3, n_seq)), dma((NACC,)), dma, dma,
            ],
            compiler_params=pltpu.CompilerParams(collective_id=0, has_side_effects=True, vmem_limit_bytes=63 * 1024 * 1024),
        )(query.reshape(rows_shape), grad_out.reshape(rows_shape), keys.reshape(kv_shape), values.reshape(kv_shape), doc_id)
        attn_out, grad_query, grad_keys, grad_values, near, far, own = out
        attn_out, grad_query = pl.pallas_call(
            copy_kernel,
            name='results',
            out_shape=[jax.ShapeDtypeStruct(rows_shape, bf16)] * 2,
            in_specs=[any_spec] * 2,
            out_specs=[any_spec] * 2,
            scratch_shapes=[pltpu.VMEM((N_COPY, COPY_BLOCK, n_rows, head_dim), bf16), dma((N_COPY,)), dma((N_COPY,))],
            compiler_params=pltpu.CompilerParams(vmem_limit_bytes=52 * 1024 * 1024),
            cost_estimate=pl.CostEstimate(flops=12_000_000_000, bytes_accessed=8 * n_seq * n_rows * head_dim,
                                          transcendentals=0),
        )(attn_out, grad_query)
        to_near = [(d, d - 2) for d in range(2, n_dev)]
        to_far = [(n_dev - 2 + e, e) for e in range(2)]
        late = own + lax.ppermute(near, 'cp', to_near) + lax.ppermute(far, 'cp', to_far)
        late_keys = (late[:, 0:piece] * head_dim ** -0.5).astype(bf16)
        late_values = late[:, piece:two].astype(bf16)
        grad_keys = jnp.concatenate([grad_keys, late_keys])
        grad_values = jnp.concatenate([grad_values, late_values])
        return (attn_out.reshape(query.shape), grad_query.reshape(query.shape),
                grad_keys.reshape(keys.shape), grad_values.reshape(values.shape))

    return jax.shard_map(per_device, mesh=mesh, in_specs=(seq_spec,) * 4 + (P('dp', 'cp'),), out_specs=(seq_spec,) * 4, check_vma=False)
```

```python
import functools

import jax
import jax.numpy as jnp
from jax import lax
from jax.experimental import pallas as pl
from jax.experimental.pallas import tpu as pltpu
from jax.sharding import PartitionSpec as P

MESH = pl.DeviceIdType.MESH
LOG2E = 1.4426950408889634
HIDDEN = -3.0e38
NACC = 12
NPRX = 4
COPY_BLOCK = 2
N_COPY = 32
N_FIRST = 1
N_TURN = 3
N_LATE = 9


HOPS = ((1, 1, 2, None), (1, 0, 2, None), (2, 1, 3, 0), (2, 2, 3, None), (0, 1, 3, 1), (1, 1, 0, 1), (0, 0, 3, None), (0, 0, 1, None))
PUSH = {0: (0, 8), 1: (2, 12), 2: (3, 3), 3: (2, 5)}
TAKE = {0: (0, 10), 1: (2, 6), 2: (2, 2), 3: (0, 1)}
SENDS = {(3, 0): ((1, 2, 0, False, None), (0, 0, 1, False, 1), (2, 2, 1, False, 0)), (3, 1): ((2, 2, 0, False, 0), (0, 0, 0, True, 1), (1, 0, 2, False, None)), (2, 0): ((1, 1, 1, True, 0), (0, 1, 0, False, None)), (2, 1): ((1, 1, 0, False, 0), (0, 3, 0, False, None)), (1, 0): ((0, 0, 0, True, 0),), (1, 1): ((0, 0, 1, False, 0),)}
RELAY = {(3, 1): (3, 0), (2, 0): (8, 0), (1, 0): (8, 0), (0, 1): (7, 2)}
FINISH = {(3, 0): (1, ()), (3, 1): (1, ()), (2, 0): (7, (1,)), (2, 1): (5, (0,)), (1, 0): (10, (1,)), (1, 1): (10, (0, 1)), (0, 0): (10, (0, 1)), (0, 1): (9, (0, 1))}
LAG_MAX = 10
FINISH_LATE = {(1, 1): (1,)}
TURNED, TURN, TURN_LAG = (3, 1, 1), (2, 1), 4


def attention_kernel(n_dev, n_heads, *refs):
    (q_ref, g_ref, k_ref, v_ref, doc_ref, o_ref, dq_ref, dk_ref, dv_ref, near_ref, far_ref, own_ref,
     kv, rx0, rx1, rx2, acc, part, prx, qg, odq, pb, dsb, fin_k, fin_v, own, docs, kdoc, odoc, vis,
     load_sem, doc_tx, doc_rx, kv_tx, kv_rx, kvp_tx, kvp_rx, qg_sem, odq_sem,
     part_tx, prx_sem, rx_sem, tx_sem, fwd_tx, late_sem) = refs
    rx = (rx0, rx1, rx2)
    n_seq, n_rows, head_dim = q_ref.shape
    piece = k_ref.shape[1]
    two = 2 * piece
    n_chip = n_dev // 2
    scale = head_dim ** -0.5
    me = lax.axis_index('cp')
    chip = me // 2
    core = me % 2
    partner = chip * 2 + (1 - core)

    def dev(c):
        return {'cp': c * 2 + core}

    def remote(src, dst, tx, rx, to):
        return pltpu.make_async_remote_copy(src_ref=src, dst_ref=dst, send_sem=tx, recv_sem=rx,
                                            device_id=to, device_id_type=MESH)

    def local_wait(ref, sem):
        pltpu.make_async_copy(ref, ref, sem).wait()

    barrier = pltpu.get_barrier_semaphore()
    for hop in range(1, n_dev):
        pl.semaphore_signal(barrier, inc=1, device_id={'cp': (me + hop) % n_dev}, device_id_type=MESH)

    def own_copies(lo, n, sem):
        seqs = pl.ds(lo, n)
        return (pltpu.make_async_copy(k_ref.at[seqs], kv.at[seqs, 0, chip, core], load_sem.at[sem]),
                pltpu.make_async_copy(v_ref.at[seqs], kv.at[seqs, 1, chip, core], load_sem.at[sem + 1]))

    own_d = pltpu.make_async_copy(doc_ref, docs.at[me], load_sem.at[4])
    own_first = own_copies(0, N_FIRST, 0)
    own_rest = own_copies(N_FIRST, n_seq - N_FIRST, 2)
    for copy in (*own_first, own_d, *own_rest):
        copy.start()

    def qg_start(b):
        pltpu.make_async_copy(q_ref.at[b], qg.at[b % 2, 0], qg_sem.at[b % 2]).start()
        pltpu.make_async_copy(g_ref.at[b], qg.at[b % 2, 1], qg_sem.at[b % 2]).start()

    def odq_start(b):
        pltpu.make_async_copy(odq.at[b % 2, 0], o_ref.at[b], odq_sem.at[b % 2]).start()
        pltpu.make_async_copy(odq.at[b % 2, 1], dq_ref.at[b], odq_sem.at[b % 2]).start()

    def odq_wait(b):
        local_wait(odq.at[b % 2], odq_sem.at[b % 2])

    qg_start(0)
    for copy in (*own_first, own_d):
        copy.wait()
    odoc[...] = docs[me].reshape(n_seq, 1, piece)
    pl.semaphore_wait(barrier, n_dev - 1)

    def run_chip(c):
        n_key = two * (c + 1)
        here = pl.ds(0, c + 1)
        first_late = n_seq - N_LATE
        first_turn = n_seq - N_TURN

        def doc_copy(to):
            return remote(docs.at[me], docs.at[me], doc_tx, doc_rx, to)

        doc_dests = [{'cp': partner}] + [{'cp': d} for d in range(two // piece * (c + 1), n_dev)]

        flows = [hop[1:] for hop in HOPS if hop[0] == c]
        through = [src for src, _, _ in flows if src > c]

        def by_core(who, fn):
            if who is None:
                fn()
            else:
                pl.when(core == who)(fn)

        def kv_sem(src, to, b):
            return kv_rx.at[0 if to == n_chip - 1 else src, b]

        def kv_copy(i, b):
            src, to, _ = flows[i]
            blk = kv.at[b, :, src, core]
            return remote(blk, blk, kv_tx.at[i], kv_sem(src, to, b), dev(to))

        def kvp_copy(b):
            blk = kv.at[b, :, here, core]
            return remote(blk, blk, kvp_tx, kvp_rx.at[b], {'cp': partner})

        def send_on(src, b):
            for i, (s, _, who) in enumerate(flows):
                if s == src:
                    by_core(who, lambda: kv_copy(i, b).start())

        def push(b):
            send_on(c, b)

        def take(b):
            if c == n_chip - 1:
                local_wait(kv.at[b, :, pl.ds(0, c), core], kv_rx.at[0, b])
            else:
                for src in range(c - 1, -1, -1):
                    local_wait(kv.at[b, :, src, core], kv_rx.at[src, b])
                    send_on(src, b)
            kvp_copy(b).start()
            for src in through:
                who = [w for s, _, w in flows if s == src][0]

                def pass_on():
                    local_wait(kv.at[b, :, src, core], kv_rx.at[src, b])
                    for i, (s, _, _) in enumerate(flows):
                        if s == src:
                            kv_copy(i, b).start()

                by_core(who, pass_on)

        def ramp(lead, fn):
            first, most = lead
            start = min(first, most)

            def at_step(t):
                b = jnp.minimum(start + 2 * t, t + most)
                pl.when(b < n_seq)(lambda: fn(b))
                if most - start > 0:
                    pl.when(t < most - start)(lambda: fn(b + 1))

            return start, at_step

        def arrived(b):
            local_wait(kv.at[b, :, here, 1 - core], kvp_rx.at[b])

        n_push, push_at = ramp(PUSH[c], push)
        n_take, take_at = ramp(TAKE[c], take)
        for b in range(n_push):
            if b == N_FIRST:
                for copy in own_rest:
                    copy.wait()
            push(b)
        if n_push <= N_FIRST:
            for copy in own_rest:
                copy.wait()
        for to in doc_dests:
            doc_copy(to).start()
        for b in range(n_take):
            take(b)

        n_doc = 2 * c + 1
        pltpu.make_async_copy(docs.at[pl.ds(0, n_doc)], docs.at[pl.ds(0, n_doc)], doc_rx).wait()
        for p in range(2 * c + 2):
            kdoc[:, :, p * piece:(p + 1) * piece] = docs[p].reshape(n_seq, 1, piece)

        def compute(b):
            slot = b % 2
            keys = kv[b, 0, here].reshape(n_key, head_dim)
            vals = kv[b, 1, here].reshape(n_key, head_dim)
            tok = lax.broadcasted_iota(jnp.int32, (piece, piece), 0)
            tok_t = lax.broadcasted_iota(jnp.int32, (piece, piece), 1)
            own_doc = odoc[b]
            q_doc = jnp.sum(jnp.where(tok == tok_t, own_doc, 0), axis=1, keepdims=True)
            key_doc = kdoc[b, :, 0:n_key]
            q_pos = me * piece + lax.broadcasted_iota(jnp.int32, (piece, n_key), 0)
            k_pos = lax.broadcasted_iota(jnp.int32, (piece, n_key), 1)
            seen = (q_doc == key_doc) & (k_pos <= q_pos)
            vis[:, 0:n_key] = jnp.where(seen, 0.0, HIDDEN)
            nt = (((1,), (1,)), ((), ()))
            tn = (((0,), (0,)), ((), ()))
            f32 = jnp.float32
            s = lax.dot_general(qg[slot, 0], keys, nt, preferred_element_type=f32)
            dp = lax.dot_general(qg[slot, 1], vals, nt, preferred_element_type=f32)
            s = s.reshape(piece, n_heads, n_key) * (scale * LOG2E) + vis[:, 0:n_key].reshape(piece, 1, n_key)
            s = s.reshape(n_rows, n_key)
            e = jnp.exp2(s - jnp.max(s, axis=1, keepdims=True))
            p = e * (1.0 / jnp.sum(e, axis=1, keepdims=True))
            pb[:, 0:n_key] = p.astype(jnp.bfloat16)
            o16 = jnp.dot(pb[:, 0:n_key], vals, preferred_element_type=f32).astype(jnp.bfloat16)
            dv = lax.dot_general(pb[:, 0:n_key], qg[slot, 1], tn, preferred_element_type=f32)
            odq[slot, 0] = o16
            delta = jnp.sum(qg[slot, 1].astype(f32) * o16.astype(f32), axis=1, keepdims=True)
            dsb[:, 0:n_key] = (p * (dp - delta)).astype(jnp.bfloat16)
            dq = jnp.dot(dsb[:, 0:n_key], keys, preferred_element_type=f32)
            odq[slot, 1] = (dq * scale).astype(jnp.bfloat16)
            dk = lax.dot_general(dsb[:, 0:n_key], qg[slot, 0], tn, preferred_element_type=f32)
            for a in range(c + 1):
                for p in range(2):
                    rows = slice((2 * a + p) * piece, (2 * a + p + 1) * piece)
                    part[slot, p, a, 0:piece, :] = dk[rows]
                    part[slot, p, a, piece:two, :] = dv[rows]

        def part_copy(b):
            return remote(part.at[b % 2, 1 - core, here], prx.at[b % NPRX, here], part_tx.at[b % 2],
                          prx_sem.at[b % NPRX], {'cp': partner})

        def unit_send(b, e, i):
            a, to, buf, _, late = SENDS[c, e][i]
            unit = acc.at[b % NACC, a]
            sem = tx_sem.at[b % NACC]

            def now(to=to, buf=buf):
                remote(unit, rx[buf].at[b], sem, rx_sem.at[buf, b], dev(to)).start()

            if (c, e, a) == TURNED:
                pl.when(b < first_turn)(now)
                pl.when(b >= first_turn)(lambda: now(*TURN))
            elif late is None:
                now()
            else:
                pl.when(b < first_late)(now)

                @pl.when(b >= first_late)
                def _():
                    pltpu.make_async_copy(unit, (near_ref, far_ref)[late].at[b - first_late], sem).start()

        def got(buf, b):
            local_wait(rx[buf].at[b], rx_sem.at[buf, b])

        def merge_partner(b):
            local_wait(prx.at[b % NPRX, here], prx_sem.at[b % NPRX])
            acc[b % NACC, here] = part[b % 2, core, here] + prx[b % NPRX, here]
            for e in range(2):
                sends = [i for i, s in enumerate(SENDS.get((c, e), ())) if not s[3]]
                if sends:
                    @pl.when(core == e)
                    def _():
                        for i in sends:
                            if (c, e, SENDS[c, e][i][0]) == (TURN[0], TURNED[1], TURNED[2]):
                                pl.when(b < first_turn)(lambda: unit_send(b, e, i))
                            else:
                                unit_send(b, e, i)

        def relay(b, e):
            buf = RELAY[c, e][1]

            def take_in():
                got(buf, b)
                if c == 0:
                    fwd_copy(b).start()
                    return
                for i, (a, _, _, after, _) in enumerate(SENDS[c, e]):
                    if after:
                        acc[b % NACC, a] = acc[b % NACC, a] + rx[buf][b]
                        unit_send(b, e, i)

            if c == 0:
                pl.when(b < first_turn)(take_in)
            else:
                take_in()

        def add_turned(b):
            got(TURN[1], b)
            a = TURNED[2]
            acc[b % NACC, a] = acc[b % NACC, a] + rx[TURN[1]][b]
            unit_send(b, TURNED[1], [s[0] for s in SENDS[c, TURNED[1]]].index(a))

        def fwd_copy(b):
            return remote(rx2.at[b], rx1.at[b], fwd_tx, rx_sem.at[1, b], dev(1))

        def finish(b, e):
            def total(bufs):
                out = acc[b % NACC, c]
                for buf in bufs:
                    got(buf, b)
                    out = out + rx[buf][b]
                return out

            @pl.when(b < first_late)
            def _():
                out = total(FINISH[c, e][1])
                fin_k[b] = (out[0:piece] * scale).astype(jnp.bfloat16)
                fin_v[b] = out[piece:two].astype(jnp.bfloat16)

            @pl.when((b >= first_late) & (b < first_turn))
            def _():
                own[b - first_late] = total(FINISH_LATE.get((c, e), ()))

            @pl.when(b >= first_turn)
            def _():
                own[b - first_late] = total(())

        n_step = n_seq + LAG_MAX

        def when_seq(b, fn):
            pl.when((b >= 0) & (b < n_seq))(lambda: fn(b))

        def sent(b):
            for e in range(2):
                n = len(SENDS.get((c, e), ()))
                if n:
                    pl.when(core == e)(lambda: local_wait(acc.at[b % NACC, pl.ds(0, n)], tx_sem.at[b % NACC]))

        def step(t, carry):
            @pl.when(t < n_seq)
            def _():
                push_at(t)
                take_at(t)

                @pl.when(t + 1 < n_seq)
                def _():
                    qg_start(t + 1)

                @pl.when(t >= 2)
                def _():
                    odq_wait(t - 2)
                    part_copy(t - 2).wait_send()

                pl.when(t >= NACC)(lambda: sent(t - NACC))
                arrived(t)
                local_wait(qg.at[t % 2], qg_sem.at[t % 2])
                compute(t)
                odq_start(t)
                part_copy(t).start()

            when_seq(t - 1, merge_partner)
            for e in range(2):
                @pl.when(core == e)
                def _():
                    if (c, e) in RELAY:
                        when_seq(t - RELAY[c, e][0], lambda b: relay(b, e))
                    if (c, e) == (TURN[0], TURNED[1]):
                        b_turn = t - TURN_LAG
                        pl.when((b_turn >= first_turn) & (b_turn < n_seq))(lambda: add_turned(b_turn))
                    when_seq(t - FINISH[c, e][0], lambda b: finish(b, e))
            return carry

        lax.fori_loop(0, n_step, step, 0)

        for b in (n_seq - 2, n_seq - 1):
            odq_wait(b)
            part_copy(b).wait_send()
        for b in range(n_seq - NACC, n_seq):
            sent(b)
        whole = kv.at[:, :, 0, 0]
        for i, (_, _, who) in enumerate(flows):
            by_core(who, lambda: local_wait(whole, kv_tx.at[i]))
        local_wait(kv.at[:, :, here, 0], kvp_tx)
        for to in doc_dests:
            doc_copy(to).wait_send()
        if c == 0:
            pl.when(core == 1)(lambda: local_wait(rx2.at[pl.ds(0, first_turn)], fwd_tx))

    for c in range(n_chip):
        pl.when(chip == c)(functools.partial(run_chip, c))

    out_k = pltpu.make_async_copy(fin_k, dk_ref, load_sem.at[0])
    out_v = pltpu.make_async_copy(fin_v, dv_ref, load_sem.at[1])
    out_own = pltpu.make_async_copy(own, own_ref, late_sem)
    out_k.start()
    out_v.start()
    out_own.start()
    out_k.wait()
    out_v.wait()
    out_own.wait()


def copy_kernel(a_ref, b_ref, a_out, b_out, buf, in_sem, out_sem):
    n_buf, n_block = buf.shape[:2]
    total = 2 * a_ref.shape[0] // n_block
    ahead = n_buf // 2

    def read(i):
        src = (a_ref, b_ref)[i % 2].at[pl.ds(i // 2 * n_block, n_block)]
        return pltpu.make_async_copy(src, buf.at[i % n_buf], in_sem.at[i % n_buf])

    def write(i):
        dst = (a_out, b_out)[i % 2].at[pl.ds(i // 2 * n_block, n_block)]
        return pltpu.make_async_copy(buf.at[i % n_buf], dst, out_sem.at[i % n_buf])

    for i in range(ahead):
        read(i).start()
    for i in range(total):
        if i + ahead < total:
            if i + ahead >= n_buf:
                write(i + ahead - n_buf).wait()
            read(i + ahead).start()
        read(i).wait()
        write(i).start()
    for i in range(max(total - n_buf, 0), total):
        write(i).wait()


def solution(mesh):
    n_dev = mesh.shape['cp']
    seq_spec = P('dp', 'cp', None, None)

    def per_device(query, keys, values, grad_out, doc_id):
        n_seq, piece, n_heads, head_dim = query.shape
        n_rows = piece * n_heads
        n_key = piece * n_dev
        two = 2 * piece
        rows_shape = (n_seq, n_rows, head_dim)
        kv_shape = (n_seq, piece, head_dim)
        late_shape = (N_LATE, two, head_dim)
        main_shape = (n_seq - N_LATE, piece, head_dim)
        bf16, f32, i32 = jnp.bfloat16, jnp.float32, jnp.int32
        dma = pltpu.SemaphoreType.DMA
        any_spec = pl.BlockSpec(memory_space=pl.ANY)
        n_chip = n_dev // 2
        out = pl.pallas_call(
            functools.partial(attention_kernel, n_dev, n_heads),
            name='attention',
            out_shape=[jax.ShapeDtypeStruct(rows_shape, bf16)] * 2 + [jax.ShapeDtypeStruct(main_shape, bf16)] * 2
            + [jax.ShapeDtypeStruct(late_shape, f32)] * 3,
            in_specs=[any_spec] * 5,
            out_specs=[any_spec] * 7,
            scratch_shapes=[
                pltpu.VMEM((n_seq, 2, n_chip, 2, piece, head_dim), bf16),
                pltpu.VMEM((n_seq, two, head_dim), f32),
                pltpu.VMEM((n_seq, two, head_dim), f32),
                pltpu.VMEM((n_seq, two, head_dim), f32),
                pltpu.VMEM((NACC, n_chip, two, head_dim), f32),
                pltpu.VMEM((2, 2, n_chip, two, head_dim), f32),
                pltpu.VMEM((NPRX, n_chip, two, head_dim), f32),
                pltpu.VMEM((2, 2, n_rows, head_dim), bf16),
                pltpu.VMEM((2, 2, n_rows, head_dim), bf16),
                pltpu.VMEM((n_rows, n_key), bf16),
                pltpu.VMEM((n_rows, n_key), bf16),
                pltpu.VMEM(main_shape, bf16),
                pltpu.VMEM(main_shape, bf16),
                pltpu.VMEM(late_shape, f32),
                pltpu.VMEM((n_dev, n_seq, piece), i32),
                pltpu.VMEM((n_seq, 1, n_key), i32),
                pltpu.VMEM((n_seq, 1, piece), i32),
                pltpu.VMEM((piece, n_key), f32),
                dma((5,)), dma, dma,
                dma((4,)), dma((n_chip, n_seq)), dma, dma((n_seq,)),
                dma((2,)), dma((2,)),
                dma((2,)), dma((NPRX,)), dma((3, n_seq)), dma((NACC,)), dma, dma,
            ],
            compiler_params=pltpu.CompilerParams(collective_id=0, has_side_effects=True, vmem_limit_bytes=63 * 1024 * 1024),
        )(query.reshape(rows_shape), grad_out.reshape(rows_shape), keys.reshape(kv_shape), values.reshape(kv_shape), doc_id)
        attn_out, grad_query, grad_keys, grad_values, near, far, own = out
        attn_out, grad_query = pl.pallas_call(
            copy_kernel,
            name='results',
            out_shape=[jax.ShapeDtypeStruct(rows_shape, bf16)] * 2,
            in_specs=[any_spec] * 2,
            out_specs=[any_spec] * 2,
            scratch_shapes=[pltpu.VMEM((N_COPY, COPY_BLOCK, n_rows, head_dim), bf16), dma((N_COPY,)), dma((N_COPY,))],
            compiler_params=pltpu.CompilerParams(vmem_limit_bytes=52 * 1024 * 1024),
            cost_estimate=pl.CostEstimate(flops=12_000_000_000, bytes_accessed=8 * n_seq * n_rows * head_dim,
                                          transcendentals=0),
        )(attn_out, grad_query)
        to_near = [(d, d - 2) for d in range(2, n_dev)]
        to_far = [(n_dev - 2 + e, e) for e in range(2)]
        from_far = lax.ppermute(far, 'cp', to_far)
        from_near = lax.ppermute(near, 'cp', to_near)
        late = own + from_far + from_near
        late_keys = (late[:, 0:piece] * head_dim ** -0.5).astype(bf16)
        late_values = late[:, piece:two].astype(bf16)
        grad_keys = jnp.concatenate([grad_keys, late_keys])
        grad_values = jnp.concatenate([grad_values, late_values])
        return (attn_out.reshape(query.shape), grad_query.reshape(query.shape),
                grad_keys.reshape(keys.shape), grad_values.reshape(values.shape))

    return jax.shard_map(per_device, mesh=mesh, in_specs=(seq_spec,) * 4 + (P('dp', 'cp'),), out_specs=(seq_spec,) * 4, check_vma=False)
```

```python
import functools

import jax
import jax.numpy as jnp
from jax import lax
from jax.experimental import pallas as pl
from jax.experimental.pallas import tpu as pltpu
from jax.sharding import PartitionSpec as P

MESH = pl.DeviceIdType.MESH
LOG2E = 1.4426950408889634
HIDDEN = -3.0e38
NACC = 12
NPRX = 4
COPY_BLOCK = 2
N_COPY = 28
N_FIRST = 1
N_TURN = 3
N_LATE = 9


HOPS = ((1, 1, 2, None), (1, 0, 2, None), (2, 1, 3, 0), (2, 2, 3, None), (0, 1, 3, 1), (1, 1, 0, 1), (0, 0, 3, None), (0, 0, 1, None))
PUSH = {0: (0, 8), 1: (2, 12), 2: (3, 3), 3: (2, 5)}
TAKE = {0: (0, 10), 1: (2, 6), 2: (2, 2), 3: (0, 1)}
SENDS = {(3, 0): ((1, 2, 0, False, None), (0, 0, 1, False, 1), (2, 2, 1, False, 0)), (3, 1): ((2, 2, 0, False, 0), (0, 0, 0, True, 1), (1, 0, 2, False, None)), (2, 0): ((1, 1, 1, True, 0), (0, 1, 0, False, None)), (2, 1): ((1, 1, 0, False, 0), (0, 3, 0, False, None)), (1, 0): ((0, 0, 0, True, 0),), (1, 1): ((0, 0, 1, False, 0),)}
RELAY = {(3, 1): (3, 0), (2, 0): (8, 0), (1, 0): (8, 0), (0, 1): (7, 2)}
FINISH = {(3, 0): (1, ()), (3, 1): (1, ()), (2, 0): (7, (1,)), (2, 1): (5, (0,)), (1, 0): (10, (1,)), (1, 1): (10, (0, 1)), (0, 0): (10, (0, 1)), (0, 1): (9, (0, 1))}
LAG_MAX = 10
FINISH_LATE = {(1, 1): (1,)}
TURNED, TURN, TURN_LAG = (3, 1, 1), (2, 1), 4


def attention_kernel(n_dev, n_heads, *refs):
    (q_ref, g_ref, k_ref, v_ref, doc_ref, o_ref, dq_ref, dk_ref, dv_ref, near_ref, far_ref, own_ref,
     kv, rx0, rx1, rx2, acc, part, prx, qg, odq, pb, dsb, fin_k, fin_v, own, docs, kdoc, odoc, vis,
     load_sem, doc_tx, doc_rx, kv_tx, kv_rx, kvp_tx, kvp_rx, qg_sem, odq_sem,
     part_tx, prx_sem, rx_sem, tx_sem, fwd_tx, late_sem) = refs
    rx = (rx0, rx1, rx2)
    n_seq, n_rows, head_dim = q_ref.shape
    piece = k_ref.shape[1]
    two = 2 * piece
    n_chip = n_dev // 2
    scale = head_dim ** -0.5
    me = lax.axis_index('cp')
    chip = me // 2
    core = me % 2
    partner = chip * 2 + (1 - core)

    def dev(c):
        return {'cp': c * 2 + core}

    def remote(src, dst, tx, rx, to):
        return pltpu.make_async_remote_copy(src_ref=src, dst_ref=dst, send_sem=tx, recv_sem=rx,
                                            device_id=to, device_id_type=MESH)

    def local_wait(ref, sem):
        pltpu.make_async_copy(ref, ref, sem).wait()

    barrier = pltpu.get_barrier_semaphore()
    for hop in range(1, n_dev):
        pl.semaphore_signal(barrier, inc=1, device_id={'cp': (me + hop) % n_dev}, device_id_type=MESH)

    def own_copies(lo, n, sem):
        seqs = pl.ds(lo, n)
        return (pltpu.make_async_copy(k_ref.at[seqs], kv.at[seqs, 0, chip, core], load_sem.at[sem]),
                pltpu.make_async_copy(v_ref.at[seqs], kv.at[seqs, 1, chip, core], load_sem.at[sem + 1]))

    own_d = pltpu.make_async_copy(doc_ref, docs.at[me], load_sem.at[4])
    own_first = own_copies(0, N_FIRST, 0)
    own_rest = own_copies(N_FIRST, n_seq - N_FIRST, 2)
    for copy in (*own_first, own_d, *own_rest):
        copy.start()

    def qg_start(b):
        pltpu.make_async_copy(q_ref.at[b], qg.at[b % 2, 0], qg_sem.at[b % 2]).start()
        pltpu.make_async_copy(g_ref.at[b], qg.at[b % 2, 1], qg_sem.at[b % 2]).start()

    def odq_start(b):
        pltpu.make_async_copy(odq.at[b % 2, 0], o_ref.at[b], odq_sem.at[b % 2]).start()
        pltpu.make_async_copy(odq.at[b % 2, 1], dq_ref.at[b], odq_sem.at[b % 2]).start()

    def odq_wait(b):
        local_wait(odq.at[b % 2], odq_sem.at[b % 2])

    qg_start(0)
    for copy in (*own_first, own_d):
        copy.wait()
    odoc[...] = docs[me].reshape(n_seq, 1, piece)
    pl.semaphore_wait(barrier, n_dev - 1)

    def run_chip(c):
        n_key = two * (c + 1)
        here = pl.ds(0, c + 1)
        first_late = n_seq - N_LATE
        first_turn = n_seq - N_TURN

        def doc_copy(to):
            return remote(docs.at[me], docs.at[me], doc_tx, doc_rx, to)

        doc_dests = [{'cp': partner}] + [{'cp': d} for d in range(two // piece * (c + 1), n_dev)]

        flows = [hop[1:] for hop in HOPS if hop[0] == c]
        through = [src for src, _, _ in flows if src > c]

        def by_core(who, fn):
            if who is None:
                fn()
            else:
                pl.when(core == who)(fn)

        def kv_sem(src, to, b):
            return kv_rx.at[0 if to == n_chip - 1 else src, b]

        def kv_copy(i, b):
            src, to, _ = flows[i]
            blk = kv.at[b, :, src, core]
            return remote(blk, blk, kv_tx.at[i], kv_sem(src, to, b), dev(to))

        def kvp_copy(b):
            blk = kv.at[b, :, here, core]
            return remote(blk, blk, kvp_tx, kvp_rx.at[b], {'cp': partner})

        def send_on(src, b):
            for i, (s, _, who) in enumerate(flows):
                if s == src:
                    by_core(who, lambda: kv_copy(i, b).start())

        def push(b):
            send_on(c, b)

        def take(b):
            if c == n_chip - 1:
                local_wait(kv.at[b, :, pl.ds(0, c), core], kv_rx.at[0, b])
            else:
                for src in range(c - 1, -1, -1):
                    local_wait(kv.at[b, :, src, core], kv_rx.at[src, b])
                    send_on(src, b)
            kvp_copy(b).start()
            for src in through:
                who = [w for s, _, w in flows if s == src][0]

                def pass_on():
                    local_wait(kv.at[b, :, src, core], kv_rx.at[src, b])
                    for i, (s, _, _) in enumerate(flows):
                        if s == src:
                            kv_copy(i, b).start()

                by_core(who, pass_on)

        def ramp(lead, fn):
            first, most = lead
            start = min(first, most)

            def at_step(t):
                b = jnp.minimum(start + 2 * t, t + most)
                pl.when(b < n_seq)(lambda: fn(b))
                if most - start > 0:
                    pl.when(t < most - start)(lambda: fn(b + 1))

            return start, at_step

        def arrived(b):
            local_wait(kv.at[b, :, here, 1 - core], kvp_rx.at[b])

        n_push, push_at = ramp(PUSH[c], push)
        n_take, take_at = ramp(TAKE[c], take)
        for b in range(n_push):
            if b == N_FIRST:
                for copy in own_rest:
                    copy.wait()
            push(b)
        if n_push <= N_FIRST:
            for copy in own_rest:
                copy.wait()
        for to in doc_dests:
            doc_copy(to).start()
        for b in range(n_take):
            take(b)

        n_doc = 2 * c + 1
        pltpu.make_async_copy(docs.at[pl.ds(0, n_doc)], docs.at[pl.ds(0, n_doc)], doc_rx).wait()
        for p in range(2 * c + 2):
            kdoc[:, :, p * piece:(p + 1) * piece] = docs[p].reshape(n_seq, 1, piece)

        def compute(b):
            slot = b % 2
            keys = kv[b, 0, here].reshape(n_key, head_dim)
            vals = kv[b, 1, here].reshape(n_key, head_dim)
            tok = lax.broadcasted_iota(jnp.int32, (piece, piece), 0)
            tok_t = lax.broadcasted_iota(jnp.int32, (piece, piece), 1)
            own_doc = odoc[b]
            q_doc = jnp.sum(jnp.where(tok == tok_t, own_doc, 0), axis=1, keepdims=True)
            key_doc = kdoc[b, :, 0:n_key]
            q_pos = me * piece + lax.broadcasted_iota(jnp.int32, (piece, n_key), 0)
            k_pos = lax.broadcasted_iota(jnp.int32, (piece, n_key), 1)
            seen = (q_doc == key_doc) & (k_pos <= q_pos)
            vis[:, 0:n_key] = jnp.where(seen, 0.0, HIDDEN)
            nt = (((1,), (1,)), ((), ()))
            tn = (((0,), (0,)), ((), ()))
            f32 = jnp.float32
            s = lax.dot_general(qg[slot, 0], keys, nt, preferred_element_type=f32)
            dp = lax.dot_general(qg[slot, 1], vals, nt, preferred_element_type=f32)
            s = s.reshape(piece, n_heads, n_key) * (scale * LOG2E) + vis[:, 0:n_key].reshape(piece, 1, n_key)
            s = s.reshape(n_rows, n_key)
            e = jnp.exp2(s - jnp.max(s, axis=1, keepdims=True))
            p = e * (1.0 / jnp.sum(e, axis=1, keepdims=True))
            pb[:, 0:n_key] = p.astype(jnp.bfloat16)
            o16 = jnp.dot(pb[:, 0:n_key], vals, preferred_element_type=f32).astype(jnp.bfloat16)
            dv = lax.dot_general(pb[:, 0:n_key], qg[slot, 1], tn, preferred_element_type=f32)
            odq[slot, 0] = o16
            delta = jnp.sum(qg[slot, 1].astype(f32) * o16.astype(f32), axis=1, keepdims=True)
            dsb[:, 0:n_key] = (p * (dp - delta)).astype(jnp.bfloat16)
            dq = jnp.dot(dsb[:, 0:n_key], keys, preferred_element_type=f32)
            odq[slot, 1] = (dq * scale).astype(jnp.bfloat16)
            dk = lax.dot_general(dsb[:, 0:n_key], qg[slot, 0], tn, preferred_element_type=f32)
            for a in range(c + 1):
                for p in range(2):
                    rows = slice((2 * a + p) * piece, (2 * a + p + 1) * piece)
                    part[slot, p, a, 0:piece, :] = dk[rows]
                    part[slot, p, a, piece:two, :] = dv[rows]

        def part_copy(b):
            return remote(part.at[b % 2, 1 - core, here], prx.at[b % NPRX, here], part_tx.at[b % 2],
                          prx_sem.at[b % NPRX], {'cp': partner})

        def unit_send(b, e, i):
            a, to, buf, _, late = SENDS[c, e][i]
            unit = acc.at[b % NACC, a]
            sem = tx_sem.at[b % NACC]

            def now(to=to, buf=buf):
                remote(unit, rx[buf].at[b], sem, rx_sem.at[buf, b], dev(to)).start()

            if (c, e, a) == TURNED:
                pl.when(b < first_turn)(now)
                pl.when(b >= first_turn)(lambda: now(*TURN))
            elif late is None:
                now()
            else:
                pl.when(b < first_late)(now)

                @pl.when(b >= first_late)
                def _():
                    pltpu.make_async_copy(unit, (near_ref, far_ref)[late].at[b - first_late], sem).start()

        def got(buf, b):
            local_wait(rx[buf].at[b], rx_sem.at[buf, b])

        def merge_partner(b):
            local_wait(prx.at[b % NPRX, here], prx_sem.at[b % NPRX])
            acc[b % NACC, here] = part[b % 2, core, here] + prx[b % NPRX, here]
            for e in range(2):
                sends = [i for i, s in enumerate(SENDS.get((c, e), ())) if not s[3]]
                if sends:
                    @pl.when(core == e)
                    def _():
                        for i in sends:
                            if (c, e, SENDS[c, e][i][0]) == (TURN[0], TURNED[1], TURNED[2]):
                                pl.when(b < first_turn)(lambda: unit_send(b, e, i))
                            else:
                                unit_send(b, e, i)

        def relay(b, e):
            buf = RELAY[c, e][1]

            def take_in():
                got(buf, b)
                if c == 0:
                    fwd_copy(b).start()
                    return
                for i, (a, _, _, after, _) in enumerate(SENDS[c, e]):
                    if after:
                        acc[b % NACC, a] = acc[b % NACC, a] + rx[buf][b]
                        unit_send(b, e, i)

            if c == 0:
                pl.when(b < first_turn)(take_in)
            else:
                take_in()

        def add_turned(b):
            got(TURN[1], b)
            a = TURNED[2]
            acc[b % NACC, a] = acc[b % NACC, a] + rx[TURN[1]][b]
            unit_send(b, TURNED[1], [s[0] for s in SENDS[c, TURNED[1]]].index(a))

        def fwd_copy(b):
            return remote(rx2.at[b], rx1.at[b], fwd_tx, rx_sem.at[1, b], dev(1))

        def finish(b, e):
            def total(bufs):
                out = acc[b % NACC, c]
                for buf in bufs:
                    got(buf, b)
                    out = out + rx[buf][b]
                return out

            @pl.when(b < first_late)
            def _():
                out = total(FINISH[c, e][1])
                fin_k[b] = (out[0:piece] * scale).astype(jnp.bfloat16)
                fin_v[b] = out[piece:two].astype(jnp.bfloat16)

            @pl.when((b >= first_late) & (b < first_turn))
            def _():
                own[b - first_late] = total(FINISH_LATE.get((c, e), ()))

            @pl.when(b >= first_turn)
            def _():
                own[b - first_late] = total(())

        n_step = n_seq + LAG_MAX

        def when_seq(b, fn):
            pl.when((b >= 0) & (b < n_seq))(lambda: fn(b))

        def sent(b):
            for e in range(2):
                n = len(SENDS.get((c, e), ()))
                if n:
                    pl.when(core == e)(lambda: local_wait(acc.at[b % NACC, pl.ds(0, n)], tx_sem.at[b % NACC]))

        def step(t, carry):
            @pl.when(t < n_seq)
            def _():
                push_at(t)
                take_at(t)

                @pl.when(t + 1 < n_seq)
                def _():
                    qg_start(t + 1)

                @pl.when(t >= 2)
                def _():
                    odq_wait(t - 2)
                    part_copy(t - 2).wait_send()

                pl.when(t >= NACC)(lambda: sent(t - NACC))
                arrived(t)
                local_wait(qg.at[t % 2], qg_sem.at[t % 2])
                compute(t)
                odq_start(t)
                part_copy(t).start()

            when_seq(t - 1, merge_partner)
            for e in range(2):
                @pl.when(core == e)
                def _():
                    if (c, e) in RELAY:
                        when_seq(t - RELAY[c, e][0], lambda b: relay(b, e))
                    if (c, e) == (TURN[0], TURNED[1]):
                        b_turn = t - TURN_LAG
                        pl.when((b_turn >= first_turn) & (b_turn < n_seq))(lambda: add_turned(b_turn))
                    when_seq(t - FINISH[c, e][0], lambda b: finish(b, e))
            return carry

        lax.fori_loop(0, n_step, step, 0)

        for b in (n_seq - 2, n_seq - 1):
            odq_wait(b)
            part_copy(b).wait_send()
        for b in range(n_seq - NACC, n_seq):
            sent(b)
        whole = kv.at[:, :, 0, 0]
        for i, (_, _, who) in enumerate(flows):
            by_core(who, lambda: local_wait(whole, kv_tx.at[i]))
        local_wait(kv.at[:, :, here, 0], kvp_tx)
        for to in doc_dests:
            doc_copy(to).wait_send()
        if c == 0:
            pl.when(core == 1)(lambda: local_wait(rx2.at[pl.ds(0, first_turn)], fwd_tx))

    for c in range(n_chip):
        pl.when(chip == c)(functools.partial(run_chip, c))

    out_k = pltpu.make_async_copy(fin_k, dk_ref, load_sem.at[0])
    out_v = pltpu.make_async_copy(fin_v, dv_ref, load_sem.at[1])
    out_own = pltpu.make_async_copy(own, own_ref, late_sem)
    out_k.start()
    out_v.start()
    out_own.start()
    out_k.wait()
    out_v.wait()
    out_own.wait()


def copy_kernel(a_ref, b_ref, k_ref, v_ref, a_out, b_out, k_out, v_out, buf, in_sem, out_sem, k_buf, v_buf, kv_sem):
    n_buf, n_block = buf.shape[:2]
    total = 2 * a_ref.shape[0] // n_block
    ahead = n_buf // 2

    def read(i):
        src = (a_ref, b_ref)[i % 2].at[pl.ds(i // 2 * n_block, n_block)]
        return pltpu.make_async_copy(src, buf.at[i % n_buf], in_sem.at[i % n_buf])

    def write(i):
        dst = (a_out, b_out)[i % 2].at[pl.ds(i // 2 * n_block, n_block)]
        return pltpu.make_async_copy(buf.at[i % n_buf], dst, out_sem.at[i % n_buf])

    rows = pl.ds(0, k_ref.shape[0])
    small_in = [pltpu.make_async_copy(k_ref, k_buf, kv_sem.at[0]), pltpu.make_async_copy(v_ref, v_buf, kv_sem.at[1])]
    small_out = [pltpu.make_async_copy(k_buf, k_out.at[rows], kv_sem.at[0]),
                 pltpu.make_async_copy(v_buf, v_out.at[rows], kv_sem.at[1])]

    for i in range(ahead):
        read(i).start()
    for copy in small_in:
        copy.start()
    for i in range(total):
        if i + ahead < total:
            if i + ahead >= n_buf:
                write(i + ahead - n_buf).wait()
            read(i + ahead).start()
        read(i).wait()
        write(i).start()
        if i == ahead:
            for copy in small_in:
                copy.wait()
            for copy in small_out:
                copy.start()
    for i in range(max(total - n_buf, 0), total):
        write(i).wait()
    for copy in small_out:
        copy.wait()


def solution(mesh):
    n_dev = mesh.shape['cp']
    seq_spec = P('dp', 'cp', None, None)

    def per_device(query, keys, values, grad_out, doc_id):
        n_seq, piece, n_heads, head_dim = query.shape
        n_rows = piece * n_heads
        n_key = piece * n_dev
        two = 2 * piece
        rows_shape = (n_seq, n_rows, head_dim)
        kv_shape = (n_seq, piece, head_dim)
        late_shape = (N_LATE, two, head_dim)
        main_shape = (n_seq - N_LATE, piece, head_dim)
        bf16, f32, i32 = jnp.bfloat16, jnp.float32, jnp.int32
        dma = pltpu.SemaphoreType.DMA
        any_spec = pl.BlockSpec(memory_space=pl.ANY)
        n_chip = n_dev // 2
        out = pl.pallas_call(
            functools.partial(attention_kernel, n_dev, n_heads),
            name='attention',
            out_shape=[jax.ShapeDtypeStruct(rows_shape, bf16)] * 2 + [jax.ShapeDtypeStruct(main_shape, bf16)] * 2
            + [jax.ShapeDtypeStruct(late_shape, f32)] * 3,
            in_specs=[any_spec] * 5,
            out_specs=[any_spec] * 7,
            scratch_shapes=[
                pltpu.VMEM((n_seq, 2, n_chip, 2, piece, head_dim), bf16),
                pltpu.VMEM((n_seq, two, head_dim), f32),
                pltpu.VMEM((n_seq, two, head_dim), f32),
                pltpu.VMEM((n_seq, two, head_dim), f32),
                pltpu.VMEM((NACC, n_chip, two, head_dim), f32),
                pltpu.VMEM((2, 2, n_chip, two, head_dim), f32),
                pltpu.VMEM((NPRX, n_chip, two, head_dim), f32),
                pltpu.VMEM((2, 2, n_rows, head_dim), bf16),
                pltpu.VMEM((2, 2, n_rows, head_dim), bf16),
                pltpu.VMEM((n_rows, n_key), bf16),
                pltpu.VMEM((n_rows, n_key), bf16),
                pltpu.VMEM(main_shape, bf16),
                pltpu.VMEM(main_shape, bf16),
                pltpu.VMEM(late_shape, f32),
                pltpu.VMEM((n_dev, n_seq, piece), i32),
                pltpu.VMEM((n_seq, 1, n_key), i32),
                pltpu.VMEM((n_seq, 1, piece), i32),
                pltpu.VMEM((piece, n_key), f32),
                dma((5,)), dma, dma,
                dma((4,)), dma((n_chip, n_seq)), dma, dma((n_seq,)),
                dma((2,)), dma((2,)),
                dma((2,)), dma((NPRX,)), dma((3, n_seq)), dma((NACC,)), dma, dma,
            ],
            compiler_params=pltpu.CompilerParams(collective_id=0, has_side_effects=True, vmem_limit_bytes=63 * 1024 * 1024),
        )(query.reshape(rows_shape), grad_out.reshape(rows_shape), keys.reshape(kv_shape), values.reshape(kv_shape), doc_id)
        attn_out, grad_query, grad_keys, grad_values, near, far, own = out
        attn_out, grad_query, grad_keys, grad_values = pl.pallas_call(
            copy_kernel,
            name='results',
            out_shape=[jax.ShapeDtypeStruct(rows_shape, bf16)] * 2 + [jax.ShapeDtypeStruct(kv_shape, bf16)] * 2,
            in_specs=[pl.BlockSpec(memory_space=pltpu.HBM)] * 4,
            out_specs=[pl.BlockSpec(memory_space=pltpu.HBM)] * 4,
            scratch_shapes=[pltpu.VMEM((N_COPY, COPY_BLOCK, n_rows, head_dim), bf16), dma((N_COPY,)), dma((N_COPY,)),
                            pltpu.VMEM(main_shape, bf16), pltpu.VMEM(main_shape, bf16), dma((2,))],
            compiler_params=pltpu.CompilerParams(vmem_limit_bytes=40 * 1024 * 1024),
            cost_estimate=pl.CostEstimate(flops=12_000_000_000, bytes_accessed=8 * n_seq * n_rows * head_dim,
                                          transcendentals=0),
        )(attn_out, grad_query, grad_keys, grad_values)
        to_near = [(d, d - 2) for d in range(2, n_dev)]
        to_far = [(n_dev - 2 + e, e) for e in range(2)]
        from_far = lax.ppermute(far, 'cp', to_far)
        from_near = lax.ppermute(near, 'cp', to_near)
        late = own + from_far + from_near
        late_keys = (late[:, 0:piece] * head_dim ** -0.5).astype(bf16)
        late_values = late[:, piece:two].astype(bf16)
        grad_keys = lax.dynamic_update_slice(grad_keys, late_keys, (n_seq - N_LATE, 0, 0))
        grad_values = lax.dynamic_update_slice(grad_values, late_values, (n_seq - N_LATE, 0, 0))
        return (attn_out.reshape(query.shape), grad_query.reshape(query.shape),
                grad_keys.reshape(keys.shape), grad_values.reshape(values.shape))

    return jax.shard_map(per_device, mesh=mesh, in_specs=(seq_spec,) * 4 + (P('dp', 'cp'),), out_specs=(seq_spec,) * 4, check_vma=False)
```

```python
import functools

import jax
import jax.numpy as jnp
from jax import lax
from jax.experimental import pallas as pl
from jax.experimental.pallas import tpu as pltpu
from jax.sharding import PartitionSpec as P

MESH = pl.DeviceIdType.MESH
LOG2E = 1.4426950408889634
HIDDEN = -3.0e38
NACC = 12
NPRX = 4
COPY_BLOCK = 2
N_COPY = 32
N_FIRST = 1
N_TURN = 3
N_LATE = 9


HOPS = ((1, 1, 2, None), (1, 0, 2, None), (2, 1, 3, 0), (2, 2, 3, None), (0, 1, 3, 1), (1, 1, 0, 1), (0, 0, 3, None), (0, 0, 1, None))
PUSH = {0: (0, 8), 1: (2, 12), 2: (3, 3), 3: (2, 5)}
TAKE = {0: (0, 10), 1: (2, 6), 2: (2, 2), 3: (0, 1)}
SENDS = {(3, 0): ((1, 2, 0, False, None), (0, 0, 1, False, 1), (2, 2, 1, False, 0)), (3, 1): ((2, 2, 0, False, 0), (0, 0, 0, True, 1), (1, 0, 2, False, None)), (2, 0): ((1, 1, 1, True, 0), (0, 1, 0, False, None)), (2, 1): ((1, 1, 0, False, 0), (0, 3, 0, False, None)), (1, 0): ((0, 0, 0, True, 0),), (1, 1): ((0, 0, 1, False, 0),)}
RELAY = {(3, 1): (3, 0), (2, 0): (8, 0), (1, 0): (8, 0), (0, 1): (7, 2)}
FINISH = {(3, 0): (1, ()), (3, 1): (1, ()), (2, 0): (7, (1,)), (2, 1): (5, (0,)), (1, 0): (10, (1,)), (1, 1): (10, (0, 1)), (0, 0): (10, (0, 1)), (0, 1): (9, (0, 1))}
LAG_MAX = 10
FINISH_LATE = {(1, 1): (1,)}
TURNED, TURN, TURN_LAG = (3, 1, 1), (2, 1), 4


def attention_kernel(n_dev, n_heads, *refs):
    (q_ref, g_ref, k_ref, v_ref, doc_ref, o_ref, dq_ref, dk_ref, dv_ref, near_ref, far_ref, own_ref,
     kv, rx0, rx1, rx2, acc, part, prx, qg, odq, pb, dsb, fin_k, fin_v, own, docs, kdoc, odoc, vis,
     load_sem, doc_tx, doc_rx, kv_tx, kv_rx, kvp_tx, kvp_rx, qg_sem, odq_sem,
     part_tx, prx_sem, rx_sem, tx_sem, fwd_tx, late_sem) = refs
    rx = (rx0, rx1, rx2)
    n_seq, n_rows, head_dim = q_ref.shape
    piece = k_ref.shape[1]
    two = 2 * piece
    n_chip = n_dev // 2
    scale = head_dim ** -0.5
    me = lax.axis_index('cp')
    chip = me // 2
    core = me % 2
    partner = chip * 2 + (1 - core)

    def dev(c):
        return {'cp': c * 2 + core}

    def remote(src, dst, tx, rx, to):
        return pltpu.make_async_remote_copy(src_ref=src, dst_ref=dst, send_sem=tx, recv_sem=rx,
                                            device_id=to, device_id_type=MESH)

    def local_wait(ref, sem):
        pltpu.make_async_copy(ref, ref, sem).wait()

    barrier = pltpu.get_barrier_semaphore()
    for hop in range(1, n_dev):
        pl.semaphore_signal(barrier, inc=1, device_id={'cp': (me + hop) % n_dev}, device_id_type=MESH)

    def own_copies(lo, n, sem):
        seqs = pl.ds(lo, n)
        return (pltpu.make_async_copy(k_ref.at[seqs], kv.at[seqs, 0, chip, core], load_sem.at[sem]),
                pltpu.make_async_copy(v_ref.at[seqs], kv.at[seqs, 1, chip, core], load_sem.at[sem + 1]))

    own_d = pltpu.make_async_copy(doc_ref, docs.at[me], load_sem.at[4])
    own_first = own_copies(0, N_FIRST, 0)
    own_rest = own_copies(N_FIRST, n_seq - N_FIRST, 2)
    for copy in (*own_first, own_d, *own_rest):
        copy.start()

    def qg_start(b):
        pltpu.make_async_copy(q_ref.at[b], qg.at[b % 2, 0], qg_sem.at[b % 2]).start()
        pltpu.make_async_copy(g_ref.at[b], qg.at[b % 2, 1], qg_sem.at[b % 2]).start()

    def odq_start(b):
        pltpu.make_async_copy(odq.at[b % 2, 0], o_ref.at[b], odq_sem.at[b % 2]).start()
        pltpu.make_async_copy(odq.at[b % 2, 1], dq_ref.at[b], odq_sem.at[b % 2]).start()

    def odq_wait(b):
        local_wait(odq.at[b % 2], odq_sem.at[b % 2])

    qg_start(0)
    for copy in (*own_first, own_d):
        copy.wait()
    odoc[...] = docs[me].reshape(n_seq, 1, piece)
    pl.semaphore_wait(barrier, n_dev - 1)

    def run_chip(c):
        n_key = two * (c + 1)
        here = pl.ds(0, c + 1)
        first_late = n_seq - N_LATE
        first_turn = n_seq - N_TURN

        def doc_copy(to):
            return remote(docs.at[me], docs.at[me], doc_tx, doc_rx, to)

        doc_dests = [{'cp': partner}] + [{'cp': d} for d in range(two // piece * (c + 1), n_dev)]

        flows = [hop[1:] for hop in HOPS if hop[0] == c]
        through = [src for src, _, _ in flows if src > c]

        def by_core(who, fn):
            if who is None:
                fn()
            else:
                pl.when(core == who)(fn)

        def kv_sem(src, to, b):
            return kv_rx.at[0 if to == n_chip - 1 else src, b]

        def kv_copy(i, b):
            src, to, _ = flows[i]
            blk = kv.at[b, :, src, core]
            return remote(blk, blk, kv_tx.at[i], kv_sem(src, to, b), dev(to))

        def kvp_copy(b):
            blk = kv.at[b, :, here, core]
            return remote(blk, blk, kvp_tx, kvp_rx.at[b], {'cp': partner})

        def send_on(src, b):
            for i, (s, _, who) in enumerate(flows):
                if s == src:
                    by_core(who, lambda: kv_copy(i, b).start())

        def push(b):
            send_on(c, b)

        def take(b):
            if c == n_chip - 1:
                local_wait(kv.at[b, :, pl.ds(0, c), core], kv_rx.at[0, b])
            else:
                for src in range(c - 1, -1, -1):
                    local_wait(kv.at[b, :, src, core], kv_rx.at[src, b])
                    send_on(src, b)
            kvp_copy(b).start()
            for src in through:
                who = [w for s, _, w in flows if s == src][0]

                def pass_on():
                    local_wait(kv.at[b, :, src, core], kv_rx.at[src, b])
                    for i, (s, _, _) in enumerate(flows):
                        if s == src:
                            kv_copy(i, b).start()

                by_core(who, pass_on)

        def ramp(lead, fn):
            first, most = lead
            start = min(first, most)

            def at_step(t):
                b = jnp.minimum(start + 2 * t, t + most)
                pl.when(b < n_seq)(lambda: fn(b))
                if most - start > 0:
                    pl.when(t < most - start)(lambda: fn(b + 1))

            return start, at_step

        def arrived(b):
            local_wait(kv.at[b, :, here, 1 - core], kvp_rx.at[b])

        n_push, push_at = ramp(PUSH[c], push)
        n_take, take_at = ramp(TAKE[c], take)
        for b in range(n_push):
            if b == N_FIRST:
                for copy in own_rest:
                    copy.wait()
            push(b)
        if n_push <= N_FIRST:
            for copy in own_rest:
                copy.wait()
        for to in doc_dests:
            doc_copy(to).start()
        for b in range(n_take):
            take(b)

        n_doc = 2 * c + 1
        pltpu.make_async_copy(docs.at[pl.ds(0, n_doc)], docs.at[pl.ds(0, n_doc)], doc_rx).wait()
        for p in range(2 * c + 2):
            kdoc[:, :, p * piece:(p + 1) * piece] = docs[p].reshape(n_seq, 1, piece)

        def compute(b):
            slot = b % 2
            keys = kv[b, 0, here].reshape(n_key, head_dim)
            vals = kv[b, 1, here].reshape(n_key, head_dim)
            tok = lax.broadcasted_iota(jnp.int32, (piece, piece), 0)
            tok_t = lax.broadcasted_iota(jnp.int32, (piece, piece), 1)
            own_doc = odoc[b]
            q_doc = jnp.sum(jnp.where(tok == tok_t, own_doc, 0), axis=1, keepdims=True)
            key_doc = kdoc[b, :, 0:n_key]
            q_pos = me * piece + lax.broadcasted_iota(jnp.int32, (piece, n_key), 0)
            k_pos = lax.broadcasted_iota(jnp.int32, (piece, n_key), 1)
            seen = (q_doc == key_doc) & (k_pos <= q_pos)
            vis[:, 0:n_key] = jnp.where(seen, 0.0, HIDDEN)
            nt = (((1,), (1,)), ((), ()))
            tn = (((0,), (0,)), ((), ()))
            f32 = jnp.float32
            s = lax.dot_general(qg[slot, 0], keys, nt, preferred_element_type=f32)
            dp = lax.dot_general(qg[slot, 1], vals, nt, preferred_element_type=f32)
            s = s.reshape(piece, n_heads, n_key) * (scale * LOG2E) + vis[:, 0:n_key].reshape(piece, 1, n_key)
            s = s.reshape(n_rows, n_key)
            e = jnp.exp2(s - jnp.max(s, axis=1, keepdims=True))
            p = e * (1.0 / jnp.sum(e, axis=1, keepdims=True))
            pb[:, 0:n_key] = p.astype(jnp.bfloat16)
            o16 = jnp.dot(pb[:, 0:n_key], vals, preferred_element_type=f32).astype(jnp.bfloat16)
            dv = lax.dot_general(pb[:, 0:n_key], qg[slot, 1], tn, preferred_element_type=f32)
            odq[slot, 0] = o16
            delta = jnp.sum(qg[slot, 1].astype(f32) * o16.astype(f32), axis=1, keepdims=True)
            dsb[:, 0:n_key] = (p * (dp - delta)).astype(jnp.bfloat16)
            dq = jnp.dot(dsb[:, 0:n_key], keys, preferred_element_type=f32)
            odq[slot, 1] = (dq * scale).astype(jnp.bfloat16)
            dk = lax.dot_general(dsb[:, 0:n_key], qg[slot, 0], tn, preferred_element_type=f32)
            for a in range(c + 1):
                for p in range(2):
                    rows = slice((2 * a + p) * piece, (2 * a + p + 1) * piece)
                    part[slot, p, a, 0:piece, :] = dk[rows]
                    part[slot, p, a, piece:two, :] = dv[rows]

        def part_copy(b):
            return remote(part.at[b % 2, 1 - core, here], prx.at[b % NPRX, here], part_tx.at[b % 2],
                          prx_sem.at[b % NPRX], {'cp': partner})

        def unit_send(b, e, i):
            a, to, buf, _, late = SENDS[c, e][i]
            unit = acc.at[b % NACC, a]
            sem = tx_sem.at[b % NACC]

            def now(to=to, buf=buf):
                remote(unit, rx[buf].at[b], sem, rx_sem.at[buf, b], dev(to)).start()

            if (c, e, a) == TURNED:
                pl.when(b < first_turn)(now)
                pl.when(b >= first_turn)(lambda: now(*TURN))
            elif late is None:
                now()
            else:
                pl.when(b < first_late)(now)

                @pl.when(b >= first_late)
                def _():
                    pltpu.make_async_copy(unit, (near_ref, far_ref)[late].at[b - first_late], sem).start()

        def got(buf, b):
            local_wait(rx[buf].at[b], rx_sem.at[buf, b])

        def merge_partner(b):
            local_wait(prx.at[b % NPRX, here], prx_sem.at[b % NPRX])
            acc[b % NACC, here] = part[b % 2, core, here] + prx[b % NPRX, here]
            for e in range(2):
                sends = [i for i, s in enumerate(SENDS.get((c, e), ())) if not s[3]]
                if sends:
                    @pl.when(core == e)
                    def _():
                        for i in sends:
                            if (c, e, SENDS[c, e][i][0]) == (TURN[0], TURNED[1], TURNED[2]):
                                pl.when(b < first_turn)(lambda: unit_send(b, e, i))
                            else:
                                unit_send(b, e, i)

        def relay(b, e):
            buf = RELAY[c, e][1]

            def take_in():
                got(buf, b)
                if c == 0:
                    fwd_copy(b).start()
                    return
                for i, (a, _, _, after, _) in enumerate(SENDS[c, e]):
                    if after:
                        acc[b % NACC, a] = acc[b % NACC, a] + rx[buf][b]
                        unit_send(b, e, i)

            if c == 0:
                pl.when(b < first_turn)(take_in)
            else:
                take_in()

        def add_turned(b):
            got(TURN[1], b)
            a = TURNED[2]
            acc[b % NACC, a] = acc[b % NACC, a] + rx[TURN[1]][b]
            unit_send(b, TURNED[1], [s[0] for s in SENDS[c, TURNED[1]]].index(a))

        def fwd_copy(b):
            return remote(rx2.at[b], rx1.at[b], fwd_tx, rx_sem.at[1, b], dev(1))

        def finish(b, e):
            def total(bufs):
                out = acc[b % NACC, c]
                for buf in bufs:
                    got(buf, b)
                    out = out + rx[buf][b]
                return out

            @pl.when(b < first_late)
            def _():
                out = total(FINISH[c, e][1])
                fin_k[b] = (out[0:piece] * scale).astype(jnp.bfloat16)
                fin_v[b] = out[piece:two].astype(jnp.bfloat16)

            @pl.when((b >= first_late) & (b < first_turn))
            def _():
                own[b - first_late] = total(FINISH_LATE.get((c, e), ()))

            @pl.when(b >= first_turn)
            def _():
                own[b - first_late] = total(())

        n_step = n_seq + LAG_MAX

        def when_seq(b, fn):
            pl.when((b >= 0) & (b < n_seq))(lambda: fn(b))

        def sent(b):
            for e in range(2):
                n = len(SENDS.get((c, e), ()))
                if n:
                    pl.when(core == e)(lambda: local_wait(acc.at[b % NACC, pl.ds(0, n)], tx_sem.at[b % NACC]))

        def step(t, carry):
            @pl.when(t < n_seq)
            def _():
                push_at(t)
                take_at(t)

                @pl.when(t + 1 < n_seq)
                def _():
                    qg_start(t + 1)

                @pl.when(t >= 2)
                def _():
                    odq_wait(t - 2)
                    part_copy(t - 2).wait_send()

                pl.when(t >= NACC)(lambda: sent(t - NACC))
                arrived(t)
                local_wait(qg.at[t % 2], qg_sem.at[t % 2])
                compute(t)
                odq_start(t)
                part_copy(t).start()

            when_seq(t - 1, merge_partner)
            for e in range(2):
                @pl.when(core == e)
                def _():
                    if (c, e) in RELAY:
                        when_seq(t - RELAY[c, e][0], lambda b: relay(b, e))
                    if (c, e) == (TURN[0], TURNED[1]):
                        b_turn = t - TURN_LAG
                        pl.when((b_turn >= first_turn) & (b_turn < n_seq))(lambda: add_turned(b_turn))
                    when_seq(t - FINISH[c, e][0], lambda b: finish(b, e))
            return carry

        lax.fori_loop(0, n_step, step, 0)

        for b in (n_seq - 2, n_seq - 1):
            odq_wait(b)
            part_copy(b).wait_send()
        for b in range(n_seq - NACC, n_seq):
            sent(b)
        whole = kv.at[:, :, 0, 0]
        for i, (_, _, who) in enumerate(flows):
            by_core(who, lambda: local_wait(whole, kv_tx.at[i]))
        local_wait(kv.at[:, :, here, 0], kvp_tx)
        for to in doc_dests:
            doc_copy(to).wait_send()
        if c == 0:
            pl.when(core == 1)(lambda: local_wait(rx2.at[pl.ds(0, first_turn)], fwd_tx))

    for c in range(n_chip):
        pl.when(chip == c)(functools.partial(run_chip, c))

    out_k = pltpu.make_async_copy(fin_k, dk_ref, load_sem.at[0])
    out_v = pltpu.make_async_copy(fin_v, dv_ref, load_sem.at[1])
    out_own = pltpu.make_async_copy(own, own_ref, late_sem)
    out_k.start()
    out_v.start()
    out_own.start()
    out_k.wait()
    out_v.wait()
    out_own.wait()


def copy_kernel(a_ref, b_ref, k_ref, v_ref, a_out, b_out, k_out, v_out, buf, in_sem, out_sem, k_buf, v_buf, kv_sem):
    n_buf, n_block = buf.shape[:2]
    total = 2 * a_ref.shape[0] // n_block
    ahead = n_buf // 2

    def read(i):
        src = (a_ref, b_ref)[i % 2].at[pl.ds(i // 2 * n_block, n_block)]
        return pltpu.make_async_copy(src, buf.at[i % n_buf], in_sem.at[i % n_buf])

    def write(i):
        dst = (a_out, b_out)[i % 2].at[pl.ds(i // 2 * n_block, n_block)]
        return pltpu.make_async_copy(buf.at[i % n_buf], dst, out_sem.at[i % n_buf])

    rows = pl.ds(0, k_ref.shape[0])
    small_in = [pltpu.make_async_copy(k_ref, k_buf, kv_sem.at[0]), pltpu.make_async_copy(v_ref, v_buf, kv_sem.at[1])]
    small_out = [pltpu.make_async_copy(k_buf, k_out.at[rows], kv_sem.at[0]),
                 pltpu.make_async_copy(v_buf, v_out.at[rows], kv_sem.at[1])]

    for i in range(ahead):
        read(i).start()
    for copy in small_in:
        copy.start()
    for i in range(total):
        if i + ahead < total:
            if i + ahead >= n_buf:
                write(i + ahead - n_buf).wait()
            read(i + ahead).start()
        read(i).wait()
        write(i).start()
        if i == ahead:
            for copy in small_in:
                copy.wait()
            for copy in small_out:
                copy.start()
    for i in range(max(total - n_buf, 0), total):
        write(i).wait()
    for copy in small_out:
        copy.wait()


def solution(mesh):
    n_dev = mesh.shape['cp']
    seq_spec = P('dp', 'cp', None, None)

    def per_device(query, keys, values, grad_out, doc_id):
        n_seq, piece, n_heads, head_dim = query.shape
        n_rows = piece * n_heads
        n_key = piece * n_dev
        two = 2 * piece
        rows_shape = (n_seq, n_rows, head_dim)
        kv_shape = (n_seq, piece, head_dim)
        late_shape = (N_LATE, two, head_dim)
        main_shape = (n_seq - N_LATE, piece, head_dim)
        bf16, f32, i32 = jnp.bfloat16, jnp.float32, jnp.int32
        dma = pltpu.SemaphoreType.DMA
        any_spec = pl.BlockSpec(memory_space=pl.ANY)
        n_chip = n_dev // 2
        out = pl.pallas_call(
            functools.partial(attention_kernel, n_dev, n_heads),
            name='attention',
            out_shape=[jax.ShapeDtypeStruct(rows_shape, bf16)] * 2 + [jax.ShapeDtypeStruct(main_shape, bf16)] * 2
            + [jax.ShapeDtypeStruct(late_shape, f32)] * 3,
            in_specs=[any_spec] * 5,
            out_specs=[any_spec] * 7,
            scratch_shapes=[
                pltpu.VMEM((n_seq, 2, n_chip, 2, piece, head_dim), bf16),
                pltpu.VMEM((n_seq, two, head_dim), f32),
                pltpu.VMEM((n_seq, two, head_dim), f32),
                pltpu.VMEM((n_seq, two, head_dim), f32),
                pltpu.VMEM((NACC, n_chip, two, head_dim), f32),
                pltpu.VMEM((2, 2, n_chip, two, head_dim), f32),
                pltpu.VMEM((NPRX, n_chip, two, head_dim), f32),
                pltpu.VMEM((2, 2, n_rows, head_dim), bf16),
                pltpu.VMEM((2, 2, n_rows, head_dim), bf16),
                pltpu.VMEM((n_rows, n_key), bf16),
                pltpu.VMEM((n_rows, n_key), bf16),
                pltpu.VMEM(main_shape, bf16),
                pltpu.VMEM(main_shape, bf16),
                pltpu.VMEM(late_shape, f32),
                pltpu.VMEM((n_dev, n_seq, piece), i32),
                pltpu.VMEM((n_seq, 1, n_key), i32),
                pltpu.VMEM((n_seq, 1, piece), i32),
                pltpu.VMEM((piece, n_key), f32),
                dma((5,)), dma, dma,
                dma((4,)), dma((n_chip, n_seq)), dma, dma((n_seq,)),
                dma((2,)), dma((2,)),
                dma((2,)), dma((NPRX,)), dma((3, n_seq)), dma((NACC,)), dma, dma,
            ],
            compiler_params=pltpu.CompilerParams(collective_id=0, has_side_effects=True, vmem_limit_bytes=63 * 1024 * 1024),
        )(query.reshape(rows_shape), grad_out.reshape(rows_shape), keys.reshape(kv_shape), values.reshape(kv_shape), doc_id)
        attn_out, grad_query, grad_keys, grad_values, near, far, own = out
        attn_out, grad_query, grad_keys, grad_values = pl.pallas_call(
            copy_kernel,
            name='results',
            out_shape=[jax.ShapeDtypeStruct(rows_shape, bf16)] * 2 + [jax.ShapeDtypeStruct(kv_shape, bf16)] * 2,
            in_specs=[pl.BlockSpec(memory_space=pltpu.HBM)] * 4,
            out_specs=[pl.BlockSpec(memory_space=pltpu.HBM)] * 4,
            scratch_shapes=[pltpu.VMEM((N_COPY, COPY_BLOCK, n_rows, head_dim), bf16), dma((N_COPY,)), dma((N_COPY,)),
                            pltpu.VMEM(main_shape, bf16), pltpu.VMEM(main_shape, bf16), dma((2,))],
            compiler_params=pltpu.CompilerParams(vmem_limit_bytes=56 * 1024 * 1024),
            cost_estimate=pl.CostEstimate(flops=12_000_000_000, bytes_accessed=8 * n_seq * n_rows * head_dim,
                                          transcendentals=0),
        )(attn_out, grad_query, grad_keys, grad_values)
        to_near = [(d, d - 2) for d in range(2, n_dev)]
        to_far = [(n_dev - 2 + e, e) for e in range(2)]
        from_far = lax.ppermute(far, 'cp', to_far)
        from_near = lax.ppermute(near, 'cp', to_near)
        late = own + from_far + from_near
        late_keys = (late[:, 0:piece] * head_dim ** -0.5).astype(bf16)
        late_values = late[:, piece:two].astype(bf16)
        grad_keys = lax.dynamic_update_slice(grad_keys, late_keys, (n_seq - N_LATE, 0, 0))
        grad_values = lax.dynamic_update_slice(grad_values, late_values, (n_seq - N_LATE, 0, 0))
        return (attn_out.reshape(query.shape), grad_query.reshape(query.shape),
                grad_keys.reshape(keys.shape), grad_values.reshape(values.shape))

    return jax.shard_map(per_device, mesh=mesh, in_specs=(seq_spec,) * 4 + (P('dp', 'cp'),), out_specs=(seq_spec,) * 4, check_vma=False)
```

```python
import functools

import jax
import jax.numpy as jnp
from jax import lax
from jax.experimental import pallas as pl
from jax.experimental.pallas import tpu as pltpu
from jax.sharding import PartitionSpec as P

MESH = pl.DeviceIdType.MESH
LOG2E = 1.4426950408889634
HIDDEN = -3.0e38
NACC = 12
NPRX = 4
COPY_BLOCK = 2
N_COPY = 32
N_FIRST = 1
N_TURN = 2
N_LATE = 9


HOPS = ((1, 1, 2, None), (1, 0, 2, None), (2, 1, 3, 0), (2, 2, 3, None), (0, 1, 3, 1), (1, 1, 0, 1), (0, 0, 3, None), (0, 0, 1, None))
PUSH = {0: (0, 8), 1: (2, 12), 2: (3, 3), 3: (2, 5)}
TAKE = {0: (0, 10), 1: (2, 6), 2: (2, 2), 3: (0, 1)}
SENDS = {(3, 0): ((1, 2, 0, False, None), (0, 0, 1, False, 1), (2, 2, 1, False, 0)), (3, 1): ((2, 2, 0, False, 0), (0, 0, 0, True, 1), (1, 0, 2, False, None)), (2, 0): ((1, 1, 1, True, 0), (0, 1, 0, False, None)), (2, 1): ((1, 1, 0, False, 0), (0, 3, 0, False, None)), (1, 0): ((0, 0, 0, True, 0),), (1, 1): ((0, 0, 1, False, 0),)}
RELAY = {(3, 1): (3, 0), (2, 0): (8, 0), (1, 0): (8, 0), (0, 1): (7, 2)}
FINISH = {(3, 0): (1, ()), (3, 1): (1, ()), (2, 0): (7, (1,)), (2, 1): (5, (0,)), (1, 0): (10, (1,)), (1, 1): (10, (0, 1)), (0, 0): (10, (0, 1)), (0, 1): (9, (0, 1))}
LAG_MAX = 10
FINISH_LATE = {(1, 1): (1,)}
TURNED, TURN, TURN_LAG = (3, 1, 1), (2, 1), 4


def attention_kernel(n_dev, n_heads, *refs):
    (q_ref, g_ref, k_ref, v_ref, doc_ref, o_ref, dq_ref, dk_ref, dv_ref, near_ref, far_ref, own_ref,
     kv, rx0, rx1, rx2, acc, part, prx, qg, odq, pb, dsb, fin_k, fin_v, own, docs, kdoc, odoc, vis,
     load_sem, doc_tx, doc_rx, kv_tx, kv_rx, kvp_tx, kvp_rx, qg_sem, odq_sem,
     part_tx, prx_sem, rx_sem, tx_sem, fwd_tx, late_sem) = refs
    rx = (rx0, rx1, rx2)
    n_seq, n_rows, head_dim = q_ref.shape
    piece = k_ref.shape[1]
    two = 2 * piece
    n_chip = n_dev // 2
    scale = head_dim ** -0.5
    me = lax.axis_index('cp')
    chip = me // 2
    core = me % 2
    partner = chip * 2 + (1 - core)

    def dev(c):
        return {'cp': c * 2 + core}

    def remote(src, dst, tx, rx, to):
        return pltpu.make_async_remote_copy(src_ref=src, dst_ref=dst, send_sem=tx, recv_sem=rx,
                                            device_id=to, device_id_type=MESH)

    def local_wait(ref, sem):
        pltpu.make_async_copy(ref, ref, sem).wait()

    barrier = pltpu.get_barrier_semaphore()
    for hop in range(1, n_dev):
        pl.semaphore_signal(barrier, inc=1, device_id={'cp': (me + hop) % n_dev}, device_id_type=MESH)

    def own_copies(lo, n, sem):
        seqs = pl.ds(lo, n)
        return (pltpu.make_async_copy(k_ref.at[seqs], kv.at[seqs, 0, chip, core], load_sem.at[sem]),
                pltpu.make_async_copy(v_ref.at[seqs], kv.at[seqs, 1, chip, core], load_sem.at[sem + 1]))

    own_d = pltpu.make_async_copy(doc_ref, docs.at[me], load_sem.at[4])
    own_first = own_copies(0, N_FIRST, 0)
    own_rest = own_copies(N_FIRST, n_seq - N_FIRST, 2)
    for copy in (*own_first, own_d, *own_rest):
        copy.start()

    def qg_start(b):
        pltpu.make_async_copy(q_ref.at[b], qg.at[b % 2, 0], qg_sem.at[b % 2]).start()
        pltpu.make_async_copy(g_ref.at[b], qg.at[b % 2, 1], qg_sem.at[b % 2]).start()

    def odq_start(b):
        pltpu.make_async_copy(odq.at[b % 2, 0], o_ref.at[b], odq_sem.at[b % 2]).start()
        pltpu.make_async_copy(odq.at[b % 2, 1], dq_ref.at[b], odq_sem.at[b % 2]).start()

    def odq_wait(b):
        local_wait(odq.at[b % 2], odq_sem.at[b % 2])

    qg_start(0)
    for copy in (*own_first, own_d):
        copy.wait()
    odoc[...] = docs[me].reshape(n_seq, 1, piece)
    pl.semaphore_wait(barrier, n_dev - 1)

    def out_copies():
        return (pltpu.make_async_copy(fin_k, dk_ref, load_sem.at[0]), pltpu.make_async_copy(fin_v, dv_ref, load_sem.at[1]))

    def run_chip(c):
        n_key = two * (c + 1)
        here = pl.ds(0, c + 1)
        first_late = n_seq - N_LATE
        first_turn = n_seq - N_TURN

        def doc_copy(to):
            return remote(docs.at[me], docs.at[me], doc_tx, doc_rx, to)

        doc_dests = [{'cp': partner}] + [{'cp': d} for d in range(two // piece * (c + 1), n_dev)]

        flows = [hop[1:] for hop in HOPS if hop[0] == c]
        through = [src for src, _, _ in flows if src > c]

        def by_core(who, fn):
            if who is None:
                fn()
            else:
                pl.when(core == who)(fn)

        def kv_sem(src, to, b):
            return kv_rx.at[0 if to == n_chip - 1 else src, b]

        def kv_copy(i, b):
            src, to, _ = flows[i]
            blk = kv.at[b, :, src, core]
            return remote(blk, blk, kv_tx.at[i], kv_sem(src, to, b), dev(to))

        def kvp_copy(b):
            blk = kv.at[b, :, here, core]
            return remote(blk, blk, kvp_tx, kvp_rx.at[b], {'cp': partner})

        def send_on(src, b):
            for i, (s, _, who) in enumerate(flows):
                if s == src:
                    by_core(who, lambda: kv_copy(i, b).start())

        def push(b):
            send_on(c, b)

        def take(b):
            if c == n_chip - 1:
                local_wait(kv.at[b, :, pl.ds(0, c), core], kv_rx.at[0, b])
            else:
                for src in range(c - 1, -1, -1):
                    local_wait(kv.at[b, :, src, core], kv_rx.at[src, b])
                    send_on(src, b)
            kvp_copy(b).start()
            for src in through:
                who = [w for s, _, w in flows if s == src][0]

                def pass_on():
                    local_wait(kv.at[b, :, src, core], kv_rx.at[src, b])
                    for i, (s, _, _) in enumerate(flows):
                        if s == src:
                            kv_copy(i, b).start()

                by_core(who, pass_on)

        def ramp(lead, fn):
            first, most = lead
            start = min(first, most)

            def at_step(t):
                b = jnp.minimum(start + 2 * t, t + most)
                pl.when(b < n_seq)(lambda: fn(b))
                if most - start > 0:
                    pl.when(t < most - start)(lambda: fn(b + 1))

            return start, at_step

        def arrived(b):
            local_wait(kv.at[b, :, here, 1 - core], kvp_rx.at[b])

        n_push, push_at = ramp(PUSH[c], push)
        n_take, take_at = ramp(TAKE[c], take)
        for b in range(n_push):
            if b == N_FIRST:
                for copy in own_rest:
                    copy.wait()
            push(b)
        if n_push <= N_FIRST:
            for copy in own_rest:
                copy.wait()
        for to in doc_dests:
            doc_copy(to).start()
        for b in range(n_take):
            take(b)

        n_doc = 2 * c + 1
        pltpu.make_async_copy(docs.at[pl.ds(0, n_doc)], docs.at[pl.ds(0, n_doc)], doc_rx).wait()
        for p in range(2 * c + 2):
            kdoc[:, :, p * piece:(p + 1) * piece] = docs[p].reshape(n_seq, 1, piece)

        def compute(b):
            slot = b % 2
            keys = kv[b, 0, here].reshape(n_key, head_dim)
            vals = kv[b, 1, here].reshape(n_key, head_dim)
            tok = lax.broadcasted_iota(jnp.int32, (piece, piece), 0)
            tok_t = lax.broadcasted_iota(jnp.int32, (piece, piece), 1)
            own_doc = odoc[b]
            q_doc = jnp.sum(jnp.where(tok == tok_t, own_doc, 0), axis=1, keepdims=True)
            key_doc = kdoc[b, :, 0:n_key]
            q_pos = me * piece + lax.broadcasted_iota(jnp.int32, (piece, n_key), 0)
            k_pos = lax.broadcasted_iota(jnp.int32, (piece, n_key), 1)
            seen = (q_doc == key_doc) & (k_pos <= q_pos)
            vis[:, 0:n_key] = jnp.where(seen, 0.0, HIDDEN)
            nt = (((1,), (1,)), ((), ()))
            tn = (((0,), (0,)), ((), ()))
            f32 = jnp.float32
            s = lax.dot_general(qg[slot, 0], keys, nt, preferred_element_type=f32)
            dp = lax.dot_general(qg[slot, 1], vals, nt, preferred_element_type=f32)
            s = s.reshape(piece, n_heads, n_key) * (scale * LOG2E) + vis[:, 0:n_key].reshape(piece, 1, n_key)
            s = s.reshape(n_rows, n_key)
            e = jnp.exp2(s - jnp.max(s, axis=1, keepdims=True))
            p = e * (1.0 / jnp.sum(e, axis=1, keepdims=True))
            pb[:, 0:n_key] = p.astype(jnp.bfloat16)
            o16 = jnp.dot(pb[:, 0:n_key], vals, preferred_element_type=f32).astype(jnp.bfloat16)
            dv = lax.dot_general(pb[:, 0:n_key], qg[slot, 1], tn, preferred_element_type=f32)
            odq[slot, 0] = o16
            delta = jnp.sum(qg[slot, 1].astype(f32) * o16.astype(f32), axis=1, keepdims=True)
            dsb[:, 0:n_key] = (p * (dp - delta)).astype(jnp.bfloat16)
            dq = jnp.dot(dsb[:, 0:n_key], keys, preferred_element_type=f32)
            odq[slot, 1] = (dq * scale).astype(jnp.bfloat16)
            dk = lax.dot_general(dsb[:, 0:n_key], qg[slot, 0], tn, preferred_element_type=f32)
            for a in range(c + 1):
                for p in range(2):
                    rows = slice((2 * a + p) * piece, (2 * a + p + 1) * piece)
                    part[slot, p, a, 0:piece, :] = dk[rows]
                    part[slot, p, a, piece:two, :] = dv[rows]

        def part_copy(b):
            return remote(part.at[b % 2, 1 - core, here], prx.at[b % NPRX, here], part_tx.at[b % 2],
                          prx_sem.at[b % NPRX], {'cp': partner})

        def unit_send(b, e, i):
            a, to, buf, _, late = SENDS[c, e][i]
            unit = acc.at[b % NACC, a]
            sem = tx_sem.at[b % NACC]

            def now(to=to, buf=buf):
                remote(unit, rx[buf].at[b], sem, rx_sem.at[buf, b], dev(to)).start()

            if (c, e, a) == TURNED:
                pl.when(b < first_turn)(now)
                pl.when(b >= first_turn)(lambda: now(*TURN))
            elif late is None:
                now()
            else:
                pl.when(b < first_late)(now)

                @pl.when(b >= first_late)
                def _():
                    pltpu.make_async_copy(unit, (near_ref, far_ref)[late].at[b - first_late], sem).start()

        def got(buf, b):
            local_wait(rx[buf].at[b], rx_sem.at[buf, b])

        def merge_partner(b):
            local_wait(prx.at[b % NPRX, here], prx_sem.at[b % NPRX])
            acc[b % NACC, here] = part[b % 2, core, here] + prx[b % NPRX, here]
            for e in range(2):
                sends = [i for i, s in enumerate(SENDS.get((c, e), ())) if not s[3]]
                if sends:
                    @pl.when(core == e)
                    def _():
                        for i in sends:
                            if (c, e, SENDS[c, e][i][0]) == (TURN[0], TURNED[1], TURNED[2]):
                                pl.when(b < first_turn)(lambda: unit_send(b, e, i))
                            else:
                                unit_send(b, e, i)

        def relay(b, e):
            buf = RELAY[c, e][1]

            def take_in():
                got(buf, b)
                if c == 0:
                    fwd_copy(b).start()
                    return
                for i, (a, _, _, after, _) in enumerate(SENDS[c, e]):
                    if after:
                        acc[b % NACC, a] = acc[b % NACC, a] + rx[buf][b]
                        unit_send(b, e, i)

            if c == 0:
                pl.when(b < first_turn)(take_in)
            else:
                take_in()

        def add_turned(b):
            got(TURN[1], b)
            a = TURNED[2]
            acc[b % NACC, a] = acc[b % NACC, a] + rx[TURN[1]][b]
            unit_send(b, TURNED[1], [s[0] for s in SENDS[c, TURNED[1]]].index(a))

        def fwd_copy(b):
            return remote(rx2.at[b], rx1.at[b], fwd_tx, rx_sem.at[1, b], dev(1))

        def finish(b, e):
            def total(bufs):
                out = acc[b % NACC, c]
                for buf in bufs:
                    got(buf, b)
                    out = out + rx[buf][b]
                return out

            @pl.when(b < first_late)
            def _():
                out = total(FINISH[c, e][1])
                fin_k[b] = (out[0:piece] * scale).astype(jnp.bfloat16)
                fin_v[b] = out[piece:two].astype(jnp.bfloat16)

            @pl.when(b == first_late)
            def _():
                for copy in out_copies():
                    copy.start()

            @pl.when((b >= first_late) & (b < first_turn))
            def _():
                own[b - first_late] = total(FINISH_LATE.get((c, e), ()))

            @pl.when(b >= first_turn)
            def _():
                own[b - first_late] = total(())

            @pl.when(b >= first_late)
            def _():
                late = b - first_late
                pltpu.make_async_copy(own.at[late], own_ref.at[late], late_sem).start()

        n_step = n_seq + LAG_MAX

        def when_seq(b, fn):
            pl.when((b >= 0) & (b < n_seq))(lambda: fn(b))

        def sent(b):
            for e in range(2):
                n = len(SENDS.get((c, e), ()))
                if n:
                    pl.when(core == e)(lambda: local_wait(acc.at[b % NACC, pl.ds(0, n)], tx_sem.at[b % NACC]))

        def step(t, carry):
            @pl.when(t < n_seq)
            def _():
                push_at(t)
                take_at(t)

                @pl.when(t + 1 < n_seq)
                def _():
                    qg_start(t + 1)

                @pl.when(t >= 2)
                def _():
                    odq_wait(t - 2)
                    part_copy(t - 2).wait_send()

                pl.when(t >= NACC)(lambda: sent(t - NACC))
                arrived(t)
                local_wait(qg.at[t % 2], qg_sem.at[t % 2])
                compute(t)
                odq_start(t)
                part_copy(t).start()

            when_seq(t - 1, merge_partner)
            for e in range(2):
                @pl.when(core == e)
                def _():
                    if (c, e) in RELAY:
                        when_seq(t - RELAY[c, e][0], lambda b: relay(b, e))
                    if (c, e) == (TURN[0], TURNED[1]):
                        b_turn = t - TURN_LAG
                        pl.when((b_turn >= first_turn) & (b_turn < n_seq))(lambda: add_turned(b_turn))
                    when_seq(t - FINISH[c, e][0], lambda b: finish(b, e))
            return carry

        lax.fori_loop(0, n_step, step, 0)

        for b in (n_seq - 2, n_seq - 1):
            odq_wait(b)
            part_copy(b).wait_send()
        for b in range(n_seq - NACC, n_seq):
            sent(b)
        whole = kv.at[:, :, 0, 0]
        for i, (_, _, who) in enumerate(flows):
            by_core(who, lambda: local_wait(whole, kv_tx.at[i]))
        local_wait(kv.at[:, :, here, 0], kvp_tx)
        for to in doc_dests:
            doc_copy(to).wait_send()
        if c == 0:
            pl.when(core == 1)(lambda: local_wait(rx2.at[pl.ds(0, first_turn)], fwd_tx))

    for c in range(n_chip):
        pl.when(chip == c)(functools.partial(run_chip, c))

    for copy in out_copies():
        copy.wait()
    local_wait(own, late_sem)


def copy_kernel(a_ref, b_ref, k_ref, v_ref, a_out, b_out, k_out, v_out, buf, in_sem, out_sem, k_buf, v_buf, kv_sem):
    n_buf, n_block = buf.shape[:2]
    total = 2 * a_ref.shape[0] // n_block
    ahead = n_buf // 2

    def read(i):
        src = (a_ref, b_ref)[i % 2].at[pl.ds(i // 2 * n_block, n_block)]
        return pltpu.make_async_copy(src, buf.at[i % n_buf], in_sem.at[i % n_buf])

    def write(i):
        dst = (a_out, b_out)[i % 2].at[pl.ds(i // 2 * n_block, n_block)]
        return pltpu.make_async_copy(buf.at[i % n_buf], dst, out_sem.at[i % n_buf])

    rows = pl.ds(0, k_ref.shape[0])
    small_in = [pltpu.make_async_copy(k_ref, k_buf, kv_sem.at[0]), pltpu.make_async_copy(v_ref, v_buf, kv_sem.at[1])]
    small_out = [pltpu.make_async_copy(k_buf, k_out.at[rows], kv_sem.at[0]),
                 pltpu.make_async_copy(v_buf, v_out.at[rows], kv_sem.at[1])]

    for i in range(ahead):
        read(i).start()
    for copy in small_in:
        copy.start()
    for i in range(total):
        if i + ahead < total:
            if i + ahead >= n_buf:
                write(i + ahead - n_buf).wait()
            read(i + ahead).start()
        read(i).wait()
        write(i).start()
        if i == ahead:
            for copy in small_in:
                copy.wait()
            for copy in small_out:
                copy.start()
    for i in range(max(total - n_buf, 0), total):
        write(i).wait()
    for copy in small_out:
        copy.wait()


def solution(mesh):
    n_dev = mesh.shape['cp']
    seq_spec = P('dp', 'cp', None, None)

    def per_device(query, keys, values, grad_out, doc_id):
        n_seq, piece, n_heads, head_dim = query.shape
        n_rows = piece * n_heads
        n_key = piece * n_dev
        two = 2 * piece
        rows_shape = (n_seq, n_rows, head_dim)
        kv_shape = (n_seq, piece, head_dim)
        late_shape = (N_LATE, two, head_dim)
        main_shape = (n_seq - N_LATE, piece, head_dim)
        bf16, f32, i32 = jnp.bfloat16, jnp.float32, jnp.int32
        dma = pltpu.SemaphoreType.DMA
        any_spec = pl.BlockSpec(memory_space=pl.ANY)
        n_chip = n_dev // 2
        out = pl.pallas_call(
            functools.partial(attention_kernel, n_dev, n_heads),
            name='attention',
            out_shape=[jax.ShapeDtypeStruct(rows_shape, bf16)] * 2 + [jax.ShapeDtypeStruct(main_shape, bf16)] * 2
            + [jax.ShapeDtypeStruct(late_shape, f32)] * 3,
            in_specs=[any_spec] * 5,
            out_specs=[any_spec] * 7,
            scratch_shapes=[
                pltpu.VMEM((n_seq, 2, n_chip, 2, piece, head_dim), bf16),
                pltpu.VMEM((n_seq, two, head_dim), f32),
                pltpu.VMEM((n_seq, two, head_dim), f32),
                pltpu.VMEM((n_seq, two, head_dim), f32),
                pltpu.VMEM((NACC, n_chip, two, head_dim), f32),
                pltpu.VMEM((2, 2, n_chip, two, head_dim), f32),
                pltpu.VMEM((NPRX, n_chip, two, head_dim), f32),
                pltpu.VMEM((2, 2, n_rows, head_dim), bf16),
                pltpu.VMEM((2, 2, n_rows, head_dim), bf16),
                pltpu.VMEM((n_rows, n_key), bf16),
                pltpu.VMEM((n_rows, n_key), bf16),
                pltpu.VMEM(main_shape, bf16),
                pltpu.VMEM(main_shape, bf16),
                pltpu.VMEM(late_shape, f32),
                pltpu.VMEM((n_dev, n_seq, piece), i32),
                pltpu.VMEM((n_seq, 1, n_key), i32),
                pltpu.VMEM((n_seq, 1, piece), i32),
                pltpu.VMEM((piece, n_key), f32),
                dma((5,)), dma, dma,
                dma((4,)), dma((n_chip, n_seq)), dma, dma((n_seq,)),
                dma((2,)), dma((2,)),
                dma((2,)), dma((NPRX,)), dma((3, n_seq)), dma((NACC,)), dma, dma,
            ],
            compiler_params=pltpu.CompilerParams(collective_id=0, has_side_effects=True, vmem_limit_bytes=63 * 1024 * 1024),
        )(query.reshape(rows_shape), grad_out.reshape(rows_shape), keys.reshape(kv_shape), values.reshape(kv_shape), doc_id)
        attn_out, grad_query, grad_keys, grad_values, near, far, own = out
        attn_out, grad_query, grad_keys, grad_values = pl.pallas_call(
            copy_kernel,
            name='results',
            out_shape=[jax.ShapeDtypeStruct(rows_shape, bf16)] * 2 + [jax.ShapeDtypeStruct(kv_shape, bf16)] * 2,
            in_specs=[pl.BlockSpec(memory_space=pltpu.HBM)] * 4,
            out_specs=[pl.BlockSpec(memory_space=pltpu.HBM)] * 4,
            scratch_shapes=[pltpu.VMEM((N_COPY, COPY_BLOCK, n_rows, head_dim), bf16), dma((N_COPY,)), dma((N_COPY,)),
                            pltpu.VMEM(main_shape, bf16), pltpu.VMEM(main_shape, bf16), dma((2,))],
            compiler_params=pltpu.CompilerParams(vmem_limit_bytes=56 * 1024 * 1024),
            cost_estimate=pl.CostEstimate(flops=12_000_000_000, bytes_accessed=8 * n_seq * n_rows * head_dim,
                                          transcendentals=0),
        )(attn_out, grad_query, grad_keys, grad_values)
        to_near = [(d, d - 2) for d in range(2, n_dev)]
        to_far = [(n_dev - 2 + e, e) for e in range(2)]
        from_far = lax.ppermute(far, 'cp', to_far)
        from_near = lax.ppermute(near, 'cp', to_near)
        late = own + from_far + from_near
        late_keys = (late[:, 0:piece] * head_dim ** -0.5).astype(bf16)
        late_values = late[:, piece:two].astype(bf16)
        grad_keys = lax.dynamic_update_slice(grad_keys, late_keys, (n_seq - N_LATE, 0, 0))
        grad_values = lax.dynamic_update_slice(grad_values, late_values, (n_seq - N_LATE, 0, 0))
        return (attn_out.reshape(query.shape), grad_query.reshape(query.shape),
                grad_keys.reshape(keys.shape), grad_values.reshape(values.shape))

    return jax.shard_map(per_device, mesh=mesh, in_specs=(seq_spec,) * 4 + (P('dp', 'cp'),), out_specs=(seq_spec,) * 4, check_vma=False)
```

```python
import functools

import jax
import jax.numpy as jnp
from jax import lax
from jax.experimental import pallas as pl
from jax.experimental.pallas import tpu as pltpu
from jax.sharding import PartitionSpec as P

MESH = pl.DeviceIdType.MESH
LOG2E = 1.4426950408889634
HIDDEN = -3.0e38
NACC = 12
NPRX = 4
COPY_BLOCK = 2
N_COPY = 32
N_FIRST = 1
N_TURN = 2
N_LATE = 9


HOPS = ((1, 1, 2, None), (1, 0, 2, None), (2, 1, 3, 0), (2, 2, 3, None), (0, 1, 3, 1), (1, 1, 0, 1), (0, 0, 3, None), (0, 0, 1, None))
PUSH = {0: (0, 8), 1: (2, 12), 2: (3, 3), 3: (2, 5)}
TAKE = {0: (0, 10), 1: (2, 6), 2: (2, 2), 3: (0, 1)}
SENDS = {(3, 0): ((1, 2, 0, False, None), (0, 0, 1, False, 1), (2, 2, 1, False, 0)), (3, 1): ((2, 2, 0, False, 0), (0, 0, 0, True, 1), (1, 0, 2, False, None)), (2, 0): ((1, 1, 1, True, 1), (0, 1, 0, False, None)), (2, 1): ((1, 1, 0, False, 1), (0, 3, 0, False, None)), (1, 0): ((0, 0, 0, True, 0),), (1, 1): ((0, 0, 1, False, 0),)}
RELAY = {(3, 1): (3, 0), (2, 0): (8, 0), (1, 0): (8, 0), (0, 1): (7, 2)}
FINISH = {(3, 0): (1, ()), (3, 1): (1, ()), (2, 0): (7, (1,)), (2, 1): (5, (0,)), (1, 0): (10, (1,)), (1, 1): (10, (0, 1)), (0, 0): (10, (0, 1)), (0, 1): (9, (0, 1))}
LAG_MAX = 10
FINISH_LATE = {(1, 1): (1,)}
TURNED, TURN, TURN_LAG = (3, 1, 1), (2, 1), 4


def attention_kernel(n_dev, n_heads, *refs):
    (q_ref, g_ref, k_ref, v_ref, doc_ref, o_ref, dq_ref, dk_ref, dv_ref, even_ref, odd_ref, own_ref,
     kv, rx0, rx1, rx2, acc, part, prx, qg, odq, pb, dsb, fin_k, fin_v, own, docs, kdoc, odoc, vis,
     load_sem, doc_tx, doc_rx, kv_tx, kv_rx, kvp_tx, kvp_rx, qg_sem, odq_sem,
     part_tx, prx_sem, rx_sem, tx_sem, fwd_tx, late_sem) = refs
    rx = (rx0, rx1, rx2)
    n_seq, n_rows, head_dim = q_ref.shape
    piece = k_ref.shape[1]
    two = 2 * piece
    n_chip = n_dev // 2
    scale = head_dim ** -0.5
    me = lax.axis_index('cp')
    chip = me // 2
    core = me % 2
    partner = chip * 2 + (1 - core)

    def dev(c):
        return {'cp': c * 2 + core}

    def remote(src, dst, tx, rx, to):
        return pltpu.make_async_remote_copy(src_ref=src, dst_ref=dst, send_sem=tx, recv_sem=rx,
                                            device_id=to, device_id_type=MESH)

    def local_wait(ref, sem):
        pltpu.make_async_copy(ref, ref, sem).wait()

    barrier = pltpu.get_barrier_semaphore()
    for hop in range(1, n_dev):
        pl.semaphore_signal(barrier, inc=1, device_id={'cp': (me + hop) % n_dev}, device_id_type=MESH)

    def own_copies(lo, n, sem):
        seqs = pl.ds(lo, n)
        return (pltpu.make_async_copy(k_ref.at[seqs], kv.at[seqs, 0, chip, core], load_sem.at[sem]),
                pltpu.make_async_copy(v_ref.at[seqs], kv.at[seqs, 1, chip, core], load_sem.at[sem + 1]))

    own_d = pltpu.make_async_copy(doc_ref, docs.at[me], load_sem.at[4])
    own_first = own_copies(0, N_FIRST, 0)
    own_rest = own_copies(N_FIRST, n_seq - N_FIRST, 2)
    for copy in (*own_first, own_d, *own_rest):
        copy.start()

    def qg_start(b):
        pltpu.make_async_copy(q_ref.at[b], qg.at[b % 2, 0], qg_sem.at[b % 2]).start()
        pltpu.make_async_copy(g_ref.at[b], qg.at[b % 2, 1], qg_sem.at[b % 2]).start()

    def odq_start(b):
        pltpu.make_async_copy(odq.at[b % 2, 0], o_ref.at[b], odq_sem.at[b % 2]).start()
        pltpu.make_async_copy(odq.at[b % 2, 1], dq_ref.at[b], odq_sem.at[b % 2]).start()

    def odq_wait(b):
        local_wait(odq.at[b % 2], odq_sem.at[b % 2])

    qg_start(0)
    for copy in (*own_first, own_d):
        copy.wait()
    odoc[...] = docs[me].reshape(n_seq, 1, piece)
    pl.semaphore_wait(barrier, n_dev - 1)

    def out_copies():
        return (pltpu.make_async_copy(fin_k, dk_ref, load_sem.at[0]), pltpu.make_async_copy(fin_v, dv_ref, load_sem.at[1]))

    def run_chip(c):
        n_key = two * (c + 1)
        here = pl.ds(0, c + 1)
        first_late = n_seq - N_LATE
        first_turn = n_seq - N_TURN

        def doc_copy(to):
            return remote(docs.at[me], docs.at[me], doc_tx, doc_rx, to)

        doc_dests = [{'cp': partner}] + [{'cp': d} for d in range(two // piece * (c + 1), n_dev)]

        flows = [hop[1:] for hop in HOPS if hop[0] == c]
        through = [src for src, _, _ in flows if src > c]

        def by_core(who, fn):
            if who is None:
                fn()
            else:
                pl.when(core == who)(fn)

        def kv_sem(src, to, b):
            return kv_rx.at[0 if to == n_chip - 1 else src, b]

        def kv_copy(i, b):
            src, to, _ = flows[i]
            blk = kv.at[b, :, src, core]
            return remote(blk, blk, kv_tx.at[i], kv_sem(src, to, b), dev(to))

        def kvp_copy(b):
            blk = kv.at[b, :, here, core]
            return remote(blk, blk, kvp_tx, kvp_rx.at[b], {'cp': partner})

        def send_on(src, b):
            for i, (s, _, who) in enumerate(flows):
                if s == src:
                    by_core(who, lambda: kv_copy(i, b).start())

        def push(b):
            send_on(c, b)

        def take(b):
            if c == n_chip - 1:
                local_wait(kv.at[b, :, pl.ds(0, c), core], kv_rx.at[0, b])
            else:
                for src in range(c - 1, -1, -1):
                    local_wait(kv.at[b, :, src, core], kv_rx.at[src, b])
                    send_on(src, b)
            kvp_copy(b).start()
            for src in through:
                who = [w for s, _, w in flows if s == src][0]

                def pass_on():
                    local_wait(kv.at[b, :, src, core], kv_rx.at[src, b])
                    for i, (s, _, _) in enumerate(flows):
                        if s == src:
                            kv_copy(i, b).start()

                by_core(who, pass_on)

        def ramp(lead, fn):
            first, most = lead
            start = min(first, most)

            def at_step(t):
                b = jnp.minimum(start + 2 * t, t + most)
                pl.when(b < n_seq)(lambda: fn(b))
                if most - start > 0:
                    pl.when(t < most - start)(lambda: fn(b + 1))

            return start, at_step

        def arrived(b):
            local_wait(kv.at[b, :, here, 1 - core], kvp_rx.at[b])

        n_push, push_at = ramp(PUSH[c], push)
        n_take, take_at = ramp(TAKE[c], take)
        for b in range(n_push):
            if b == N_FIRST:
                for copy in own_rest:
                    copy.wait()
            push(b)
        if n_push <= N_FIRST:
            for copy in own_rest:
                copy.wait()
        for to in doc_dests:
            doc_copy(to).start()
        for b in range(n_take):
            take(b)

        n_doc = 2 * c + 1
        pltpu.make_async_copy(docs.at[pl.ds(0, n_doc)], docs.at[pl.ds(0, n_doc)], doc_rx).wait()
        for p in range(2 * c + 2):
            kdoc[:, :, p * piece:(p + 1) * piece] = docs[p].reshape(n_seq, 1, piece)

        def compute(b):
            slot = b % 2
            keys = kv[b, 0, here].reshape(n_key, head_dim)
            vals = kv[b, 1, here].reshape(n_key, head_dim)
            tok = lax.broadcasted_iota(jnp.int32, (piece, piece), 0)
            tok_t = lax.broadcasted_iota(jnp.int32, (piece, piece), 1)
            own_doc = odoc[b]
            q_doc = jnp.sum(jnp.where(tok == tok_t, own_doc, 0), axis=1, keepdims=True)
            key_doc = kdoc[b, :, 0:n_key]
            q_pos = me * piece + lax.broadcasted_iota(jnp.int32, (piece, n_key), 0)
            k_pos = lax.broadcasted_iota(jnp.int32, (piece, n_key), 1)
            seen = (q_doc == key_doc) & (k_pos <= q_pos)
            vis[:, 0:n_key] = jnp.where(seen, 0.0, HIDDEN)
            nt = (((1,), (1,)), ((), ()))
            tn = (((0,), (0,)), ((), ()))
            f32 = jnp.float32
            s = lax.dot_general(qg[slot, 0], keys, nt, preferred_element_type=f32)
            dp = lax.dot_general(qg[slot, 1], vals, nt, preferred_element_type=f32)
            s = s.reshape(piece, n_heads, n_key) * (scale * LOG2E) + vis[:, 0:n_key].reshape(piece, 1, n_key)
            s = s.reshape(n_rows, n_key)
            e = jnp.exp2(s - jnp.max(s, axis=1, keepdims=True))
            p = e * (1.0 / jnp.sum(e, axis=1, keepdims=True))
            pb[:, 0:n_key] = p.astype(jnp.bfloat16)
            o16 = jnp.dot(pb[:, 0:n_key], vals, preferred_element_type=f32).astype(jnp.bfloat16)
            dv = lax.dot_general(pb[:, 0:n_key], qg[slot, 1], tn, preferred_element_type=f32)
            odq[slot, 0] = o16
            delta = jnp.sum(qg[slot, 1].astype(f32) * o16.astype(f32), axis=1, keepdims=True)
            dsb[:, 0:n_key] = (p * (dp - delta)).astype(jnp.bfloat16)
            dq = jnp.dot(dsb[:, 0:n_key], keys, preferred_element_type=f32)
            odq[slot, 1] = (dq * scale).astype(jnp.bfloat16)
            dk = lax.dot_general(dsb[:, 0:n_key], qg[slot, 0], tn, preferred_element_type=f32)
            for a in range(c + 1):
                for p in range(2):
                    rows = slice((2 * a + p) * piece, (2 * a + p + 1) * piece)
                    part[slot, p, a, 0:piece, :] = dk[rows]
                    part[slot, p, a, piece:two, :] = dv[rows]

        def part_copy(b):
            return remote(part.at[b % 2, 1 - core, here], prx.at[b % NPRX, here], part_tx.at[b % 2],
                          prx_sem.at[b % NPRX], {'cp': partner})

        def unit_send(b, e, i):
            a, to, buf, _, late = SENDS[c, e][i]
            unit = acc.at[b % NACC, a]
            sem = tx_sem.at[b % NACC]

            def now(to=to, buf=buf):
                remote(unit, rx[buf].at[b], sem, rx_sem.at[buf, b], dev(to)).start()

            if (c, e, a) == TURNED:
                pl.when(b < first_turn)(now)
                pl.when(b >= first_turn)(lambda: now(*TURN))
            elif late is None:
                now()
            else:
                pl.when(b < first_late)(now)

                @pl.when(b >= first_late)
                def _():
                    pltpu.make_async_copy(unit, (even_ref, odd_ref)[late].at[b - first_late], sem).start()

        def got(buf, b):
            local_wait(rx[buf].at[b], rx_sem.at[buf, b])

        def merge_partner(b):
            local_wait(prx.at[b % NPRX, here], prx_sem.at[b % NPRX])
            acc[b % NACC, here] = part[b % 2, core, here] + prx[b % NPRX, here]
            for e in range(2):
                sends = [i for i, s in enumerate(SENDS.get((c, e), ())) if not s[3]]
                if sends:
                    @pl.when(core == e)
                    def _():
                        for i in sends:
                            if (c, e, SENDS[c, e][i][0]) == (TURN[0], TURNED[1], TURNED[2]):
                                pl.when(b < first_turn)(lambda: unit_send(b, e, i))
                            else:
                                unit_send(b, e, i)

        def relay(b, e):
            buf = RELAY[c, e][1]

            def take_in():
                got(buf, b)
                if c == 0:
                    fwd_copy(b).start()
                    return
                for i, (a, _, _, after, _) in enumerate(SENDS[c, e]):
                    if after:
                        acc[b % NACC, a] = acc[b % NACC, a] + rx[buf][b]
                        unit_send(b, e, i)

            if c == 0:
                pl.when(b < first_turn)(take_in)
            else:
                take_in()

        def add_turned(b):
            got(TURN[1], b)
            a = TURNED[2]
            acc[b % NACC, a] = acc[b % NACC, a] + rx[TURN[1]][b]
            unit_send(b, TURNED[1], [s[0] for s in SENDS[c, TURNED[1]]].index(a))

        def fwd_copy(b):
            return remote(rx2.at[b], rx1.at[b], fwd_tx, rx_sem.at[1, b], dev(1))

        def finish(b, e):
            def total(bufs):
                out = acc[b % NACC, c]
                for buf in bufs:
                    got(buf, b)
                    out = out + rx[buf][b]
                return out

            @pl.when(b < first_late)
            def _():
                out = total(FINISH[c, e][1])
                fin_k[b] = (out[0:piece] * scale).astype(jnp.bfloat16)
                fin_v[b] = out[piece:two].astype(jnp.bfloat16)

            @pl.when(b == first_late)
            def _():
                for copy in out_copies():
                    copy.start()

            @pl.when((b >= first_late) & (b < first_turn))
            def _():
                own[b - first_late] = total(FINISH_LATE.get((c, e), ()))

            @pl.when(b >= first_turn)
            def _():
                own[b - first_late] = total(())

            @pl.when(b >= first_late)
            def _():
                late = b - first_late
                pltpu.make_async_copy(own.at[late], own_ref.at[late], late_sem).start()

        n_step = n_seq + LAG_MAX

        def when_seq(b, fn):
            pl.when((b >= 0) & (b < n_seq))(lambda: fn(b))

        def sent(b):
            for e in range(2):
                n = len(SENDS.get((c, e), ()))
                if n:
                    pl.when(core == e)(lambda: local_wait(acc.at[b % NACC, pl.ds(0, n)], tx_sem.at[b % NACC]))

        def step(t, carry):
            @pl.when(t < n_seq)
            def _():
                push_at(t)
                take_at(t)

                @pl.when(t + 1 < n_seq)
                def _():
                    qg_start(t + 1)

                @pl.when(t >= 2)
                def _():
                    odq_wait(t - 2)
                    part_copy(t - 2).wait_send()

                pl.when(t >= NACC)(lambda: sent(t - NACC))
                arrived(t)
                local_wait(qg.at[t % 2], qg_sem.at[t % 2])
                compute(t)
                odq_start(t)
                part_copy(t).start()

            when_seq(t - 1, merge_partner)
            for e in range(2):
                @pl.when(core == e)
                def _():
                    if (c, e) in RELAY:
                        when_seq(t - RELAY[c, e][0], lambda b: relay(b, e))
                    if (c, e) == (TURN[0], TURNED[1]):
                        b_turn = t - TURN_LAG
                        pl.when((b_turn >= first_turn) & (b_turn < n_seq))(lambda: add_turned(b_turn))
                    when_seq(t - FINISH[c, e][0], lambda b: finish(b, e))
            return carry

        lax.fori_loop(0, n_step, step, 0)

        for b in (n_seq - 2, n_seq - 1):
            odq_wait(b)
            part_copy(b).wait_send()
        for b in range(n_seq - NACC, n_seq):
            sent(b)
        whole = kv.at[:, :, 0, 0]
        for i, (_, _, who) in enumerate(flows):
            by_core(who, lambda: local_wait(whole, kv_tx.at[i]))
        local_wait(kv.at[:, :, here, 0], kvp_tx)
        for to in doc_dests:
            doc_copy(to).wait_send()
        if c == 0:
            pl.when(core == 1)(lambda: local_wait(rx2.at[pl.ds(0, first_turn)], fwd_tx))

    for c in range(n_chip):
        pl.when(chip == c)(functools.partial(run_chip, c))

    for copy in out_copies():
        copy.wait()
    local_wait(own, late_sem)


def copy_kernel(a_ref, b_ref, k_ref, v_ref, a_out, b_out, k_out, v_out, buf, in_sem, out_sem, k_buf, v_buf, kv_sem):
    n_buf, n_block = buf.shape[:2]
    total = 2 * a_ref.shape[0] // n_block
    ahead = n_buf // 2

    def read(i):
        src = (a_ref, b_ref)[i % 2].at[pl.ds(i // 2 * n_block, n_block)]
        return pltpu.make_async_copy(src, buf.at[i % n_buf], in_sem.at[i % n_buf])

    def write(i):
        dst = (a_out, b_out)[i % 2].at[pl.ds(i // 2 * n_block, n_block)]
        return pltpu.make_async_copy(buf.at[i % n_buf], dst, out_sem.at[i % n_buf])

    rows = pl.ds(0, k_ref.shape[0])
    small_in = [pltpu.make_async_copy(k_ref, k_buf, kv_sem.at[0]), pltpu.make_async_copy(v_ref, v_buf, kv_sem.at[1])]
    small_out = [pltpu.make_async_copy(k_buf, k_out.at[rows], kv_sem.at[0]),
                 pltpu.make_async_copy(v_buf, v_out.at[rows], kv_sem.at[1])]

    for i in range(ahead):
        read(i).start()
    for copy in small_in:
        copy.start()
    for i in range(total):
        if i + ahead < total:
            if i + ahead >= n_buf:
                write(i + ahead - n_buf).wait()
            read(i + ahead).start()
        read(i).wait()
        write(i).start()
        if i == ahead:
            for copy in small_in:
                copy.wait()
            for copy in small_out:
                copy.start()
    for i in range(max(total - n_buf, 0), total):
        write(i).wait()
    for copy in small_out:
        copy.wait()


def solution(mesh):
    n_dev = mesh.shape['cp']
    seq_spec = P('dp', 'cp', None, None)

    def per_device(query, keys, values, grad_out, doc_id):
        n_seq, piece, n_heads, head_dim = query.shape
        n_rows = piece * n_heads
        n_key = piece * n_dev
        two = 2 * piece
        rows_shape = (n_seq, n_rows, head_dim)
        kv_shape = (n_seq, piece, head_dim)
        late_shape = (N_LATE, two, head_dim)
        main_shape = (n_seq - N_LATE, piece, head_dim)
        bf16, f32, i32 = jnp.bfloat16, jnp.float32, jnp.int32
        dma = pltpu.SemaphoreType.DMA
        any_spec = pl.BlockSpec(memory_space=pl.ANY)
        n_chip = n_dev // 2
        out = pl.pallas_call(
            functools.partial(attention_kernel, n_dev, n_heads),
            name='attention',
            out_shape=[jax.ShapeDtypeStruct(rows_shape, bf16)] * 2 + [jax.ShapeDtypeStruct(main_shape, bf16)] * 2
            + [jax.ShapeDtypeStruct(late_shape, f32)] * 3,
            in_specs=[any_spec] * 5,
            out_specs=[any_spec] * 7,
            scratch_shapes=[
                pltpu.VMEM((n_seq, 2, n_chip, 2, piece, head_dim), bf16),
                pltpu.VMEM((n_seq, two, head_dim), f32),
                pltpu.VMEM((n_seq, two, head_dim), f32),
                pltpu.VMEM((n_seq, two, head_dim), f32),
                pltpu.VMEM((NACC, n_chip, two, head_dim), f32),
                pltpu.VMEM((2, 2, n_chip, two, head_dim), f32),
                pltpu.VMEM((NPRX, n_chip, two, head_dim), f32),
                pltpu.VMEM((2, 2, n_rows, head_dim), bf16),
                pltpu.VMEM((2, 2, n_rows, head_dim), bf16),
                pltpu.VMEM((n_rows, n_key), bf16),
                pltpu.VMEM((n_rows, n_key), bf16),
                pltpu.VMEM(main_shape, bf16),
                pltpu.VMEM(main_shape, bf16),
                pltpu.VMEM(late_shape, f32),
                pltpu.VMEM((n_dev, n_seq, piece), i32),
                pltpu.VMEM((n_seq, 1, n_key), i32),
                pltpu.VMEM((n_seq, 1, piece), i32),
                pltpu.VMEM((piece, n_key), f32),
                dma((5,)), dma, dma,
                dma((4,)), dma((n_chip, n_seq)), dma, dma((n_seq,)),
                dma((2,)), dma((2,)),
                dma((2,)), dma((NPRX,)), dma((3, n_seq)), dma((NACC,)), dma, dma,
            ],
            compiler_params=pltpu.CompilerParams(collective_id=0, has_side_effects=True, vmem_limit_bytes=63 * 1024 * 1024),
        )(query.reshape(rows_shape), grad_out.reshape(rows_shape), keys.reshape(kv_shape), values.reshape(kv_shape), doc_id)
        attn_out, grad_query, grad_keys, grad_values, even, odd, own = out
        attn_out, grad_query, grad_keys, grad_values = pl.pallas_call(
            copy_kernel,
            name='results',
            out_shape=[jax.ShapeDtypeStruct(rows_shape, bf16)] * 2 + [jax.ShapeDtypeStruct(kv_shape, bf16)] * 2,
            in_specs=[pl.BlockSpec(memory_space=pltpu.HBM)] * 4,
            out_specs=[pl.BlockSpec(memory_space=pltpu.HBM)] * 4,
            scratch_shapes=[pltpu.VMEM((N_COPY, COPY_BLOCK, n_rows, head_dim), bf16), dma((N_COPY,)), dma((N_COPY,)),
                            pltpu.VMEM(main_shape, bf16), pltpu.VMEM(main_shape, bf16), dma((2,))],
            compiler_params=pltpu.CompilerParams(vmem_limit_bytes=56 * 1024 * 1024),
            cost_estimate=pl.CostEstimate(flops=12_000_000_000, bytes_accessed=8 * n_seq * n_rows * head_dim,
                                          transcendentals=0),
        )(attn_out, grad_query, grad_keys, grad_values)
        odd_hops = [(n_dev - 2 + e, e) for e in range(2)] + [(d + 2, d) for d in range(2, n_dev - 4)]
        even_hops = [(d + 2, d) for d in range(2)] + [(d + 2, d) for d in range(n_dev - 4, n_dev - 2)]
        from_odd = lax.ppermute(odd, 'cp', odd_hops)
        from_even = lax.ppermute(even, 'cp', even_hops)
        late = own + from_odd + from_even
        late_keys = (late[:, 0:piece] * head_dim ** -0.5).astype(bf16)
        late_values = late[:, piece:two].astype(bf16)
        grad_keys = lax.dynamic_update_slice(grad_keys, late_keys, (n_seq - N_LATE, 0, 0))
        grad_values = lax.dynamic_update_slice(grad_values, late_values, (n_seq - N_LATE, 0, 0))
        return (attn_out.reshape(query.shape), grad_query.reshape(query.shape),
                grad_keys.reshape(keys.shape), grad_values.reshape(values.shape))

    return jax.shard_map(per_device, mesh=mesh, in_specs=(seq_spec,) * 4 + (P('dp', 'cp'),), out_specs=(seq_spec,) * 4, check_vma=False)
```

```python
import functools

import jax
import jax.numpy as jnp
from jax import lax
from jax.experimental import pallas as pl
from jax.experimental.pallas import tpu as pltpu
from jax.sharding import PartitionSpec as P

MESH = pl.DeviceIdType.MESH
LOG2E = 1.4426950408889634
HIDDEN = -3.0e38
NACC = 12
NPRX = 4
COPY_BLOCK = 2
N_COPY = 32
N_FIRST = 1
N_TURN = 2
N_LATE = 8


HOPS = ((1, 1, 2, None), (1, 0, 2, None), (2, 1, 3, 0), (2, 2, 3, None), (0, 1, 3, 1), (1, 1, 0, 1), (0, 0, 3, None), (0, 0, 1, None))
PUSH = {0: (0, 8), 1: (2, 12), 2: (3, 3), 3: (2, 5)}
TAKE = {0: (0, 10), 1: (2, 6), 2: (2, 2), 3: (0, 1)}
SENDS = {(3, 0): ((1, 2, 0, False, None), (0, 0, 1, False, 1), (2, 2, 1, False, 0)), (3, 1): ((2, 2, 0, False, 0), (0, 0, 0, True, 1), (1, 0, 2, False, None)), (2, 0): ((1, 1, 1, True, 0), (0, 1, 0, False, None)), (2, 1): ((1, 1, 0, False, 0), (0, 3, 0, False, None)), (1, 0): ((0, 0, 0, True, 0),), (1, 1): ((0, 0, 1, False, 0),)}
RELAY = {(3, 1): (3, 0), (2, 0): (8, 0), (1, 0): (8, 0), (0, 1): (7, 2)}
FINISH = {(3, 0): (1, ()), (3, 1): (1, ()), (2, 0): (7, (1,)), (2, 1): (5, (0,)), (1, 0): (10, (1,)), (1, 1): (10, (0, 1)), (0, 0): (10, (0, 1)), (0, 1): (9, (0, 1))}
LAG_MAX = 10
FINISH_LATE = {(1, 1): (1,)}
TURNED, TURN, TURN_LAG = (3, 1, 1), (2, 1), 4


def attention_kernel(n_dev, n_heads, *refs):
    (q_ref, g_ref, k_ref, v_ref, doc_ref, o_ref, dq_ref, dk_ref, dv_ref, near_ref, far_ref, own_ref,
     kv, rx0, rx1, rx2, acc, part, prx, qg, odq, pb, dsb, fin_k, fin_v, own, docs, kdoc, odoc, vis,
     load_sem, doc_tx, doc_rx, kv_tx, kv_rx, kvp_tx, kvp_rx, qg_sem, odq_sem,
     part_tx, prx_sem, rx_sem, tx_sem, fwd_tx, late_sem) = refs
    rx = (rx0, rx1, rx2)
    n_seq, n_rows, head_dim = q_ref.shape
    piece = k_ref.shape[1]
    two = 2 * piece
    n_chip = n_dev // 2
    scale = head_dim ** -0.5
    me = lax.axis_index('cp')
    chip = me // 2
    core = me % 2
    partner = chip * 2 + (1 - core)

    def dev(c):
        return {'cp': c * 2 + core}

    def remote(src, dst, tx, rx, to):
        return pltpu.make_async_remote_copy(src_ref=src, dst_ref=dst, send_sem=tx, recv_sem=rx,
                                            device_id=to, device_id_type=MESH)

    def local_wait(ref, sem):
        pltpu.make_async_copy(ref, ref, sem).wait()

    barrier = pltpu.get_barrier_semaphore()
    for hop in range(1, n_dev):
        pl.semaphore_signal(barrier, inc=1, device_id={'cp': (me + hop) % n_dev}, device_id_type=MESH)

    def own_copies(lo, n, sem):
        seqs = pl.ds(lo, n)
        return (pltpu.make_async_copy(k_ref.at[seqs], kv.at[seqs, 0, chip, core], load_sem.at[sem]),
                pltpu.make_async_copy(v_ref.at[seqs], kv.at[seqs, 1, chip, core], load_sem.at[sem + 1]))

    own_d = pltpu.make_async_copy(doc_ref, docs.at[me], load_sem.at[4])
    own_first = own_copies(0, N_FIRST, 0)
    own_rest = own_copies(N_FIRST, n_seq - N_FIRST, 2)
    for copy in (*own_first, own_d, *own_rest):
        copy.start()

    def qg_start(b):
        pltpu.make_async_copy(q_ref.at[b], qg.at[b % 2, 0], qg_sem.at[b % 2]).start()
        pltpu.make_async_copy(g_ref.at[b], qg.at[b % 2, 1], qg_sem.at[b % 2]).start()

    def odq_start(b):
        pltpu.make_async_copy(odq.at[b % 2, 0], o_ref.at[b], odq_sem.at[b % 2]).start()
        pltpu.make_async_copy(odq.at[b % 2, 1], dq_ref.at[b], odq_sem.at[b % 2]).start()

    def odq_wait(b):
        local_wait(odq.at[b % 2], odq_sem.at[b % 2])

    qg_start(0)
    for copy in (*own_first, own_d):
        copy.wait()
    odoc[...] = docs[me].reshape(n_seq, 1, piece)
    pl.semaphore_wait(barrier, n_dev - 1)

    def out_copies():
        return (pltpu.make_async_copy(fin_k, dk_ref, load_sem.at[0]), pltpu.make_async_copy(fin_v, dv_ref, load_sem.at[1]))

    def run_chip(c):
        n_key = two * (c + 1)
        here = pl.ds(0, c + 1)
        first_late = n_seq - N_LATE
        first_turn = n_seq - N_TURN

        def doc_copy(to):
            return remote(docs.at[me], docs.at[me], doc_tx, doc_rx, to)

        doc_dests = [{'cp': partner}] + [{'cp': d} for d in range(two // piece * (c + 1), n_dev)]

        flows = [hop[1:] for hop in HOPS if hop[0] == c]
        through = [src for src, _, _ in flows if src > c]

        def by_core(who, fn):
            if who is None:
                fn()
            else:
                pl.when(core == who)(fn)

        def kv_sem(src, to, b):
            return kv_rx.at[0 if to == n_chip - 1 else src, b]

        def kv_copy(i, b):
            src, to, _ = flows[i]
            blk = kv.at[b, :, src, core]
            return remote(blk, blk, kv_tx.at[i], kv_sem(src, to, b), dev(to))

        def kvp_copy(b):
            blk = kv.at[b, :, here, core]
            return remote(blk, blk, kvp_tx, kvp_rx.at[b], {'cp': partner})

        def send_on(src, b):
            for i, (s, _, who) in enumerate(flows):
                if s == src:
                    by_core(who, lambda: kv_copy(i, b).start())

        def push(b):
            send_on(c, b)

        def take(b):
            if c == n_chip - 1:
                local_wait(kv.at[b, :, pl.ds(0, c), core], kv_rx.at[0, b])
            else:
                for src in range(c - 1, -1, -1):
                    local_wait(kv.at[b, :, src, core], kv_rx.at[src, b])
                    send_on(src, b)
            kvp_copy(b).start()
            for src in through:
                who = [w for s, _, w in flows if s == src][0]

                def pass_on():
                    local_wait(kv.at[b, :, src, core], kv_rx.at[src, b])
                    for i, (s, _, _) in enumerate(flows):
                        if s == src:
                            kv_copy(i, b).start()

                by_core(who, pass_on)

        def ramp(lead, fn):
            first, most = lead
            start = min(first, most)

            def at_step(t):
                b = jnp.minimum(start + 2 * t, t + most)
                pl.when(b < n_seq)(lambda: fn(b))
                if most - start > 0:
                    pl.when(t < most - start)(lambda: fn(b + 1))

            return start, at_step

        def arrived(b):
            local_wait(kv.at[b, :, here, 1 - core], kvp_rx.at[b])

        n_push, push_at = ramp(PUSH[c], push)
        n_take, take_at = ramp(TAKE[c], take)
        for b in range(n_push):
            if b == N_FIRST:
                for copy in own_rest:
                    copy.wait()
            push(b)
        if n_push <= N_FIRST:
            for copy in own_rest:
                copy.wait()
        for to in doc_dests:
            doc_copy(to).start()
        for b in range(n_take):
            take(b)

        n_doc = 2 * c + 1
        pltpu.make_async_copy(docs.at[pl.ds(0, n_doc)], docs.at[pl.ds(0, n_doc)], doc_rx).wait()
        for p in range(2 * c + 2):
            kdoc[:, :, p * piece:(p + 1) * piece] = docs[p].reshape(n_seq, 1, piece)

        def compute(b):
            slot = b % 2
            keys = kv[b, 0, here].reshape(n_key, head_dim)
            vals = kv[b, 1, here].reshape(n_key, head_dim)
            tok = lax.broadcasted_iota(jnp.int32, (piece, piece), 0)
            tok_t = lax.broadcasted_iota(jnp.int32, (piece, piece), 1)
            own_doc = odoc[b]
            q_doc = jnp.sum(jnp.where(tok == tok_t, own_doc, 0), axis=1, keepdims=True)
            key_doc = kdoc[b, :, 0:n_key]
            q_pos = me * piece + lax.broadcasted_iota(jnp.int32, (piece, n_key), 0)
            k_pos = lax.broadcasted_iota(jnp.int32, (piece, n_key), 1)
            seen = (q_doc == key_doc) & (k_pos <= q_pos)
            vis[:, 0:n_key] = jnp.where(seen, 0.0, HIDDEN)
            nt = (((1,), (1,)), ((), ()))
            tn = (((0,), (0,)), ((), ()))
            f32 = jnp.float32
            s = lax.dot_general(qg[slot, 0], keys, nt, preferred_element_type=f32)
            dp = lax.dot_general(qg[slot, 1], vals, nt, preferred_element_type=f32)
            s = s.reshape(piece, n_heads, n_key) * (scale * LOG2E) + vis[:, 0:n_key].reshape(piece, 1, n_key)
            s = s.reshape(n_rows, n_key)
            e = jnp.exp2(s - jnp.max(s, axis=1, keepdims=True))
            p = e * (1.0 / jnp.sum(e, axis=1, keepdims=True))
            pb[:, 0:n_key] = p.astype(jnp.bfloat16)
            o16 = jnp.dot(pb[:, 0:n_key], vals, preferred_element_type=f32).astype(jnp.bfloat16)
            dv = lax.dot_general(pb[:, 0:n_key], qg[slot, 1], tn, preferred_element_type=f32)
            odq[slot, 0] = o16
            delta = jnp.sum(qg[slot, 1].astype(f32) * o16.astype(f32), axis=1, keepdims=True)
            dsb[:, 0:n_key] = (p * (dp - delta)).astype(jnp.bfloat16)
            dq = jnp.dot(dsb[:, 0:n_key], keys, preferred_element_type=f32)
            odq[slot, 1] = (dq * scale).astype(jnp.bfloat16)
            dk = lax.dot_general(dsb[:, 0:n_key], qg[slot, 0], tn, preferred_element_type=f32)
            for a in range(c + 1):
                for p in range(2):
                    rows = slice((2 * a + p) * piece, (2 * a + p + 1) * piece)
                    part[slot, p, a, 0:piece, :] = dk[rows]
                    part[slot, p, a, piece:two, :] = dv[rows]

        def part_copy(b):
            return remote(part.at[b % 2, 1 - core, here], prx.at[b % NPRX, here], part_tx.at[b % 2],
                          prx_sem.at[b % NPRX], {'cp': partner})

        def unit_send(b, e, i):
            a, to, buf, _, late = SENDS[c, e][i]
            unit = acc.at[b % NACC, a]
            sem = tx_sem.at[b % NACC]

            def now(to=to, buf=buf):
                remote(unit, rx[buf].at[b], sem, rx_sem.at[buf, b], dev(to)).start()

            if (c, e, a) == TURNED:
                pl.when(b < first_turn)(now)
                pl.when(b >= first_turn)(lambda: now(*TURN))
            elif late is None:
                now()
            else:
                pl.when(b < first_late)(now)

                @pl.when(b >= first_late)
                def _():
                    pltpu.make_async_copy(unit, (near_ref, far_ref)[late].at[b - first_late], sem).start()

        def got(buf, b):
            local_wait(rx[buf].at[b], rx_sem.at[buf, b])

        def merge_partner(b):
            local_wait(prx.at[b % NPRX, here], prx_sem.at[b % NPRX])
            acc[b % NACC, here] = part[b % 2, core, here] + prx[b % NPRX, here]
            for e in range(2):
                sends = [i for i, s in enumerate(SENDS.get((c, e), ())) if not s[3]]
                if sends:
                    @pl.when(core == e)
                    def _():
                        for i in sends:
                            if (c, e, SENDS[c, e][i][0]) == (TURN[0], TURNED[1], TURNED[2]):
                                pl.when(b < first_turn)(lambda: unit_send(b, e, i))
                            else:
                                unit_send(b, e, i)

        def relay(b, e):
            buf = RELAY[c, e][1]

            def take_in():
                got(buf, b)
                if c == 0:
                    fwd_copy(b).start()
                    return
                for i, (a, _, _, after, _) in enumerate(SENDS[c, e]):
                    if after:
                        acc[b % NACC, a] = acc[b % NACC, a] + rx[buf][b]
                        unit_send(b, e, i)

            if c == 0:
                pl.when(b < first_turn)(take_in)
            else:
                take_in()

        def add_turned(b):
            got(TURN[1], b)
            a = TURNED[2]
            acc[b % NACC, a] = acc[b % NACC, a] + rx[TURN[1]][b]
            unit_send(b, TURNED[1], [s[0] for s in SENDS[c, TURNED[1]]].index(a))

        def fwd_copy(b):
            return remote(rx2.at[b], rx1.at[b], fwd_tx, rx_sem.at[1, b], dev(1))

        def finish(b, e):
            def total(bufs):
                out = acc[b % NACC, c]
                for buf in bufs:
                    got(buf, b)
                    out = out + rx[buf][b]
                return out

            @pl.when(b < first_late)
            def _():
                out = total(FINISH[c, e][1])
                fin_k[b] = (out[0:piece] * scale).astype(jnp.bfloat16)
                fin_v[b] = out[piece:two].astype(jnp.bfloat16)

            @pl.when(b == first_late)
            def _():
                for copy in out_copies():
                    copy.start()

            @pl.when((b >= first_late) & (b < first_turn))
            def _():
                own[b - first_late] = total(FINISH_LATE.get((c, e), ()))

            @pl.when(b >= first_turn)
            def _():
                own[b - first_late] = total(())

            @pl.when(b >= first_late)
            def _():
                late = b - first_late
                pltpu.make_async_copy(own.at[late], own_ref.at[late], late_sem).start()

        n_step = n_seq + LAG_MAX

        def when_seq(b, fn):
            pl.when((b >= 0) & (b < n_seq))(lambda: fn(b))

        def sent(b):
            for e in range(2):
                n = len(SENDS.get((c, e), ()))
                if n:
                    pl.when(core == e)(lambda: local_wait(acc.at[b % NACC, pl.ds(0, n)], tx_sem.at[b % NACC]))

        def step(t, carry):
            @pl.when(t < n_seq)
            def _():
                push_at(t)
                take_at(t)

                @pl.when(t + 1 < n_seq)
                def _():
                    qg_start(t + 1)

                @pl.when(t >= 2)
                def _():
                    odq_wait(t - 2)
                    part_copy(t - 2).wait_send()

                pl.when(t >= NACC)(lambda: sent(t - NACC))
                arrived(t)
                local_wait(qg.at[t % 2], qg_sem.at[t % 2])
                compute(t)
                odq_start(t)
                part_copy(t).start()

            when_seq(t - 1, merge_partner)
            for e in range(2):
                @pl.when(core == e)
                def _():
                    if (c, e) in RELAY:
                        when_seq(t - RELAY[c, e][0], lambda b: relay(b, e))
                    if (c, e) == (TURN[0], TURNED[1]):
                        b_turn = t - TURN_LAG
                        pl.when((b_turn >= first_turn) & (b_turn < n_seq))(lambda: add_turned(b_turn))
                    when_seq(t - FINISH[c, e][0], lambda b: finish(b, e))
            return carry

        lax.fori_loop(0, n_step, step, 0)

        for b in (n_seq - 2, n_seq - 1):
            odq_wait(b)
            part_copy(b).wait_send()
        for b in range(n_seq - NACC, n_seq):
            sent(b)
        whole = kv.at[:, :, 0, 0]
        for i, (_, _, who) in enumerate(flows):
            by_core(who, lambda: local_wait(whole, kv_tx.at[i]))
        local_wait(kv.at[:, :, here, 0], kvp_tx)
        for to in doc_dests:
            doc_copy(to).wait_send()
        if c == 0:
            pl.when(core == 1)(lambda: local_wait(rx2.at[pl.ds(0, first_turn)], fwd_tx))

    for c in range(n_chip):
        pl.when(chip == c)(functools.partial(run_chip, c))

    for copy in out_copies():
        copy.wait()
    local_wait(own, late_sem)


def copy_kernel(a_ref, b_ref, k_ref, v_ref, a_out, b_out, k_out, v_out, buf, in_sem, out_sem, k_buf, v_buf, kv_sem):
    n_buf, n_block = buf.shape[:2]
    total = 2 * a_ref.shape[0] // n_block
    ahead = n_buf // 2

    def read(i):
        src = (a_ref, b_ref)[i % 2].at[pl.ds(i // 2 * n_block, n_block)]
        return pltpu.make_async_copy(src, buf.at[i % n_buf], in_sem.at[i % n_buf])

    def write(i):
        dst = (a_out, b_out)[i % 2].at[pl.ds(i // 2 * n_block, n_block)]
        return pltpu.make_async_copy(buf.at[i % n_buf], dst, out_sem.at[i % n_buf])

    rows = pl.ds(0, k_ref.shape[0])
    small_in = [pltpu.make_async_copy(k_ref, k_buf, kv_sem.at[0]), pltpu.make_async_copy(v_ref, v_buf, kv_sem.at[1])]
    small_out = [pltpu.make_async_copy(k_buf, k_out.at[rows], kv_sem.at[0]),
                 pltpu.make_async_copy(v_buf, v_out.at[rows], kv_sem.at[1])]

    for i in range(ahead):
        read(i).start()
    for copy in small_in:
        copy.start()
    for i in range(total):
        if i + ahead < total:
            if i + ahead >= n_buf:
                write(i + ahead - n_buf).wait()
            read(i + ahead).start()
        read(i).wait()
        write(i).start()
        if i == ahead:
            for copy in small_in:
                copy.wait()
            for copy in small_out:
                copy.start()
    for i in range(max(total - n_buf, 0), total):
        write(i).wait()
    for copy in small_out:
        copy.wait()


def solution(mesh):
    n_dev = mesh.shape['cp']
    seq_spec = P('dp', 'cp', None, None)

    def per_device(query, keys, values, grad_out, doc_id):
        n_seq, piece, n_heads, head_dim = query.shape
        n_rows = piece * n_heads
        n_key = piece * n_dev
        two = 2 * piece
        rows_shape = (n_seq, n_rows, head_dim)
        kv_shape = (n_seq, piece, head_dim)
        late_shape = (N_LATE, two, head_dim)
        main_shape = (n_seq - N_LATE, piece, head_dim)
        bf16, f32, i32 = jnp.bfloat16, jnp.float32, jnp.int32
        dma = pltpu.SemaphoreType.DMA
        any_spec = pl.BlockSpec(memory_space=pl.ANY)
        n_chip = n_dev // 2
        out = pl.pallas_call(
            functools.partial(attention_kernel, n_dev, n_heads),
            name='attention',
            out_shape=[jax.ShapeDtypeStruct(rows_shape, bf16)] * 2 + [jax.ShapeDtypeStruct(main_shape, bf16)] * 2
            + [jax.ShapeDtypeStruct(late_shape, f32)] * 3,
            in_specs=[any_spec] * 5,
            out_specs=[any_spec] * 7,
            scratch_shapes=[
                pltpu.VMEM((n_seq, 2, n_chip, 2, piece, head_dim), bf16),
                pltpu.VMEM((n_seq, two, head_dim), f32),
                pltpu.VMEM((n_seq, two, head_dim), f32),
                pltpu.VMEM((n_seq, two, head_dim), f32),
                pltpu.VMEM((NACC, n_chip, two, head_dim), f32),
                pltpu.VMEM((2, 2, n_chip, two, head_dim), f32),
                pltpu.VMEM((NPRX, n_chip, two, head_dim), f32),
                pltpu.VMEM((2, 2, n_rows, head_dim), bf16),
                pltpu.VMEM((2, 2, n_rows, head_dim), bf16),
                pltpu.VMEM((n_rows, n_key), bf16),
                pltpu.VMEM((n_rows, n_key), bf16),
                pltpu.VMEM(main_shape, bf16),
                pltpu.VMEM(main_shape, bf16),
                pltpu.VMEM(late_shape, f32),
                pltpu.VMEM((n_dev, n_seq, piece), i32),
                pltpu.VMEM((n_seq, 1, n_key), i32),
                pltpu.VMEM((n_seq, 1, piece), i32),
                pltpu.VMEM((piece, n_key), f32),
                dma((5,)), dma, dma,
                dma((4,)), dma((n_chip, n_seq)), dma, dma((n_seq,)),
                dma((2,)), dma((2,)),
                dma((2,)), dma((NPRX,)), dma((3, n_seq)), dma((NACC,)), dma, dma,
            ],
            compiler_params=pltpu.CompilerParams(collective_id=0, has_side_effects=True, vmem_limit_bytes=63 * 1024 * 1024),
        )(query.reshape(rows_shape), grad_out.reshape(rows_shape), keys.reshape(kv_shape), values.reshape(kv_shape), doc_id)
        attn_out, grad_query, grad_keys, grad_values, near, far, own = out
        attn_out, grad_query, grad_keys, grad_values = pl.pallas_call(
            copy_kernel,
            name='results',
            out_shape=[jax.ShapeDtypeStruct(rows_shape, bf16)] * 2 + [jax.ShapeDtypeStruct(kv_shape, bf16)] * 2,
            in_specs=[pl.BlockSpec(memory_space=pltpu.HBM)] * 4,
            out_specs=[pl.BlockSpec(memory_space=pltpu.HBM)] * 4,
            scratch_shapes=[pltpu.VMEM((N_COPY, COPY_BLOCK, n_rows, head_dim), bf16), dma((N_COPY,)), dma((N_COPY,)),
                            pltpu.VMEM(main_shape, bf16), pltpu.VMEM(main_shape, bf16), dma((2,))],
            compiler_params=pltpu.CompilerParams(vmem_limit_bytes=56 * 1024 * 1024),
            cost_estimate=pl.CostEstimate(flops=12_000_000_000, bytes_accessed=8 * n_seq * n_rows * head_dim,
                                          transcendentals=0),
        )(attn_out, grad_query, grad_keys, grad_values)
        to_near = [(d, d - 2) for d in range(2, n_dev)]
        to_far = [(n_dev - 2 + e, e) for e in range(2)]
        from_far = lax.ppermute(far, 'cp', to_far)
        from_near = lax.ppermute(near, 'cp', to_near)
        late = own + from_far + from_near
        late_keys = (late[:, 0:piece] * head_dim ** -0.5).astype(bf16)
        late_values = late[:, piece:two].astype(bf16)
        grad_keys = lax.dynamic_update_slice(grad_keys, late_keys, (n_seq - N_LATE, 0, 0))
        grad_values = lax.dynamic_update_slice(grad_values, late_values, (n_seq - N_LATE, 0, 0))
        return (attn_out.reshape(query.shape), grad_query.reshape(query.shape),
                grad_keys.reshape(keys.shape), grad_values.reshape(values.shape))

    return jax.shard_map(per_device, mesh=mesh, in_specs=(seq_spec,) * 4 + (P('dp', 'cp'),), out_specs=(seq_spec,) * 4, check_vma=False)
```

```python
import functools

import jax
import jax.numpy as jnp
from jax import lax
from jax.experimental import pallas as pl
from jax.experimental.pallas import tpu as pltpu
from jax.sharding import PartitionSpec as P

MESH = pl.DeviceIdType.MESH
LOG2E = 1.4426950408889634
HIDDEN = -3.0e38
NACC = 12
NPRX = 4
COPY_BLOCK = 2
N_COPY = 32
N_FIRST = 1
N_TURN = 2
N_LATE = 8


HOPS = ((1, 1, 2, None), (1, 0, 2, None), (2, 1, 3, 0), (2, 2, 3, None), (0, 1, 3, 1), (1, 1, 0, 1), (0, 0, 3, None), (0, 0, 1, None))
PUSH = {0: (0, 8), 1: (2, 12), 2: (3, 3), 3: (2, 5)}
TAKE = {0: (0, 10), 1: (2, 6), 2: (2, 2), 3: (0, 1)}
SENDS = {(3, 0): ((1, 2, 0, False, None), (0, 0, 1, False, 1), (2, 2, 1, False, 0)), (3, 1): ((2, 2, 0, False, 0), (0, 0, 0, True, 1), (1, 0, 2, False, None)), (2, 0): ((1, 1, 1, True, 0), (0, 1, 0, False, None)), (2, 1): ((1, 1, 0, False, 0), (0, 3, 0, False, None)), (1, 0): ((0, 0, 0, True, 0),), (1, 1): ((0, 0, 1, False, 0),)}
RELAY = {(3, 1): (3, 0), (2, 0): (8, 0), (1, 0): (8, 0), (0, 1): (7, 2)}
FINISH = {(3, 0): (1, ()), (3, 1): (1, ()), (2, 0): (7, (1,)), (2, 1): (5, (0,)), (1, 0): (10, (1,)), (1, 1): (10, (0, 1)), (0, 0): (10, (0, 1)), (0, 1): (9, (0, 1))}
LAG_MAX = 10
FINISH_LATE = {(1, 1): (1,)}
TURNED, TURN, TURN_LAG = (3, 1, 1), (2, 1), 4


def attention_kernel(n_dev, n_heads, *refs):
    (q_ref, g_ref, k_ref, v_ref, doc_ref, o_ref, dq_ref, dk_ref, dv_ref, near_ref, far_ref, own_ref,
     kv, rx0, rx1, rx2, acc, part, prx, qg, odq, pb, dsb, fin_k, fin_v, own, docs, kdoc, odoc, vis,
     load_sem, doc_tx, doc_rx, kv_tx, kv_rx, kvp_tx, kvp_rx, qg_sem, odq_sem,
     part_tx, prx_sem, rx_sem, tx_sem, fwd_tx, late_sem) = refs
    rx = (rx0, rx1, rx2)
    n_seq, n_rows, head_dim = q_ref.shape
    piece = k_ref.shape[1]
    two = 2 * piece
    n_chip = n_dev // 2
    scale = head_dim ** -0.5
    me = lax.axis_index('cp')
    chip = me // 2
    core = me % 2
    partner = chip * 2 + (1 - core)

    def dev(c):
        return {'cp': c * 2 + core}

    def remote(src, dst, tx, rx, to):
        return pltpu.make_async_remote_copy(src_ref=src, dst_ref=dst, send_sem=tx, recv_sem=rx,
                                            device_id=to, device_id_type=MESH)

    def local_wait(ref, sem):
        pltpu.make_async_copy(ref, ref, sem).wait()

    barrier = pltpu.get_barrier_semaphore()
    for hop in range(1, n_dev):
        pl.semaphore_signal(barrier, inc=1, device_id={'cp': (me + hop) % n_dev}, device_id_type=MESH)

    def own_copies(lo, n, sem):
        seqs = pl.ds(lo, n)
        return (pltpu.make_async_copy(k_ref.at[seqs], kv.at[seqs, 0, chip, core], load_sem.at[sem]),
                pltpu.make_async_copy(v_ref.at[seqs], kv.at[seqs, 1, chip, core], load_sem.at[sem + 1]))

    own_d = pltpu.make_async_copy(doc_ref, docs.at[me], load_sem.at[4])
    own_first = own_copies(0, N_FIRST, 0)
    own_rest = own_copies(N_FIRST, n_seq - N_FIRST, 2)
    for copy in (*own_first, own_d, *own_rest):
        copy.start()

    def qg_start(b):
        pltpu.make_async_copy(q_ref.at[b], qg.at[b % 2, 0], qg_sem.at[b % 2]).start()
        pltpu.make_async_copy(g_ref.at[b], qg.at[b % 2, 1], qg_sem.at[b % 2]).start()

    def odq_start(b):
        pltpu.make_async_copy(odq.at[b % 2, 0], o_ref.at[b], odq_sem.at[b % 2]).start()
        pltpu.make_async_copy(odq.at[b % 2, 1], dq_ref.at[b], odq_sem.at[b % 2]).start()

    def odq_wait(b):
        local_wait(odq.at[b % 2], odq_sem.at[b % 2])

    qg_start(0)
    for copy in (*own_first, own_d):
        copy.wait()
    odoc[...] = docs[me].reshape(n_seq, 1, piece)
    pl.semaphore_wait(barrier, n_dev - 1)

    def out_copies():
        return (pltpu.make_async_copy(fin_k, dk_ref, load_sem.at[0]), pltpu.make_async_copy(fin_v, dv_ref, load_sem.at[1]))

    def run_chip(c):
        n_key = two * (c + 1)
        here = pl.ds(0, c + 1)
        first_late = n_seq - N_LATE
        first_turn = n_seq - N_TURN

        def doc_copy(to):
            return remote(docs.at[me], docs.at[me], doc_tx, doc_rx, to)

        doc_dests = [{'cp': partner}] + [{'cp': d} for d in range(two // piece * (c + 1), n_dev)]

        flows = [hop[1:] for hop in HOPS if hop[0] == c]
        through = [src for src, _, _ in flows if src > c]

        def by_core(who, fn):
            if who is None:
                fn()
            else:
                pl.when(core == who)(fn)

        def kv_sem(src, to, b):
            return kv_rx.at[0 if to == n_chip - 1 else src, b]

        def kv_copy(i, b):
            src, to, _ = flows[i]
            blk = kv.at[b, :, src, core]
            return remote(blk, blk, kv_tx.at[i], kv_sem(src, to, b), dev(to))

        def kvp_copy(b):
            blk = kv.at[b, :, here, core]
            return remote(blk, blk, kvp_tx, kvp_rx.at[b], {'cp': partner})

        def send_on(src, b):
            for i, (s, _, who) in enumerate(flows):
                if s == src:
                    by_core(who, lambda: kv_copy(i, b).start())

        def push(b):
            send_on(c, b)

        def take(b):
            if c == n_chip - 1:
                local_wait(kv.at[b, :, pl.ds(0, c), core], kv_rx.at[0, b])
            else:
                for src in range(c - 1, -1, -1):
                    local_wait(kv.at[b, :, src, core], kv_rx.at[src, b])
                    send_on(src, b)
            kvp_copy(b).start()
            for src in through:
                who = [w for s, _, w in flows if s == src][0]

                def pass_on():
                    local_wait(kv.at[b, :, src, core], kv_rx.at[src, b])
                    for i, (s, _, _) in enumerate(flows):
                        if s == src:
                            kv_copy(i, b).start()

                by_core(who, pass_on)

        def ramp(lead, fn):
            first, most = lead
            start = min(first, most)

            def at_step(t):
                b = jnp.minimum(start + 2 * t, t + most)
                pl.when(b < n_seq)(lambda: fn(b))

            def at_early_step(t):
                if most - start > 0:
                    pl.when(t < most - start)(lambda: fn(start + 2 * t + 1))

            return start, at_step, at_early_step

        def arrived(b):
            local_wait(kv.at[b, :, here, 1 - core], kvp_rx.at[b])

        n_push, push_at, push_early = ramp(PUSH[c], push)
        n_take, take_at, take_early = ramp(TAKE[c], take)
        for b in range(n_push):
            if b == N_FIRST:
                for copy in own_rest:
                    copy.wait()
            push(b)
        if n_push <= N_FIRST:
            for copy in own_rest:
                copy.wait()
        for to in doc_dests:
            doc_copy(to).start()
        for b in range(n_take):
            take(b)

        n_doc = 2 * c + 1
        pltpu.make_async_copy(docs.at[pl.ds(0, n_doc)], docs.at[pl.ds(0, n_doc)], doc_rx).wait()
        for p in range(2 * c + 2):
            kdoc[:, :, p * piece:(p + 1) * piece] = docs[p].reshape(n_seq, 1, piece)

        def compute(b):
            slot = b % 2
            keys = kv[b, 0, here].reshape(n_key, head_dim)
            vals = kv[b, 1, here].reshape(n_key, head_dim)
            tok = lax.broadcasted_iota(jnp.int32, (piece, piece), 0)
            tok_t = lax.broadcasted_iota(jnp.int32, (piece, piece), 1)
            own_doc = odoc[b]
            q_doc = jnp.sum(jnp.where(tok == tok_t, own_doc, 0), axis=1, keepdims=True)
            key_doc = kdoc[b, :, 0:n_key]
            q_pos = me * piece + lax.broadcasted_iota(jnp.int32, (piece, n_key), 0)
            k_pos = lax.broadcasted_iota(jnp.int32, (piece, n_key), 1)
            seen = (q_doc == key_doc) & (k_pos <= q_pos)
            vis[:, 0:n_key] = jnp.where(seen, 0.0, HIDDEN)
            nt = (((1,), (1,)), ((), ()))
            tn = (((0,), (0,)), ((), ()))
            f32 = jnp.float32
            s = lax.dot_general(qg[slot, 0], keys, nt, preferred_element_type=f32)
            dp = lax.dot_general(qg[slot, 1], vals, nt, preferred_element_type=f32)
            s = s.reshape(piece, n_heads, n_key) * (scale * LOG2E) + vis[:, 0:n_key].reshape(piece, 1, n_key)
            s = s.reshape(n_rows, n_key)
            e = jnp.exp2(s - jnp.max(s, axis=1, keepdims=True))
            p = e * (1.0 / jnp.sum(e, axis=1, keepdims=True))
            pb[:, 0:n_key] = p.astype(jnp.bfloat16)
            o16 = jnp.dot(pb[:, 0:n_key], vals, preferred_element_type=f32).astype(jnp.bfloat16)
            dv = lax.dot_general(pb[:, 0:n_key], qg[slot, 1], tn, preferred_element_type=f32)
            odq[slot, 0] = o16
            delta = jnp.sum(qg[slot, 1].astype(f32) * o16.astype(f32), axis=1, keepdims=True)
            dsb[:, 0:n_key] = (p * (dp - delta)).astype(jnp.bfloat16)
            dq = jnp.dot(dsb[:, 0:n_key], keys, preferred_element_type=f32)
            odq[slot, 1] = (dq * scale).astype(jnp.bfloat16)
            dk = lax.dot_general(dsb[:, 0:n_key], qg[slot, 0], tn, preferred_element_type=f32)
            for a in range(c + 1):
                for p in range(2):
                    rows = slice((2 * a + p) * piece, (2 * a + p + 1) * piece)
                    part[slot, p, a, 0:piece, :] = dk[rows]
                    part[slot, p, a, piece:two, :] = dv[rows]

        def part_copy(b):
            return remote(part.at[b % 2, 1 - core, here], prx.at[b % NPRX, here], part_tx.at[b % 2],
                          prx_sem.at[b % NPRX], {'cp': partner})

        def unit_send(b, e, i):
            a, to, buf, _, late = SENDS[c, e][i]
            unit = acc.at[b % NACC, a]
            sem = tx_sem.at[b % NACC]

            def now(to=to, buf=buf):
                remote(unit, rx[buf].at[b], sem, rx_sem.at[buf, b], dev(to)).start()

            if (c, e, a) == TURNED:
                pl.when(b < first_turn)(now)
                pl.when(b >= first_turn)(lambda: now(*TURN))
            elif late is None:
                now()
            else:
                pl.when(b < first_late)(now)

                @pl.when(b >= first_late)
                def _():
                    pltpu.make_async_copy(unit, (near_ref, far_ref)[late].at[b - first_late], sem).start()

        def got(buf, b):
            local_wait(rx[buf].at[b], rx_sem.at[buf, b])

        def merge_partner(b):
            local_wait(prx.at[b % NPRX, here], prx_sem.at[b % NPRX])
            acc[b % NACC, here] = part[b % 2, core, here] + prx[b % NPRX, here]
            for e in range(2):
                sends = [i for i, s in enumerate(SENDS.get((c, e), ())) if not s[3]]
                if sends:
                    @pl.when(core == e)
                    def _():
                        for i in sends:
                            if (c, e, SENDS[c, e][i][0]) == (TURN[0], TURNED[1], TURNED[2]):
                                pl.when(b < first_turn)(lambda: unit_send(b, e, i))
                            else:
                                unit_send(b, e, i)

        def relay(b, e):
            buf = RELAY[c, e][1]

            def take_in():
                got(buf, b)
                if c == 0:
                    fwd_copy(b).start()
                    return
                for i, (a, _, _, after, _) in enumerate(SENDS[c, e]):
                    if after:
                        acc[b % NACC, a] = acc[b % NACC, a] + rx[buf][b]
                        unit_send(b, e, i)

            if c == 0:
                pl.when(b < first_turn)(take_in)
            else:
                take_in()

        def add_turned(b):
            got(TURN[1], b)
            a = TURNED[2]
            acc[b % NACC, a] = acc[b % NACC, a] + rx[TURN[1]][b]
            unit_send(b, TURNED[1], [s[0] for s in SENDS[c, TURNED[1]]].index(a))

        def fwd_copy(b):
            return remote(rx2.at[b], rx1.at[b], fwd_tx, rx_sem.at[1, b], dev(1))

        def finish(b, e):
            def total(bufs):
                out = acc[b % NACC, c]
                for buf in bufs:
                    got(buf, b)
                    out = out + rx[buf][b]
                return out

            @pl.when(b < first_late)
            def _():
                out = total(FINISH[c, e][1])
                fin_k[b] = (out[0:piece] * scale).astype(jnp.bfloat16)
                fin_v[b] = out[piece:two].astype(jnp.bfloat16)

            @pl.when(b == first_late)
            def _():
                for copy in out_copies():
                    copy.start()

            @pl.when((b >= first_late) & (b < first_turn))
            def _():
                own[b - first_late] = total(FINISH_LATE.get((c, e), ()))

            @pl.when(b >= first_turn)
            def _():
                own[b - first_late] = total(())

            @pl.when(b >= first_late)
            def _():
                late = b - first_late
                pltpu.make_async_copy(own.at[late], own_ref.at[late], late_sem).start()

        n_step = n_seq + LAG_MAX

        def when_seq(b, fn):
            pl.when((b >= 0) & (b < n_seq))(lambda: fn(b))

        def sent(b):
            for e in range(2):
                n = len(SENDS.get((c, e), ()))
                if n:
                    pl.when(core == e)(lambda: local_wait(acc.at[b % NACC, pl.ds(0, n)], tx_sem.at[b % NACC]))

        def step(t, carry):
            @pl.when(t < n_seq)
            def _():
                push_at(t)
                push_early(t)
                take_at(t)
                if c < n_chip - 1:
                    take_early(t)

                @pl.when(t + 1 < n_seq)
                def _():
                    qg_start(t + 1)

                @pl.when(t >= 2)
                def _():
                    odq_wait(t - 2)
                    part_copy(t - 2).wait_send()

                pl.when(t >= NACC)(lambda: sent(t - NACC))
                arrived(t)
                local_wait(qg.at[t % 2], qg_sem.at[t % 2])
                compute(t)
                odq_start(t)
                part_copy(t).start()
                if c == n_chip - 1:
                    take_early(t)

            when_seq(t - 1, merge_partner)
            for e in range(2):
                @pl.when(core == e)
                def _():
                    if (c, e) in RELAY:
                        when_seq(t - RELAY[c, e][0], lambda b: relay(b, e))
                    if (c, e) == (TURN[0], TURNED[1]):
                        b_turn = t - TURN_LAG
                        pl.when((b_turn >= first_turn) & (b_turn < n_seq))(lambda: add_turned(b_turn))
                    when_seq(t - FINISH[c, e][0], lambda b: finish(b, e))
            return carry

        lax.fori_loop(0, n_step, step, 0)

        for b in (n_seq - 2, n_seq - 1):
            odq_wait(b)
            part_copy(b).wait_send()
        for b in range(n_seq - NACC, n_seq):
            sent(b)
        whole = kv.at[:, :, 0, 0]
        for i, (_, _, who) in enumerate(flows):
            by_core(who, lambda: local_wait(whole, kv_tx.at[i]))
        local_wait(kv.at[:, :, here, 0], kvp_tx)
        for to in doc_dests:
            doc_copy(to).wait_send()
        if c == 0:
            pl.when(core == 1)(lambda: local_wait(rx2.at[pl.ds(0, first_turn)], fwd_tx))

    for c in range(n_chip):
        pl.when(chip == c)(functools.partial(run_chip, c))

    for copy in out_copies():
        copy.wait()
    local_wait(own, late_sem)


def copy_kernel(a_ref, b_ref, k_ref, v_ref, a_out, b_out, k_out, v_out, buf, in_sem, out_sem, k_buf, v_buf, kv_sem):
    n_buf, n_block = buf.shape[:2]
    total = 2 * a_ref.shape[0] // n_block
    ahead = n_buf // 2

    def read(i):
        src = (a_ref, b_ref)[i % 2].at[pl.ds(i // 2 * n_block, n_block)]
        return pltpu.make_async_copy(src, buf.at[i % n_buf], in_sem.at[i % n_buf])

    def write(i):
        dst = (a_out, b_out)[i % 2].at[pl.ds(i // 2 * n_block, n_block)]
        return pltpu.make_async_copy(buf.at[i % n_buf], dst, out_sem.at[i % n_buf])

    rows = pl.ds(0, k_ref.shape[0])
    small_in = [pltpu.make_async_copy(k_ref, k_buf, kv_sem.at[0]), pltpu.make_async_copy(v_ref, v_buf, kv_sem.at[1])]
    small_out = [pltpu.make_async_copy(k_buf, k_out.at[rows], kv_sem.at[0]),
                 pltpu.make_async_copy(v_buf, v_out.at[rows], kv_sem.at[1])]

    for i in range(ahead):
        read(i).start()
    for copy in small_in:
        copy.start()
    for i in range(total):
        if i + ahead < total:
            if i + ahead >= n_buf:
                write(i + ahead - n_buf).wait()
            read(i + ahead).start()
        read(i).wait()
        write(i).start()
        if i == ahead:
            for copy in small_in:
                copy.wait()
            for copy in small_out:
                copy.start()
    for i in range(max(total - n_buf, 0), total):
        write(i).wait()
    for copy in small_out:
        copy.wait()


def solution(mesh):
    n_dev = mesh.shape['cp']
    seq_spec = P('dp', 'cp', None, None)

    def per_device(query, keys, values, grad_out, doc_id):
        n_seq, piece, n_heads, head_dim = query.shape
        n_rows = piece * n_heads
        n_key = piece * n_dev
        two = 2 * piece
        rows_shape = (n_seq, n_rows, head_dim)
        kv_shape = (n_seq, piece, head_dim)
        late_shape = (N_LATE, two, head_dim)
        main_shape = (n_seq - N_LATE, piece, head_dim)
        bf16, f32, i32 = jnp.bfloat16, jnp.float32, jnp.int32
        dma = pltpu.SemaphoreType.DMA
        any_spec = pl.BlockSpec(memory_space=pl.ANY)
        n_chip = n_dev // 2
        out = pl.pallas_call(
            functools.partial(attention_kernel, n_dev, n_heads),
            name='attention',
            out_shape=[jax.ShapeDtypeStruct(rows_shape, bf16)] * 2 + [jax.ShapeDtypeStruct(main_shape, bf16)] * 2
            + [jax.ShapeDtypeStruct(late_shape, f32)] * 3,
            in_specs=[any_spec] * 5,
            out_specs=[any_spec] * 7,
            scratch_shapes=[
                pltpu.VMEM((n_seq, 2, n_chip, 2, piece, head_dim), bf16),
                pltpu.VMEM((n_seq, two, head_dim), f32),
                pltpu.VMEM((n_seq, two, head_dim), f32),
                pltpu.VMEM((n_seq, two, head_dim), f32),
                pltpu.VMEM((NACC, n_chip, two, head_dim), f32),
                pltpu.VMEM((2, 2, n_chip, two, head_dim), f32),
                pltpu.VMEM((NPRX, n_chip, two, head_dim), f32),
                pltpu.VMEM((2, 2, n_rows, head_dim), bf16),
                pltpu.VMEM((2, 2, n_rows, head_dim), bf16),
                pltpu.VMEM((n_rows, n_key), bf16),
                pltpu.VMEM((n_rows, n_key), bf16),
                pltpu.VMEM(main_shape, bf16),
                pltpu.VMEM(main_shape, bf16),
                pltpu.VMEM(late_shape, f32),
                pltpu.VMEM((n_dev, n_seq, piece), i32),
                pltpu.VMEM((n_seq, 1, n_key), i32),
                pltpu.VMEM((n_seq, 1, piece), i32),
                pltpu.VMEM((piece, n_key), f32),
                dma((5,)), dma, dma,
                dma((4,)), dma((n_chip, n_seq)), dma, dma((n_seq,)),
                dma((2,)), dma((2,)),
                dma((2,)), dma((NPRX,)), dma((3, n_seq)), dma((NACC,)), dma, dma,
            ],
            compiler_params=pltpu.CompilerParams(collective_id=0, has_side_effects=True, vmem_limit_bytes=63 * 1024 * 1024),
        )(query.reshape(rows_shape), grad_out.reshape(rows_shape), keys.reshape(kv_shape), values.reshape(kv_shape), doc_id)
        attn_out, grad_query, grad_keys, grad_values, near, far, own = out
        attn_out, grad_query, grad_keys, grad_values = pl.pallas_call(
            copy_kernel,
            name='results',
            out_shape=[jax.ShapeDtypeStruct(rows_shape, bf16)] * 2 + [jax.ShapeDtypeStruct(kv_shape, bf16)] * 2,
            in_specs=[pl.BlockSpec(memory_space=pltpu.HBM)] * 4,
            out_specs=[pl.BlockSpec(memory_space=pltpu.HBM)] * 4,
            scratch_shapes=[pltpu.VMEM((N_COPY, COPY_BLOCK, n_rows, head_dim), bf16), dma((N_COPY,)), dma((N_COPY,)),
                            pltpu.VMEM(main_shape, bf16), pltpu.VMEM(main_shape, bf16), dma((2,))],
            compiler_params=pltpu.CompilerParams(vmem_limit_bytes=56 * 1024 * 1024),
            cost_estimate=pl.CostEstimate(flops=12_000_000_000, bytes_accessed=8 * n_seq * n_rows * head_dim,
                                          transcendentals=0),
        )(attn_out, grad_query, grad_keys, grad_values)
        to_near = [(d, d - 2) for d in range(2, n_dev)]
        to_far = [(n_dev - 2 + e, e) for e in range(2)]
        from_far = lax.ppermute(far, 'cp', to_far)
        from_near = lax.ppermute(near, 'cp', to_near)
        late = own + from_far + from_near
        late_keys = (late[:, 0:piece] * head_dim ** -0.5).astype(bf16)
        late_values = late[:, piece:two].astype(bf16)
        grad_keys = lax.dynamic_update_slice(grad_keys, late_keys, (n_seq - N_LATE, 0, 0))
        grad_values = lax.dynamic_update_slice(grad_values, late_values, (n_seq - N_LATE, 0, 0))
        return (attn_out.reshape(query.shape), grad_query.reshape(query.shape),
                grad_keys.reshape(keys.shape), grad_values.reshape(values.shape))

    return jax.shard_map(per_device, mesh=mesh, in_specs=(seq_spec,) * 4 + (P('dp', 'cp'),), out_specs=(seq_spec,) * 4, check_vma=False)
```
